32 devices in a mesh: dp: 4 (over z), seq: 4 (over y, x), tensor: 2 (over core).
Axes of the slice: x: 2, y: 2, z: 4, core: 2. Of those that a mesh axis runs over, the one named last changes fastest.
Arguments:
- tokens: bfloat16 [1088, 12, 384], P(('seq', 'tensor'), 'dp'), may hold values from -16 to 16
- out_grad: float32 [1088, 12, 384], P('seq', 'dp'), may hold values from -6 to 6
- keep_mask: int32 [1088, 12], P(None, 'dp'), may hold values from 0 to 1, as said below
- w_qkv: float32 [3, 384, 384], P(None, None, 'tensor'), may hold values from -0.3125 to 0.3125
- w_out: float32 [384, 384], P('tensor'), may hold values from -6 to 6
- w_gate_up: float32 [2, 384, 1024], P(None, None, 'tensor'), may hold values from -0.3125 to 0.3125
- w_down: float32 [1024, 384], P('tensor'), may hold values from -0.1875 to 0.1875
- norm_pack: float32 [4, 384], replicated, may hold values from -1.5 to 1.75
- inner_pack: float32 [2, 1024], P(None, 'tensor'), may hold values from -1.5 to 1.75
- moment_qkv: float32 [3, 384, 384], P(None, None, 'tensor'), may hold values from -0.6 to 0.6
- moment_out: float32 [384, 384], P('tensor'), may hold values from -0.6 to 0.6
- moment_gate_up: float32 [2, 384, 1024], P(None, None, 'tensor'), may hold values from -0.6 to 0.6
- moment_down: float32 [1024, 384], P('tensor'), may hold values from -0.6 to 0.6
- moment_norm: float32 [4, 384], replicated, may hold values from -0.6 to 0.6
- moment_inner: float32 [2, 1024], P(None, 'tensor'), may hold values from -0.6 to 0.6
- error_qkv: float32 [16, 3, 384, 384], P(('dp', 'seq'), None, None, 'tensor'), may hold values from -5 to 5
- error_out: float32 [16, 384, 384], P(('dp', 'seq'), 'tensor'), may hold values from -5 to 5
- error_gate_up: float32 [16, 2, 384, 1024], P(('dp', 'seq'), None, None, 'tensor'), may hold values from -5 to 5
- error_down: float32 [16, 1024, 384], P(('dp', 'seq'), 'tensor'), may hold values from -5 to 5
- basis_qkv: float32 [3, 384, 8], P(None, 'tensor'), may hold values from -6 to 6
- basis_out: float32 [384, 8], P('tensor'), may hold values from -6 to 6
- basis_gate_up: float32 [2, 1024, 8], P(None, 'tensor'), may hold values from -6 to 6
- basis_down: float32 [1024, 8], P('tensor'), may hold values from -6 to 6
Outputs:
- residual: float32 [1088, 12, 384], P(('seq', 'tensor'), 'dp')
- input_grad: float32 [1088, 12, 384], P(('seq', 'tensor'), 'dp')
- factor_left: float32 [5, 384, 8], replicated
- factor_qkv: float32 [3, 384, 8], P(None, 'tensor')
- factor_out: float32 [384, 8], P('tensor')
- factor_gate_up: float32 [2, 1024, 8], P(None, 'tensor')
- factor_down: float32 [1024, 8], P('tensor')
- new_error_qkv: float32 [16, 3, 384, 384], P(('dp', 'seq'), None, None, 'tensor')
- new_error_out: float32 [16, 384, 384], P(('dp', 'seq'), 'tensor')
- new_error_gate_up: float32 [16, 2, 384, 1024], P(('dp', 'seq'), None, None, 'tensor')
- new_error_down: float32 [16, 1024, 384], P(('dp', 'seq'), 'tensor')
- new_moment_qkv: float32 [3, 384, 384], P(None, None, 'tensor')
- new_moment_out: float32 [384, 384], P('tensor')
- new_moment_gate_up: float32 [2, 384, 1024], P(None, None, 'tensor')
- new_moment_down: float32 [1024, 384], P('tensor')
- new_moment_norm: float32 [4, 384], replicated
- new_moment_inner: float32 [2, 1024], P(None, 'tensor')
- new_w_qkv: float32 [3, 384, 384], P(None, None, 'tensor')
- new_w_out: float32 [384, 384], P('tensor')
- new_w_gate_up: float32 [2, 384, 1024], P(None, None, 'tensor')
- new_w_down: float32 [1024, 384], P('tensor')
- new_norm_pack: float32 [4, 384], replicated
- new_inner_pack: float32 [2, 1024], P(None, 'tensor')
- branch_rms: float32 [2], replicated
The draws below stay inside these ranges and needn't reach their ends.
Inputs may be any that keep to these rules, and one draw needn't show every extreme that they name: keep_mask is 1 at slot 0 of every image and 0 at every slot after 32 * 32.
All inputs are finite; a program needn't handle non-finite values.
Results may differ from the reference program's by a relative error of at most 0.014.
The reference program's roundings to bfloat16 on the way count: a program that leaves them out, or rounds other values in their place, can miss the bound.
Values may be sent and summed in bfloat16 or wider, within the bound.
A program may use at most 192 MiB of HBM per device.

```python
import jax
import jax.numpy as jnp
from jax import lax

D = 384
HEADS = 6
DH = 64
FF = 1024
GRID = 32
SLOTS = 1088
RANK = 8
IMG_DEV = 3
IMAGES = 12
REPLICAS = 16
N_DP = 4
N_SEQ = 4


def clipped_normal(key, shape):
    return jnp.clip(jax.random.normal(key, shape, jnp.float32), -5.0, 5.0)


def draw_tokens(key, part):
    base = jax.random.fold_in(key, 21)
    column = jnp.exp(jax.random.uniform(jax.random.fold_in(base, 1), (1, 1, D), jnp.float32, -1.15, 1.15))
    values = clipped_normal(jax.random.fold_in(base, 2), (SLOTS, IMAGES, D))
    return (values * column).astype(jnp.bfloat16)


def draw_keep_mask(key, part):
    coin = jax.random.randint(jax.random.fold_in(key, 11), (SLOTS, IMAGES), 0, 4)
    slot_ids = jnp.arange(SLOTS, dtype=jnp.int32)[:, None]
    kept = jnp.where(coin > 0, 1, 0)
    kept = jnp.where(slot_ids == 0, 1, kept)
    kept = jnp.where(slot_ids > GRID * GRID, 0, kept)
    return kept.astype(jnp.int32)


def pack_draw(key, rows, width):
    noise = clipped_normal(key, (rows, width))
    row_ids = jnp.arange(rows, dtype=jnp.int32)[:, None]
    return jnp.where(row_ids % 2 == 0, 1.0 + 0.15 * noise, 0.3 * noise).astype(jnp.float32)


def draw_norm_pack(key, part):
    return pack_draw(jax.random.fold_in(key, 31), 4, D)


def draw_inner_pack(key, part):
    return pack_draw(jax.random.fold_in(key, 32), 2, FF)


def error_draw(key, tag, shape):
    base = jax.random.fold_in(key, tag)
    common = 0.5 * clipped_normal(jax.random.fold_in(base, 1), shape[1:])
    own = 0.5 * clipped_normal(jax.random.fold_in(base, 2), shape)
    return (common[None] + own).astype(jnp.float32)


def draw_error_qkv(key, part):
    return error_draw(key, 41, (REPLICAS, 3, D, D))


def draw_error_out(key, part):
    return error_draw(key, 42, (REPLICAS, D, D))


def draw_error_gate_up(key, part):
    return error_draw(key, 43, (REPLICAS, 2, D, FF))


def draw_error_down(key, part):
    return error_draw(key, 44, (REPLICAS, FF, D))


def steps_of(rng, extent, shards, smallest, high):
    def one(axis_at, parts):
        heights = jax.random.uniform(jax.random.fold_in(jax.random.fold_in(rng, 6), axis_at), (parts,), jnp.float32, smallest / len(shards), high / len(shards))
        return jnp.repeat(jnp.exp(heights), extent[axis_at] // parts).reshape((-1,) + (1,) * (len(extent) - axis_at - 1))

    loudness = one(*shards[0])
    for cut in shards[1:]:
        loudness = loudness * one(*cut)
    return loudness


def normal_values(own_key, shape, scale, most, cuts=(), held_as=jnp.bfloat16):
    level = steps_of(own_key, shape, cuts, -0.22, 0.18) if cuts else 1.0
    drawn = jax.random.normal(own_key, shape, jnp.float32) * scale * level
    return jnp.minimum(jnp.maximum(drawn, -most), most).astype(held_as)


def setup_inputs(seed: int = 0) -> dict:
    key_list = jax.random.split(jax.random.key(seed), 24)
    tokens = draw_tokens(jax.random.fold_in(key_list[23], 71), 0)
    out_grad = normal_values(key_list[1], (SLOTS, IMAGES, D), 1.0, 6.0, ((0, 4), (1, 4)), jnp.float32)
    keep_mask = draw_keep_mask(jax.random.fold_in(key_list[23], 71), 0)
    w_qkv = normal_values(key_list[3], (3, D, D), D ** -0.5, 0.3125, ((2, 2),), jnp.float32)
    w_out = normal_values(key_list[4], (D, D), (max(1, 4 * D // SLOTS)) ** -0.5, 6.0, ((0, 2),), jnp.float32)
    w_gate_up = normal_values(key_list[5], (2, D, FF), D ** -0.5, 0.3125, ((2, 2),), jnp.float32)
    w_down = normal_values(key_list[6], (FF, D), FF ** -0.5, 0.1875, ((0, 2),), jnp.float32)
    norm_pack = draw_norm_pack(jax.random.fold_in(key_list[23], 71), 0)
    inner_pack = draw_inner_pack(jax.random.fold_in(key_list[23], 71), 0)
    moment_qkv = normal_values(key_list[9], (3, D, D), 0.1, 0.6, ((2, 2),), jnp.float32)
    moment_out = normal_values(key_list[10], (D, D), 0.1, 0.6, ((0, 2),), jnp.float32)
    moment_gate_up = normal_values(key_list[11], (2, D, FF), 0.1, 0.6, ((2, 2),), jnp.float32)
    moment_down = normal_values(key_list[12], (FF, D), 0.1, 0.6, ((0, 2),), jnp.float32)
    moment_norm = normal_values(key_list[13], (4, D), 0.1, 0.6, (), jnp.float32)
    moment_inner = normal_values(key_list[14], (2, FF), 0.1, 0.6, ((1, 2),), jnp.float32)
    error_qkv = draw_error_qkv(jax.random.fold_in(key_list[23], 71), 0)
    error_out = draw_error_out(jax.random.fold_in(key_list[23], 71), 0)
    error_gate_up = draw_error_gate_up(jax.random.fold_in(key_list[23], 71), 0)
    error_down = draw_error_down(jax.random.fold_in(key_list[23], 71), 0)
    basis_qkv = normal_values(key_list[19], (3, D, RANK), 1.0, 6.0, ((1, 2),), jnp.float32)
    basis_out = normal_values(key_list[20], (D, RANK), 1.0, 6.0, ((0, 2),), jnp.float32)
    basis_gate_up = normal_values(key_list[21], (2, FF, RANK), 1.0, 6.0, ((1, 2),), jnp.float32)
    basis_down = normal_values(key_list[22], (FF, RANK), 1.0, 6.0, ((0, 2),), jnp.float32)
    return {"tokens": tokens, "out_grad": out_grad, "keep_mask": keep_mask, "w_qkv": w_qkv, "w_out": w_out, "w_gate_up": w_gate_up, "w_down": w_down, "norm_pack": norm_pack, "inner_pack": inner_pack, "moment_qkv": moment_qkv, "moment_out": moment_out, "moment_gate_up": moment_gate_up, "moment_down": moment_down, "moment_norm": moment_norm, "moment_inner": moment_inner, "error_qkv": error_qkv, "error_out": error_out, "error_gate_up": error_gate_up, "error_down": error_down, "basis_qkv": basis_qkv, "basis_out": basis_out, "basis_gate_up": basis_gate_up, "basis_down": basis_down}


EPSILON = 1e-06
MOMENTUM = 0.9
STEP_RATE = 0.5
HIGH = lax.Precision.HIGHEST

@jax.custom_vjp
def low(v):
    return lax.optimization_barrier(v.astype(jnp.bfloat16)).astype(jnp.float32)

@jax.custom_vjp
def low_back(v):
    return v

def low_keep(v):
    return (low(v), None)

def low_pass(kept, grad):
    return (grad,)

def back_keep(v):
    return (v, None)

def back_low(kept, grad):
    return (low(grad),)
low.defvjp(low_keep, low_pass)
low_back.defvjp(back_keep, back_low)

def layer_norm(values, gain, bias):
    centre = values - lax.optimization_barrier(jnp.mean(values, -1, keepdims=True))
    spread = lax.optimization_barrier(jnp.mean(centre * centre, -1, keepdims=True))
    return centre * lax.rsqrt(spread + EPSILON) * gain + bias

def rope_tables(first_slot, count):
    slot_ids = first_slot + jnp.arange(count, dtype=jnp.int32)
    inside = jnp.logical_and(slot_ids >= 1, slot_ids <= GRID * GRID)
    patch = jnp.where(inside, slot_ids - 1, 0)
    row_pos = (patch // GRID).astype(jnp.float32)
    col_pos = (patch % GRID).astype(jnp.float32)
    quarter = DH // 4
    freqs = 10000.0 ** (-jnp.arange(quarter, dtype=jnp.float32) / quarter)
    angles = jnp.concatenate([row_pos[:, None] * freqs, col_pos[:, None] * freqs], -1) * (16.0 / GRID)
    return (jnp.cos(angles), jnp.sin(angles))

def rotate(heads, cosine_table, sine_table):
    quarter = heads.shape[-1] // 4
    first = jnp.concatenate([heads[..., :quarter], heads[..., 2 * quarter:3 * quarter]], -1)
    second = jnp.concatenate([heads[..., quarter:2 * quarter], heads[..., 3 * quarter:]], -1)
    cosine = cosine_table[:, None, None, :]
    sine = sine_table[:, None, None, :]
    new_first = first * cosine - second * sine
    new_second = second * cosine + first * sine
    return jnp.concatenate([new_first[..., :quarter], new_second[..., :quarter], new_first[..., quarter:], new_second[..., quarter:]], -1)

def orthonormal(matrix):
    columns = []
    for index in range(RANK):
        column = matrix[:, index]
        for done in columns:
            column = column - jnp.sum(done * column) * done
        column = column * lax.rsqrt(jnp.sum(column * column) + EPSILON)
        columns.append(column)
    return jnp.stack(columns, -1)

def block_forward(params, inputs, key_ok, cosine_table, sine_table):
    w_qkv, w_out, w_gate_up, w_down, norm_pack, inner_pack = params
    images = inputs.shape[1]
    seq_rows = SLOTS // N_SEQ
    blocks = inputs.reshape(N_SEQ, seq_rows, images, D)
    gain_one = norm_pack[:, 0][:, None, None, :]
    bias_one = norm_pack[:, 1][:, None, None, :]
    gain_two = norm_pack[:, 2][:, None, None, :]
    bias_two = norm_pack[:, 3][:, None, None, :]
    gain_three = inner_pack[:, 0][:, None, None, :]
    bias_three = inner_pack[:, 1][:, None, None, :]
    normed_one = low(layer_norm(blocks, gain_one, bias_one))
    projected = low_back(jnp.einsum('stbd,sjde->jstbe', normed_one, low(w_qkv), precision=HIGH))
    projected = projected.reshape(3, SLOTS, images, HEADS, DH)
    queries = low(rotate(projected[0], cosine_table, sine_table))
    keys_all = low(rotate(projected[1], cosine_table, sine_table))
    values_all = low(projected[2])
    scores = low_back(jnp.einsum('qbhd,kbhd->bhqk', queries, keys_all, precision=HIGH) * DH ** (-0.5))
    scores = jnp.where(key_ok, scores, -1e+30)
    row_max = lax.optimization_barrier(jnp.max(scores, -1, keepdims=True))
    exponent = jnp.exp(scores - row_max)
    attn_probs = exponent / lax.optimization_barrier(jnp.sum(exponent, -1, keepdims=True))
    attended = jnp.einsum('bhqk,kbhd->qbhd', low(attn_probs), values_all, precision=HIGH)
    attended = low(low_back(attended)).reshape(N_SEQ, seq_rows, images, D)
    branch_one = low_back(jnp.einsum('stbh,she->stbe', attended, low(w_out), precision=HIGH))
    middle = blocks + branch_one
    normed_two = low(layer_norm(middle, gain_two, bias_two))
    gate_up = low_back(jnp.einsum('stbd,sjdf->jstbf', normed_two, low(w_gate_up), precision=HIGH))
    hidden = gate_up[0] / (1.0 + jnp.exp(-gate_up[0])) * gate_up[1]
    normed_three = low(layer_norm(hidden, gain_three, bias_three))
    branch_two = low_back(jnp.einsum('stbf,sfe->stbe', normed_three, low(w_down), precision=HIGH))
    output = (middle + branch_two).reshape(SLOTS, images, D)
    squares = jnp.stack([jnp.sum(branch_one * branch_one), jnp.sum(branch_two * branch_two)])
    return (output, squares)

def reference(tokens, out_grad, keep_mask, w_qkv, w_out, w_gate_up, w_down, norm_pack, inner_pack, moment_qkv, moment_out, moment_gate_up, moment_down, moment_norm, moment_inner, error_qkv, error_out, error_gate_up, error_down, basis_qkv, basis_out, basis_gate_up, basis_down):
    weights = (w_qkv, w_out, w_gate_up, w_down, norm_pack, inner_pack)
    cosine_table, sine_table = rope_tables(0, SLOTS)

    def group(item):
        token_group, grad_group, mask_group = item
        copies = tuple((jnp.broadcast_to(weight, (N_SEQ,) + weight.shape) for weight in weights))
        key_ok = (jnp.transpose(mask_group) > 0)[:, None, None, :]

        def forward(params, inputs):
            return block_forward(params, inputs, key_ok, cosine_table, sine_table)
        output, pull, squares = jax.vjp(forward, copies, token_group.astype(jnp.float32), has_aux=True)
        cotangent = grad_group * mask_group[:, :, None].astype(jnp.float32)
        grads, grad_input = pull(cotangent)
        return (output, grad_input, grads, squares)

    def split(array):
        return jnp.moveaxis(array.reshape((SLOTS, N_DP, IMG_DEV) + array.shape[2:]), 1, 0)

    def join(array):
        return jnp.moveaxis(array, 0, 1).reshape((SLOTS, N_DP * IMG_DEV) + array.shape[3:])
    outputs, grad_inputs, grads, squares = lax.map(group, (split(tokens), split(out_grad), split(keep_mask)))
    grad_scale = (IMG_DEV * (SLOTS // N_SEQ)) ** (-0.5)
    grads = tuple((part.reshape((REPLICAS,) + part.shape[2:]) * grad_scale for part in grads))
    grad_qkv, grad_out, grad_gate_up, grad_down, grad_norm, grad_inner = grads
    full_qkv = grad_qkv + error_qkv
    full_out = grad_out + error_out
    full_gate_up = grad_gate_up + error_gate_up
    full_down = grad_down + error_down
    left_parts = jnp.concatenate([jnp.einsum('rjde,jes->ds', full_qkv, basis_qkv, precision=HIGH)[None], jnp.einsum('rhe,hs->es', full_out, basis_out, precision=HIGH)[None], jnp.einsum('rjdf,jfs->jds', full_gate_up, basis_gate_up, precision=HIGH), jnp.einsum('rfd,fs->ds', full_down, basis_down, precision=HIGH)[None]], 0)
    factor_left = jnp.stack([orthonormal(left_parts[index]) for index in range(5)])
    factor_qkv = jnp.einsum('rjde,ds->jes', full_qkv, factor_left[0], precision=HIGH) / REPLICAS
    factor_out = jnp.einsum('rhe,es->hs', full_out, factor_left[1], precision=HIGH) / REPLICAS
    factor_gate_up = jnp.einsum('rjdf,jds->jfs', full_gate_up, factor_left[2:4], precision=HIGH) / REPLICAS
    factor_down = jnp.einsum('rfd,ds->fs', full_down, factor_left[4], precision=HIGH) / REPLICAS
    approx_qkv = jnp.einsum('ds,jes->jde', factor_left[0], factor_qkv, precision=HIGH)
    approx_out = jnp.einsum('es,hs->he', factor_left[1], factor_out, precision=HIGH)
    approx_gate_up = jnp.einsum('jds,jfs->jdf', factor_left[2:4], factor_gate_up, precision=HIGH)
    approx_down = jnp.einsum('ds,fs->fd', factor_left[4], factor_down, precision=HIGH)
    new_moment_qkv = MOMENTUM * moment_qkv + approx_qkv
    new_moment_out = MOMENTUM * moment_out + approx_out
    new_moment_gate_up = MOMENTUM * moment_gate_up + approx_gate_up
    new_moment_down = MOMENTUM * moment_down + approx_down
    new_moment_norm = MOMENTUM * moment_norm + lax.optimization_barrier(jnp.sum(grad_norm, 0)) / REPLICAS
    new_moment_inner = MOMENTUM * moment_inner + lax.optimization_barrier(jnp.sum(grad_inner, 0)) / REPLICAS
    total_squares = lax.optimization_barrier(jnp.sum(squares, 0))
    branch_rms = jnp.sqrt(total_squares / (SLOTS * IMAGES * D))
    return (join(outputs), join(grad_inputs), factor_left, factor_qkv, factor_out, factor_gate_up, factor_down, full_qkv - approx_qkv[None], full_out - approx_out[None], full_gate_up - approx_gate_up[None], full_down - approx_down[None], new_moment_qkv, new_moment_out, new_moment_gate_up, new_moment_down, new_moment_norm, new_moment_inner, w_qkv - STEP_RATE * new_moment_qkv, w_out - STEP_RATE * new_moment_out, w_gate_up - STEP_RATE * new_moment_gate_up, w_down - STEP_RATE * new_moment_down, norm_pack - STEP_RATE * new_moment_norm, inner_pack - STEP_RATE * new_moment_inner, branch_rms)
```

```python
import functools

import jax
import jax.numpy as jnp
from jax import lax
from jax.experimental import pallas as pl
from jax.experimental.pallas import tpu as pltpu
from jax.sharding import PartitionSpec as P

DH = 64
FF = 1024
GRID = 32
RANK = 8


EPSILON = 1e-06
MOMENTUM = 0.9
STEP_RATE = 0.5
MESH = pl.DeviceIdType.MESH
BF = jnp.bfloat16
F32 = jnp.float32


def norm_parts(values, gain, bias):
    centre = values - jnp.mean(values, -1, keepdims=True)
    spread = jnp.mean(centre * centre, -1, keepdims=True)
    inverse = lax.rsqrt(spread + EPSILON)
    normed = centre * inverse
    return (normed * gain + bias, normed, inverse)


def norm_back(grad, normed, inverse, gain):
    scaled = grad * gain
    return inverse * (
        scaled
        - jnp.mean(scaled, -1, keepdims=True)
        - normed * jnp.mean(scaled * normed, -1, keepdims=True)
    )


def rope_tables(first_slot, count):
    slot_ids = first_slot + jnp.arange(count, dtype=jnp.int32)
    inside = jnp.logical_and(slot_ids >= 1, slot_ids <= GRID * GRID)
    patch = jnp.where(inside, slot_ids - 1, 0)
    row_pos = (patch // GRID).astype(jnp.float32)
    col_pos = (patch % GRID).astype(jnp.float32)
    quarter = DH // 4
    freqs = 10000.0 ** (-jnp.arange(quarter, dtype=jnp.float32) / quarter)
    angles = jnp.concatenate([row_pos[:, None] * freqs, col_pos[:, None] * freqs], -1) * (
        16.0 / GRID
    )
    return (jnp.cos(angles), jnp.sin(angles))


def rotate(heads, cosine_table, sine_table):
    quarter = heads.shape[-1] // 4
    first = jnp.concatenate([heads[..., :quarter], heads[..., 2 * quarter : 3 * quarter]], -1)
    second = jnp.concatenate([heads[..., quarter : 2 * quarter], heads[..., 3 * quarter :]], -1)
    cosine = cosine_table[:, None, None, :]
    sine = sine_table[:, None, None, :]
    new_first = first * cosine - second * sine
    new_second = second * cosine + first * sine
    return jnp.concatenate(
        [
            new_first[..., :quarter],
            new_second[..., :quarter],
            new_first[..., quarter:],
            new_second[..., quarter:],
        ],
        -1,
    )


def split(value):
    high = value.astype(BF)
    return high, (value - high.astype(F32)).astype(BF)


def dot(left, right, dims):
    return lax.dot_general(left, right, (dims, ((), ())), preferred_element_type=F32)


NN = ((1,), (0,))
NT = ((1,), (1,))
TN = ((0,), (0,))


def fine_dot(left, right, dims):
    left_high, left_low = split(left)
    right_high, right_low = split(right)
    return (
        dot(left_high, right_high, dims)
        + dot(left_high, right_low, dims)
        + dot(left_low, right_high, dims)
    )


def gram_schmidt(stack):
    rows = lax.broadcasted_iota(jnp.int32, (1, RANK, 1), 1)
    for index in range(RANK):
        column = stack[:, index : index + 1, :]
        products = jnp.sum(stack * column, -1, keepdims=True)
        scale = lax.rsqrt(products[:, index : index + 1, :] + EPSILON)
        done = column * scale
        rest = stack - (products * scale) * done
        stack = jnp.where(rows < index, stack, jnp.where(rows == index, done, rest))
    return stack


def exchange(axis, size, buffers, sends, receives):
    me = lax.axis_index(axis)
    copies = []
    for step in range(1, size):
        peer = lax.rem(me + step, size)
        for number, buffer in enumerate(buffers):
            copy = pltpu.make_async_remote_copy(
                src_ref=buffer.at[me],
                dst_ref=buffer.at[me],
                send_sem=sends.at[number, step],
                recv_sem=receives.at[number, step],
                device_id={axis: peer},
                device_id_type=MESH,
            )
            copy.start()
            copies.append(copy)
    for copy in copies:
        copy.wait()


def total(buffer, size):
    value = buffer[0]
    for index in range(1, size):
        value = value + buffer[index]
    return value


def greet(axes, barrier):
    count = 0
    for axis, size in axes:
        me = lax.axis_index(axis)
        for step in range(1, size):
            pl.semaphore_signal(
                barrier, inc=1, device_id={axis: lax.rem(me + step, size)}, device_id_type=MESH
            )
            count += 1
    pl.semaphore_wait(barrier, count)


def factor_kernel(sizes, *refs):
    (
        full_qkv, full_out, full_gate_up, full_down,
        basis_qkv, basis_out, basis_gate_up, basis_down, extra, inner,
        left_cols, left_cols_fine, left_rows_fine, extra_sum, narrow_cols, narrow_rows_fine, out_cols_fine,
        wide_cols, wide_rows_fine, down_cols_fine, inner_sum,
        sum_t, sum_s, sum_d, narrow_s, narrow_d, wide_s, wide_d,
        send_t, recv_t, send_s, recv_s, send_d, recv_d, send_ns, recv_ns, send_nd, recv_nd,
    ) = refs
    nd, ns, nt = sizes
    greet((("tensor", nt), ("seq", ns), ("dp", nd)), pltpu.get_barrier_semaphore())
    me_t, me_s, me_d = (lax.axis_index(axis) for axis in ("tensor", "seq", "dp"))
    own = sum_t.at[me_t]
    bases = [jnp.transpose(basis_qkv[index]) for index in range(3)]
    own[0:8] = sum(fine_dot(bases[index], full_qkv[index], NT) for index in range(3))
    own[8:16] = fine_dot(jnp.transpose(basis_out[...]), full_out[...], NN)
    for index in range(2):
        own[16 + 8 * index : 24 + 8 * index] = fine_dot(
            jnp.transpose(basis_gate_up[index]), full_gate_up[index], NT
        )
    own[32:40] = fine_dot(jnp.transpose(basis_down[...]), full_down[...], NN)
    own[40:48] = extra[...]
    exchange("tensor", nt, (sum_t,), send_t, recv_t)
    sum_s[me_s] = total(sum_t, nt)
    exchange("seq", ns, (sum_s,), send_s, recv_s)
    sum_d[me_d] = total(sum_s, ns)
    exchange("dp", nd, (sum_d,), send_d, recv_d)
    summed = total(sum_d, nd)
    share = 1.0 / (ns * nd)
    extra_sum[0:4] = summed[40:44] * share
    extra_sum[4:8] = summed[44:48]
    left = gram_schmidt(summed[0:40].reshape(5, RANK, summed.shape[-1]))
    for index in range(5):
        left_cols[index] = jnp.transpose(left[index])
        high, low = split(left[index])
        triple = jnp.concatenate([high.astype(F32), high.astype(F32), low.astype(F32)], 0)
        left_rows_fine[index] = triple.astype(BF)
        left_cols_fine[index] = jnp.transpose(triple).astype(BF)
    for index in range(3):
        narrow_s[me_s, 8 * index : 8 * index + 8] = fine_dot(left[0], full_qkv[index], NN)
    narrow_s[me_s, 24:32] = fine_dot(left[1], full_out[...], NT)
    for index in range(2):
        wide_s[me_s, 8 * index : 8 * index + 8] = fine_dot(left[2 + index], full_gate_up[index], NN)
    wide_s[me_s, 16:24] = fine_dot(left[4], full_down[...], NT)
    wide_s[me_s, 24:32] = inner[...]
    exchange("seq", ns, (narrow_s, wide_s), send_ns, recv_ns)
    narrow_d[me_d] = total(narrow_s, ns)
    wide_d[me_d] = total(wide_s, ns)
    exchange("dp", nd, (narrow_d, wide_d), send_nd, recv_nd)
    narrow = total(narrow_d, nd) * share
    wide = total(wide_d, nd) * share
    inner_sum[...] = wide[24:32]

    def triple_of(rows):
        high, low = split(rows)
        return jnp.concatenate([high.astype(F32), low.astype(F32), high.astype(F32)], 0)

    for index in range(4):
        part = narrow[8 * index : 8 * index + 8]
        narrow_cols[index] = jnp.transpose(part)
        if index < 3:
            narrow_rows_fine[index] = triple_of(part).astype(BF)
        else:
            out_cols_fine[...] = jnp.transpose(triple_of(part)).astype(BF)
    for index in range(3):
        part = wide[8 * index : 8 * index + 8]
        wide_cols[index] = jnp.transpose(part)
        if index < 2:
            wide_rows_fine[index] = triple_of(part).astype(BF)
        else:
            down_cols_fine[...] = jnp.transpose(triple_of(part)).astype(BF)


def factors(mesh_sizes, fulls, bases, extra, inner):
    nd, ns, nt = mesh_sizes
    _, width, narrow = fulls[0].shape
    wide = fulls[2].shape[-1]
    shape = jax.ShapeDtypeStruct
    outs = (
        shape((5, width, RANK), F32),
        shape((5, width, 3 * RANK), BF),
        shape((5, 3 * RANK, width), BF),
        shape((8, width), F32),
        shape((4, narrow, RANK), F32),
        shape((3, 3 * RANK, narrow), BF),
        shape((narrow, 3 * RANK), BF),
        shape((3, wide, RANK), F32),
        shape((2, 3 * RANK, wide), BF),
        shape((wide, 3 * RANK), BF),
        shape((8, wide), F32),
    )
    sems = []
    for count, size in ((1, nt), (1, ns), (1, nd), (2, ns), (2, nd)):
        sems += [pltpu.SemaphoreType.DMA((count, size))] * 2
    vmem = pl.BlockSpec(memory_space=pltpu.VMEM)
    return pl.pallas_call(
        functools.partial(factor_kernel, mesh_sizes),
        out_shape=outs,
        in_specs=[vmem] * 10,
        out_specs=[vmem] * len(outs),
        scratch_shapes=[
            pltpu.VMEM((nt, 48, width), F32),
            pltpu.VMEM((ns, 48, width), F32),
            pltpu.VMEM((nd, 48, width), F32),
            pltpu.VMEM((ns, 32, narrow), F32),
            pltpu.VMEM((nd, 32, narrow), F32),
            pltpu.VMEM((ns, 32, wide), F32),
            pltpu.VMEM((nd, 32, wide), F32),
            *sems,
        ],
        compiler_params=pltpu.CompilerParams(
            collective_id=0, has_side_effects=True, vmem_limit_bytes=48 * 2**20
        ),
        name="factors",
    )(*fulls, *bases, extra, inner)


def update_kernel(*refs):
    (
        full_qkv, full_out, full_gate_up, full_down,
        moment_qkv, moment_out, moment_gate_up, moment_down,
        w_qkv, w_out, w_gate_up, w_down,
        left_cols, left_cols_fine, left_rows_fine, extra_sum, narrow_cols, narrow_rows_fine, out_cols_fine,
        wide_cols, wide_rows_fine, down_cols_fine, inner_sum,
        norm_pack, moment_norm, inner_pack, moment_inner,
        factor_left, factor_qkv, factor_out, factor_gate_up, factor_down,
        error_qkv, error_out, error_gate_up, error_down,
        new_moment_qkv, new_moment_out, new_moment_gate_up, new_moment_down, new_moment_norm, new_moment_inner,
        new_w_qkv, new_w_out, new_w_gate_up, new_w_down, new_norm_pack, new_inner_pack,
    ) = refs

    def put(approx, full, moment, weight, error, new_moment, new_weight):
        error[...] = full[...] - approx
        fresh = MOMENTUM * moment[...] + approx
        new_moment[...] = fresh
        new_weight[...] = weight[...] - STEP_RATE * fresh

    for index in range(3):
        put(
            dot(left_cols_fine[0], narrow_rows_fine[index], NN),
            *(ref.at[index] for ref in (full_qkv, moment_qkv, w_qkv, error_qkv, new_moment_qkv, new_w_qkv)),
        )
    put(
        dot(out_cols_fine[...], left_rows_fine[1], NN),
        full_out, moment_out, w_out, error_out, new_moment_out, new_w_out,
    )
    for index in range(2):
        put(
            dot(left_cols_fine[2 + index], wide_rows_fine[index], NN),
            *(ref.at[index] for ref in (full_gate_up, moment_gate_up, w_gate_up, error_gate_up, new_moment_gate_up, new_w_gate_up)),
        )
    put(
        dot(down_cols_fine[...], left_rows_fine[4], NN),
        full_down, moment_down, w_down, error_down, new_moment_down, new_w_down,
    )

    @pl.when(pl.program_id(0) == 0)
    def _():
        factor_left[...] = left_cols[...]
        factor_qkv[...] = narrow_cols[0:3]
        factor_out[...] = narrow_cols[3]
        factor_gate_up[...] = wide_cols[0:2]
        factor_down[...] = wide_cols[2]
        fresh = MOMENTUM * moment_norm[...] + extra_sum[0:4]
        new_moment_norm[...] = fresh
        new_norm_pack[...] = norm_pack[...] - STEP_RATE * fresh
        fresh = MOMENTUM * moment_inner[...] + inner_sum[0:2]
        new_moment_inner[...] = fresh
        new_inner_pack[...] = inner_pack[...] - STEP_RATE * fresh


def update(fulls, moments, weights, parts, norms):
    steps = 4
    _, width, narrow = fulls[0].shape
    wide = fulls[2].shape[-1]
    part = width // steps

    def whole(array):
        zeros = (0,) * array.ndim
        return pl.BlockSpec(array.shape, lambda step, zeros=zeros: zeros)

    matrices = [
        pl.BlockSpec((3, part, narrow), lambda step: (0, step, 0)),
        pl.BlockSpec((narrow // steps, width), lambda step: (step, 0)),
        pl.BlockSpec((2, part, wide), lambda step: (0, step, 0)),
        pl.BlockSpec((wide // steps, width), lambda step: (step, 0)),
    ]
    specs = [whole(array) for array in parts]
    specs[1] = pl.BlockSpec((5, part, 3 * RANK), lambda step: (0, step, 0))
    specs[6] = pl.BlockSpec((narrow // steps, 3 * RANK), lambda step: (step, 0))
    specs[9] = pl.BlockSpec((wide // steps, 3 * RANK), lambda step: (step, 0))
    shape = jax.ShapeDtypeStruct
    small = [
        shape((5, width, RANK), F32),
        shape((3, narrow, RANK), F32),
        shape((narrow, RANK), F32),
        shape((2, wide, RANK), F32),
        shape((wide, RANK), F32),
    ]
    like = [shape(array.shape, F32) for array in fulls]
    norm, inner = shape((4, width), F32), shape((2, wide), F32)
    return pl.pallas_call(
        update_kernel,
        grid=(steps,),
        out_shape=[*small, *like, *like, norm, inner, *like, norm, inner],
        in_specs=[*matrices * 3, *specs, *(whole(array) for array in norms)],
        out_specs=[
            *(whole(array) for array in small),
            *matrices * 2,
            whole(norm),
            whole(inner),
            *matrices,
            whole(norm),
            whole(inner),
        ],
        compiler_params=pltpu.CompilerParams(vmem_limit_bytes=48 * 2**20),
        name="update",
    )(*fulls, *moments, *weights, *parts, *norms)


def per_device(
    tokens,
    out_grad,
    keep_mask,
    w_qkv,
    w_out,
    w_gate_up,
    w_down,
    norm_pack,
    inner_pack,
    moment_qkv,
    moment_out,
    moment_gate_up,
    moment_down,
    moment_norm,
    moment_inner,
    error_qkv,
    error_out,
    error_gate_up,
    error_down,
    basis_qkv,
    basis_out,
    basis_gate_up,
    basis_down,
):
    own_rows, images, width = tokens.shape
    seq_rows = out_grad.shape[0]
    slot_count = keep_mask.shape[0]
    local_width = w_out.shape[0]
    local_heads = local_width // DH
    head_shape = (seq_rows, images, local_heads, DH)
    block_start = lax.axis_index("seq") * seq_rows
    own_start = lax.axis_index("tensor") * own_rows
    score_scale = DH ** (-0.5)
    grad_scale = (images * seq_rows) ** (-0.5)
    key_ok = (jnp.transpose(keep_mask) > 0)[:, None, None, :]
    block_mask = lax.dynamic_slice_in_dim(keep_mask.astype(jnp.float32), block_start, seq_rows, 0)
    cotangent = out_grad * block_mask[:, :, None]
    cotangent_own = lax.dynamic_slice_in_dim(cotangent, own_start, own_rows, 0)
    qkv_low = w_qkv.astype(jnp.bfloat16)
    out_low = w_out.astype(jnp.bfloat16)
    gate_up_low = w_gate_up.astype(jnp.bfloat16)
    down_low = w_down.astype(jnp.bfloat16)
    inputs = tokens.astype(jnp.float32)
    normed_one, hat_one, inverse_one = norm_parts(inputs, norm_pack[0], norm_pack[1])
    rows_one = lax.all_gather(normed_one.astype(jnp.bfloat16), "tensor", axis=0, tiled=True)
    projected = jnp.einsum("tbd,jde->jtbe", rows_one, qkv_low, preferred_element_type=jnp.float32)
    cosine_table, sine_table = rope_tables(block_start, seq_rows)
    queries = rotate(projected[0].reshape(head_shape), cosine_table, sine_table).astype(
        jnp.bfloat16
    )
    keys_own = rotate(projected[1].reshape(head_shape), cosine_table, sine_table).astype(
        jnp.bfloat16
    )
    values_own = projected[2].astype(jnp.bfloat16)
    keys_flat, values_flat = (
        lax.all_gather(keys_own.reshape(seq_rows, images, local_width), "seq", axis=0, tiled=True),
        lax.all_gather(values_own, "seq", axis=0, tiled=True),
    )
    keys_all = keys_flat.reshape(slot_count, images, local_heads, DH)
    values_all = values_flat.reshape(slot_count, images, local_heads, DH)
    scores = (
        jnp.einsum("qbhd,kbhd->bhqk", queries, keys_all, preferred_element_type=jnp.float32)
        * score_scale
    )
    scores = jnp.where(key_ok, scores, -1e30)
    row_max = jnp.max(scores, -1, keepdims=True)
    exponent = jnp.exp(scores - row_max)
    row_total = jnp.sum(exponent, -1, keepdims=True)
    attn_probs = exponent / row_total
    log_total = row_max + jnp.log(row_total)
    attended = jnp.einsum(
        "bhqk,kbhd->qbhd",
        attn_probs.astype(jnp.bfloat16),
        values_all,
        preferred_element_type=jnp.float32,
    )
    attended = attended.astype(jnp.bfloat16).reshape(seq_rows, images, local_width)
    rows = attended
    branch_one = lax.psum_scatter(
        jnp.einsum("tbh,he->tbe", rows, out_low, preferred_element_type=jnp.float32),
        "tensor",
        scatter_dimension=0,
        tiled=True,
    )
    middle = inputs + branch_one
    normed_two, hat_two, inverse_two = norm_parts(middle, norm_pack[2], norm_pack[3])
    rows_two = lax.all_gather(normed_two.astype(jnp.bfloat16), "tensor", axis=0, tiled=True)
    gate_up = jnp.einsum("tbd,jdf->jtbf", rows_two, gate_up_low, preferred_element_type=jnp.float32)
    gate = gate_up[0]
    upward = gate_up[1]
    sigmoid = 1.0 / (1.0 + jnp.exp(-gate))
    hidden = gate * sigmoid * upward
    sum_first, sum_second = lax.psum(
        (jnp.sum(hidden, -1, keepdims=True), jnp.sum(hidden * hidden, -1, keepdims=True)), "tensor"
    )
    hidden_mean = sum_first / FF
    inverse_three = lax.rsqrt(sum_second / FF - hidden_mean * hidden_mean + EPSILON)
    hat_three = (hidden - hidden_mean) * inverse_three
    normed_three = (hat_three * inner_pack[0] + inner_pack[1]).astype(jnp.bfloat16)
    rows = normed_three
    branch_two = lax.psum_scatter(
        jnp.einsum("tbf,fe->tbe", rows, down_low, preferred_element_type=jnp.float32),
        "tensor",
        scatter_dimension=0,
        tiled=True,
    )
    residual = middle + branch_two
    grad_branch = cotangent.astype(jnp.bfloat16)
    grad_down = jnp.einsum(
        "tbf,tbe->fe", normed_three, grad_branch, preferred_element_type=jnp.float32
    )
    grad_normed = jnp.einsum(
        "tbe,fe->tbf", grad_branch, down_low, preferred_element_type=jnp.float32
    )
    grad_inner = jnp.stack([jnp.sum(grad_normed * hat_three, (0, 1)), jnp.sum(grad_normed, (0, 1))])
    grad_scaled = grad_normed * inner_pack[0]
    back_first, back_second = lax.psum(
        (
            jnp.sum(grad_scaled, -1, keepdims=True),
            jnp.sum(grad_scaled * hat_three, -1, keepdims=True),
        ),
        "tensor",
    )
    grad_hidden = inverse_three * (grad_scaled - back_first / FF - hat_three * back_second / FF)
    grad_gate = grad_hidden * upward * (sigmoid + gate * sigmoid * (1.0 - sigmoid))
    grad_up = grad_hidden * gate * sigmoid
    grad_gate_up_rows = jnp.stack([grad_gate, grad_up]).astype(jnp.bfloat16)
    grad_gate_up = jnp.einsum(
        "tbd,jtbf->jdf", rows_two, grad_gate_up_rows, preferred_element_type=jnp.float32
    )
    rows = grad_gate_up_rows
    grad_two = lax.psum_scatter(
        jnp.einsum("jtbf,jdf->tbd", rows, gate_up_low, preferred_element_type=jnp.float32),
        "tensor",
        scatter_dimension=0,
        tiled=True,
    )
    grad_middle = cotangent_own + norm_back(grad_two, hat_two, inverse_two, norm_pack[2])
    grad_middle_rows = lax.all_gather(
        grad_middle.astype(jnp.bfloat16), "tensor", axis=0, tiled=True
    )
    grad_out = jnp.einsum(
        "tbh,tbe->he", attended, grad_middle_rows, preferred_element_type=jnp.float32
    )
    grad_attended = jnp.einsum(
        "tbe,he->tbh", grad_middle_rows, out_low, preferred_element_type=jnp.float32
    )
    grad_attended = grad_attended.astype(jnp.bfloat16).reshape(head_shape)
    again = (
        jnp.einsum("qbhd,kbhd->bhqk", queries, keys_all, preferred_element_type=jnp.float32)
        * score_scale
    )
    again = jnp.where(key_ok, again, -1e30)
    probs_again = jnp.exp(again - log_total)
    probs_low = probs_again.astype(jnp.bfloat16)
    grad_probs = jnp.einsum(
        "qbhd,kbhd->bhqk", grad_attended, values_all, preferred_element_type=jnp.float32
    )
    row_delta = jnp.sum(probs_again * grad_probs, -1, keepdims=True)
    grad_scores = (probs_again * (grad_probs - row_delta)).astype(jnp.bfloat16)
    grad_queries = (
        jnp.einsum("bhqk,kbhd->qbhd", grad_scores, keys_all, preferred_element_type=jnp.float32)
        * score_scale
    )
    key_part = (
        jnp.einsum("bhqk,qbhd->kbhd", grad_scores, queries, preferred_element_type=jnp.float32)
        * score_scale
    )
    value_part = jnp.einsum(
        "bhqk,qbhd->kbhd", probs_low, grad_attended, preferred_element_type=jnp.float32
    )
    key_grads = lax.psum_scatter(
        jnp.concatenate(
            [
                key_part.reshape(seq_rows * lax.axis_size("seq"), images, local_width),
                value_part.reshape(seq_rows * lax.axis_size("seq"), images, local_width),
            ],
            -1,
        ),
        "seq",
        scatter_dimension=0,
        tiled=True,
    )
    grad_keys = key_grads[..., :local_width].reshape(head_shape)
    grad_values = key_grads[..., local_width:]
    grad_query_raw = rotate(grad_queries, cosine_table, -sine_table).reshape(
        seq_rows, images, local_width
    )
    grad_key_raw = rotate(grad_keys, cosine_table, -sine_table).reshape(
        seq_rows, images, local_width
    )
    grad_projected = jnp.stack([grad_query_raw, grad_key_raw, grad_values]).astype(jnp.bfloat16)
    grad_qkv = jnp.einsum(
        "tbd,jtbe->jde", rows_one, grad_projected, preferred_element_type=jnp.float32
    )
    rows = grad_projected
    grad_one = lax.psum_scatter(
        jnp.einsum("jtbe,jde->tbd", rows, qkv_low, preferred_element_type=jnp.float32),
        "tensor",
        scatter_dimension=0,
        tiled=True,
    )
    input_grad = grad_middle + norm_back(grad_one, hat_one, inverse_one, norm_pack[0])
    full_qkv = grad_qkv * grad_scale + error_qkv[0]
    full_out = grad_out * grad_scale + error_out[0]
    full_gate_up = grad_gate_up * grad_scale + error_gate_up[0]
    full_down = grad_down * grad_scale + error_down[0]
    grad_norm = (
        jnp.stack(
            [
                jnp.sum(grad_one * hat_one, (0, 1)),
                jnp.sum(grad_one, (0, 1)),
                jnp.sum(grad_two * hat_two, (0, 1)),
                jnp.sum(grad_two, (0, 1)),
            ]
        )
        * grad_scale
    )
    squares = jnp.stack([jnp.sum(branch_one * branch_one), jnp.sum(branch_two * branch_two)])
    extra = jnp.concatenate(
        [grad_norm, jnp.pad(squares[None], ((0, 3), (0, width - 2)))], 0
    )
    inner = jnp.pad(grad_inner * grad_scale, ((0, 6), (0, 0)))
    sizes = tuple(lax.axis_size(axis) for axis in ("dp", "seq", "tensor"))
    fulls = (full_qkv, full_out, full_gate_up, full_down)
    parts = factors(sizes, fulls, (basis_qkv, basis_out, basis_gate_up, basis_down), extra, inner)
    (
        factor_left, factor_qkv, factor_out, factor_gate_up, factor_down,
        error_qkv, error_out, error_gate_up, error_down,
        *rest,
    ) = update(
        fulls,
        (moment_qkv, moment_out, moment_gate_up, moment_down),
        (w_qkv, w_out, w_gate_up, w_down),
        parts,
        (norm_pack, moment_norm, inner_pack, moment_inner),
    )
    branch_rms = jnp.sqrt(parts[3][4, :2] / (slot_count * images * lax.axis_size("dp") * width))
    return (
        residual, input_grad,
        factor_left, factor_qkv, factor_out, factor_gate_up, factor_down,
        error_qkv[None], error_out[None], error_gate_up[None], error_down[None],
        *rest,
        branch_rms,
    )


def solution(mesh):
    placed = (
        P(("seq", "tensor"), "dp", None),
        P("seq", "dp", None),
        P(None, "dp"),
        P(None, None, "tensor"),
        P("tensor", None),
        P(None, None, "tensor"),
        P("tensor", None),
        P(),
        P(None, "tensor"),
        P(None, None, "tensor"),
        P("tensor", None),
        P(None, None, "tensor"),
        P("tensor", None),
        P(),
        P(None, "tensor"),
        P(("dp", "seq"), None, None, "tensor"),
        P(("dp", "seq"), "tensor", None),
        P(("dp", "seq"), None, None, "tensor"),
        P(("dp", "seq"), "tensor", None),
        P(None, "tensor", None),
        P("tensor", None),
        P(None, "tensor", None),
        P("tensor", None),
    )
    return jax.shard_map(
        per_device,
        mesh=mesh,
        in_specs=placed,
        out_specs=(
            P(("seq", "tensor"), "dp", None),
            P(("seq", "tensor"), "dp", None),
            P(),
            P(None, "tensor", None),
            P("tensor", None),
            P(None, "tensor", None),
            P("tensor", None),
            P(("dp", "seq"), None, None, "tensor"),
            P(("dp", "seq"), "tensor", None),
            P(("dp", "seq"), None, None, "tensor"),
            P(("dp", "seq"), "tensor", None),
            P(None, None, "tensor"),
            P("tensor", None),
            P(None, None, "tensor"),
            P("tensor", None),
            P(),
            P(None, "tensor"),
            P(None, None, "tensor"),
            P("tensor", None),
            P(None, None, "tensor"),
            P("tensor", None),
            P(),
            P(None, "tensor"),
            P(),
        ),
        check_vma=False,
    )
```

```python
import functools

import jax
import jax.numpy as jnp
from jax import lax
from jax.experimental import pallas as pl
from jax.experimental.pallas import tpu as pltpu
from jax.sharding import PartitionSpec as P

DH = 64
FF = 1024
GRID = 32
RANK = 8
QUARTER = DH // 4
CHUNK = 16


EPSILON = 1e-06
MOMENTUM = 0.9
STEP_RATE = 0.5
MESH = pl.DeviceIdType.MESH
BF = jnp.bfloat16
F32 = jnp.float32


def split(value):
    high = value.astype(BF)
    return high, (value - high.astype(F32)).astype(BF)


def dot(left, right, dims):
    return lax.dot_general(left, right, (dims, ((), ())), preferred_element_type=F32)


NN = ((1,), (0,))
NT = ((1,), (1,))
TN = ((0,), (0,))


def fine_dot(left, right, dims):
    left_high, left_low = split(left)
    right_high, right_low = split(right)
    return (
        dot(left_high, right_high, dims)
        + dot(left_high, right_low, dims)
        + dot(left_low, right_high, dims)
    )


def gram_schmidt(stack):
    rows = lax.broadcasted_iota(jnp.int32, (1, RANK, 1), 1)
    for index in range(RANK):
        column = stack[:, index : index + 1, :]
        products = jnp.sum(stack * column, -1, keepdims=True)
        scale = lax.rsqrt(products[:, index : index + 1, :] + EPSILON)
        done = column * scale
        rest = stack - (products * scale) * done
        stack = jnp.where(rows < index, stack, jnp.where(rows == index, done, rest))
    return stack


def exchange(axis, size, buffers, sends, receives):
    me = lax.axis_index(axis)
    copies = []
    for step in range(1, size):
        peer = lax.rem(me + step, size)
        for number, buffer in enumerate(buffers):
            copy = pltpu.make_async_remote_copy(
                src_ref=buffer.at[me],
                dst_ref=buffer.at[me],
                send_sem=sends.at[number, step],
                recv_sem=receives.at[number, step],
                device_id={axis: peer},
                device_id_type=MESH,
            )
            copy.start()
            copies.append(copy)
    for copy in copies:
        copy.wait()


def total(buffer, size):
    value = buffer[0]
    for index in range(1, size):
        value = value + buffer[index]
    return value


def greet(axes, barrier):
    count = 0
    for axis, size in axes:
        me = lax.axis_index(axis)
        for step in range(1, size):
            pl.semaphore_signal(
                barrier, inc=1, device_id={axis: lax.rem(me + step, size)}, device_id_type=MESH
            )
            count += 1
    pl.semaphore_wait(barrier, count)


def factor_kernel(sizes, *refs):
    (
        full_qkv, full_out, full_gate_up, full_down,
        basis_qkv, basis_out, basis_gate_up, basis_down, extra, inner,
        left_rows, left_rows_fine, left_cols_fine, extra_sum,
        narrow_rows, narrow_cols_fine, wide_rows, wide_rows_fine, down_cols_fine, inner_sum,
        sum_t, sum_s, sum_d, narrow_s, narrow_d, wide_s, wide_d,
        send_t, recv_t, send_s, recv_s, send_d, recv_d, send_ns, recv_ns, send_nd, recv_nd,
    ) = refs
    nd, ns, nt = sizes
    greet((("tensor", nt), ("seq", ns), ("dp", nd)), pltpu.get_barrier_semaphore())
    me_t, me_s, me_d = (lax.axis_index(axis) for axis in ("tensor", "seq", "dp"))
    own = sum_t.at[me_t]
    own[0:8] = sum(fine_dot(basis_qkv[index], full_qkv[index], NN) for index in range(3))
    own[8:16] = fine_dot(basis_out[...], full_out[...], NN)
    for index in range(2):
        own[16 + 8 * index : 24 + 8 * index] = fine_dot(
            basis_gate_up[index], full_gate_up[index], NT
        )
    own[32:40] = fine_dot(basis_down[...], full_down[...], NN)
    own[40:48] = extra[...]
    exchange("tensor", nt, (sum_t,), send_t, recv_t)
    sum_s[me_s] = total(sum_t, nt)
    exchange("seq", ns, (sum_s,), send_s, recv_s)
    sum_d[me_d] = total(sum_s, ns)
    exchange("dp", nd, (sum_d,), send_d, recv_d)
    summed = total(sum_d, nd)
    share = 1.0 / (ns * nd)
    extra_sum[0:4] = summed[40:44] * share
    extra_sum[4:8] = summed[44:48]
    left = gram_schmidt(summed[0:40].reshape(5, RANK, summed.shape[-1]))
    for index in range(5):
        left_rows[index] = left[index]
        high, low = split(left[index])
        triple = jnp.concatenate([high.astype(F32), high.astype(F32), low.astype(F32)], 0)
        left_rows_fine[index] = triple.astype(BF)
        if index in (2, 3):
            left_cols_fine[index - 2] = jnp.transpose(triple).astype(BF)
    for index in range(3):
        narrow_s[me_s, 8 * index : 8 * index + 8] = fine_dot(left[0], full_qkv[index], NT)
    narrow_s[me_s, 24:32] = fine_dot(left[1], full_out[...], NT)
    for index in range(2):
        wide_s[me_s, 8 * index : 8 * index + 8] = fine_dot(left[2 + index], full_gate_up[index], NN)
    wide_s[me_s, 16:24] = fine_dot(left[4], full_down[...], NT)
    wide_s[me_s, 24:32] = inner[...]
    exchange("seq", ns, (narrow_s, wide_s), send_ns, recv_ns)
    narrow_d[me_d] = total(narrow_s, ns)
    wide_d[me_d] = total(wide_s, ns)
    exchange("dp", nd, (narrow_d, wide_d), send_nd, recv_nd)
    narrow = total(narrow_d, nd) * share
    wide = total(wide_d, nd) * share
    inner_sum[...] = wide[24:32]

    def triple_of(rows):
        high, low = split(rows)
        return jnp.concatenate([high.astype(F32), low.astype(F32), high.astype(F32)], 0)

    for index in range(4):
        part = narrow[8 * index : 8 * index + 8]
        narrow_rows[index] = part
        narrow_cols_fine[index] = jnp.transpose(triple_of(part)).astype(BF)
    for index in range(3):
        part = wide[8 * index : 8 * index + 8]
        wide_rows[index] = part
        if index < 2:
            wide_rows_fine[index] = triple_of(part).astype(BF)
        else:
            down_cols_fine[...] = jnp.transpose(triple_of(part)).astype(BF)


def factors(mesh_sizes, fulls, bases, extra, inner):
    nd, ns, nt = mesh_sizes
    _, narrow, width = fulls[0].shape
    wide = fulls[2].shape[-1]
    shape = jax.ShapeDtypeStruct
    outs = (
        shape((5, RANK, width), F32),
        shape((5, 3 * RANK, width), BF),
        shape((2, width, 3 * RANK), BF),
        shape((8, width), F32),
        shape((4, RANK, narrow), F32),
        shape((4, narrow, 3 * RANK), BF),
        shape((3, RANK, wide), F32),
        shape((2, 3 * RANK, wide), BF),
        shape((wide, 3 * RANK), BF),
        shape((8, wide), F32),
    )
    sems = []
    for count, size in ((1, nt), (1, ns), (1, nd), (2, ns), (2, nd)):
        sems += [pltpu.SemaphoreType.DMA((count, size))] * 2
    vmem = pl.BlockSpec(memory_space=pltpu.VMEM)
    return pl.pallas_call(
        functools.partial(factor_kernel, mesh_sizes),
        out_shape=outs,
        in_specs=[vmem] * 10,
        out_specs=[vmem] * len(outs),
        scratch_shapes=[
            pltpu.VMEM((nt, 48, width), F32),
            pltpu.VMEM((ns, 48, width), F32),
            pltpu.VMEM((nd, 48, width), F32),
            pltpu.VMEM((ns, 32, narrow), F32),
            pltpu.VMEM((nd, 32, narrow), F32),
            pltpu.VMEM((ns, 32, wide), F32),
            pltpu.VMEM((nd, 32, wide), F32),
            *sems,
        ],
        compiler_params=pltpu.CompilerParams(
            collective_id=0, has_side_effects=True, vmem_limit_bytes=24 * 2**20
        ),
        name="factors",
    )(*fulls, *bases, extra, inner)


def update_kernel(*refs):
    (
        full_qkv, full_out, full_gate_up, full_down,
        moment_qkv, moment_out, moment_gate_up, moment_down,
        w_qkv, w_out, w_gate_up, w_down,
        left_rows, left_rows_fine, left_cols_fine, extra_sum,
        narrow_rows, narrow_cols_fine, wide_rows, wide_rows_fine, down_cols_fine, inner_sum,
        norm_pack, moment_norm, inner_pack, moment_inner,
        factor_left, factor_qkv, factor_out, factor_gate_up, factor_down,
        error_qkv, error_out, error_gate_up, error_down,
        new_moment_qkv, new_moment_out, new_moment_gate_up, new_moment_down, new_moment_norm, new_moment_inner,
        new_w_qkv, new_w_out, new_w_gate_up, new_w_down, new_norm_pack, new_inner_pack,
    ) = refs

    def put(approx, full, moment, weight, error, new_moment, new_weight):
        error[...] = full[...] - approx
        fresh = MOMENTUM * moment[...] + approx
        new_moment[...] = fresh
        new_weight[...] = weight[...] - STEP_RATE * fresh

    for index in range(3):
        put(
            dot(narrow_cols_fine[index], left_rows_fine[0], NN),
            *(ref.at[index] for ref in (full_qkv, moment_qkv, w_qkv, error_qkv, new_moment_qkv, new_w_qkv)),
        )
    put(
        dot(narrow_cols_fine[3], left_rows_fine[1], NN),
        full_out, moment_out, w_out, error_out, new_moment_out, new_w_out,
    )
    for index in range(2):
        put(
            dot(left_cols_fine[index], wide_rows_fine[index], NN),
            *(ref.at[index] for ref in (full_gate_up, moment_gate_up, w_gate_up, error_gate_up, new_moment_gate_up, new_w_gate_up)),
        )
    put(
        dot(down_cols_fine[...], left_rows_fine[4], NN),
        full_down, moment_down, w_down, error_down, new_moment_down, new_w_down,
    )

    @pl.when(pl.program_id(0) == 0)
    def _():
        factor_left[...] = left_rows[...]
        factor_qkv[...] = narrow_rows[0:3]
        factor_out[...] = narrow_rows[3]
        factor_gate_up[...] = wide_rows[0:2]
        factor_down[...] = wide_rows[2]
        fresh = MOMENTUM * moment_norm[...] + extra_sum[0:4]
        new_moment_norm[...] = fresh
        new_norm_pack[...] = norm_pack[...] - STEP_RATE * fresh
        fresh = MOMENTUM * moment_inner[...] + inner_sum[0:2]
        new_moment_inner[...] = fresh
        new_inner_pack[...] = inner_pack[...] - STEP_RATE * fresh


def update(fulls, moments, weights, parts, norms):
    steps = 4
    _, narrow, width = fulls[0].shape
    wide = fulls[2].shape[-1]
    part = width // steps

    def whole(array):
        zeros = (0,) * array.ndim
        return pl.BlockSpec(array.shape, lambda step, zeros=zeros: zeros)

    matrices = [
        pl.BlockSpec((3, narrow // steps, width), lambda step: (0, step, 0)),
        pl.BlockSpec((narrow // steps, width), lambda step: (step, 0)),
        pl.BlockSpec((2, part, wide), lambda step: (0, step, 0)),
        pl.BlockSpec((wide // steps, width), lambda step: (step, 0)),
    ]
    specs = [whole(array) for array in parts]
    specs[2] = pl.BlockSpec((2, part, 3 * RANK), lambda step: (0, step, 0))
    specs[5] = pl.BlockSpec((4, narrow // steps, 3 * RANK), lambda step: (0, step, 0))
    specs[8] = pl.BlockSpec((wide // steps, 3 * RANK), lambda step: (step, 0))
    shape = jax.ShapeDtypeStruct
    small = [
        shape((5, RANK, width), F32),
        shape((3, RANK, narrow), F32),
        shape((RANK, narrow), F32),
        shape((2, RANK, wide), F32),
        shape((RANK, wide), F32),
    ]
    like = [shape(array.shape, F32) for array in fulls]
    norm, inner = shape((4, width), F32), shape((2, wide), F32)
    return pl.pallas_call(
        update_kernel,
        grid=(steps,),
        out_shape=[*small, *like, *like, norm, inner, *like, norm, inner],
        in_specs=[*matrices * 3, *specs, *(whole(array) for array in norms)],
        out_specs=[
            *(whole(array) for array in small),
            *matrices * 2,
            whole(norm),
            whole(inner),
            *matrices,
            whole(norm),
            whole(inner),
        ],
        compiler_params=pltpu.CompilerParams(vmem_limit_bytes=48 * 2**20),
        name="update",
    )(*fulls, *moments, *weights, *parts, *norms)


def swap_quarters(value):
    lane = lax.broadcasted_iota(jnp.int32, (1, 128), 1)
    low = lax.rem(lax.div(lane, QUARTER), 2) == 0
    tiles = []
    for start in range(0, value.shape[-1], 128):
        tile = value[:, start : start + 128]
        tiles.append(
            jnp.where(low, pltpu.roll(tile, 128 - QUARTER, 1), pltpu.roll(tile, QUARTER, 1))
        )
    return jnp.concatenate(tiles, -1)


def norm_parts(values, gain, bias):
    centre = values - jnp.mean(values, -1, keepdims=True)
    spread = jnp.mean(centre * centre, -1, keepdims=True)
    inverse = lax.rsqrt(spread + EPSILON)
    normed = centre * inverse
    return (normed * gain + bias, normed, inverse)


def norm_back(grad, normed, inverse, gain):
    scaled = grad * gain
    return inverse * (
        scaled
        - jnp.mean(scaled, -1, keepdims=True)
        - normed * jnp.mean(scaled * normed, -1, keepdims=True)
    )


def column_sums(value):
    return jnp.sum(value, 0, keepdims=True)


def block_kernel(sizes, images, *refs):
    (
        tokens, keep, mask, cosine, sine, norm_pack, inner_pack, w_qkv,
        w_out_hbm, w_gate_up_hbm, w_down_hbm, out_grad_hbm,
        error_qkv_hbm, error_out_hbm, error_gate_up_hbm, error_down_hbm,
        residual, input_grad, full_qkv, full_out, full_gate_up, full_down, extra, inner,
        normed_one, normed_one_all, keys_values, queries, probs, scores, grad_scores,
        attended, attended_low, attended_in, attended_send,
        out_low, gate_up_low, down_low, inner_all, query_low, key_value_low,
        normed_two, grad_middle_low, grad_middle, normed_three, grad_gate, grad_up,
        normed_three_send, grad_gate_send, grad_up_send,
        grad_attended, grad_attended_send, grad_attended_all, grad_query, grad_query_low, grad_pairs,
        pairs_send, pairs_recv, grad_one, grad_one_recv, sum_query, sum_pairs, inner_sums, inner_recv,
        w_out, w_gate_up, w_down, out_grad, error_qkv, error_out, error_gate_up, error_down,
        local_sems, one_send, one_recv, weight_send, weight_recv, pair_send, pair_recv,
        att_send, att_recv, datt_send, datt_recv, rows_send, rows_recv, back_send, back_recv,
        final_send, final_recv,
    ) = refs
    nd, ns, nt = sizes
    me_t, me_s = lax.axis_index("tensor"), lax.axis_index("seq")
    other = 1 - me_t
    own, width = tokens.shape[1], tokens.shape[2]
    seq_rows = 2 * own
    slots = ns * seq_rows
    heads = w_qkv.shape[1] // DH
    hidden_all = 2 * w_down.shape[0]
    scale = (images * seq_rows) ** (-0.5)
    own_rows = pl.ds(pl.multiple_of(me_t * own, 8), own)
    other_rows = pl.ds(pl.multiple_of(other * own, 8), own)

    loads = [
        pltpu.make_async_copy(source, target, local_sems.at[number])
        for number, (source, target) in enumerate(
            (
                (w_out_hbm, w_out), (w_gate_up_hbm, w_gate_up), (w_down_hbm, w_down), (out_grad_hbm, out_grad),
                (error_qkv_hbm, error_qkv), (error_out_hbm, error_out),
                (error_gate_up_hbm, error_gate_up), (error_down_hbm, error_down),
            )
        )
    ]
    for load in loads:
        load.start()

    def to_partner(source, target, send, receive):
        return pltpu.make_async_remote_copy(
            src_ref=source, dst_ref=target, send_sem=send, recv_sem=receive,
            device_id={"tensor": other}, device_id_type=MESH,
        )

    def to_seq(source, target, send, receive, step):
        return pltpu.make_async_remote_copy(
            src_ref=source, dst_ref=target, send_sem=send, recv_sem=receive,
            device_id={"seq": lax.rem(me_s + step, ns)}, device_id_type=MESH,
        )

    def one_copy(image):
        block = normed_one.at[me_t, image]
        return to_partner(block, block, one_send.at[image], one_recv.at[image])

    def weight_copies():
        return [
            to_partner(ref.at[me_t], ref.at[me_t], weight_send.at[number], weight_recv.at[number])
            for number, ref in enumerate((out_low, gate_up_low, down_low, inner_all))
        ]

    def pair_copies(image):
        block = keys_values.at[image, me_s]
        return [
            to_seq(block, block, pair_send.at[image, step], pair_recv.at[image, step], step)
            for step in range(1, ns)
        ]

    def att_copy(image):
        return to_partner(
            attended_send.at[image], attended_in.at[me_t, image], att_send.at[image], att_recv.at[image]
        )

    def datt_copy(image):
        return to_partner(
            grad_attended_send.at[image], grad_attended.at[me_t, image], datt_send.at[image], datt_recv.at[image]
        )

    def row_copies(image):
        moves = (
            (normed_two.at[me_t, image], normed_two),
            (grad_middle_low.at[me_t, image], grad_middle_low),
            (normed_three_send.at[image], normed_three),
            (grad_gate_send.at[image], grad_gate),
            (grad_up_send.at[image], grad_up),
        )
        return [
            to_partner(source, target.at[me_t, image], rows_send.at[image, number], rows_recv.at[image, number])
            for number, (source, target) in enumerate(moves)
        ]

    def back_copies(image):
        return [
            to_seq(
                pairs_send.at[image, lax.rem(me_s + step, ns)], pairs_recv.at[image, step],
                back_send.at[image, step], back_recv.at[image, step], step,
            )
            for step in range(1, ns)
        ]

    def final_copy(image):
        return to_partner(
            grad_one.at[image, other_rows], grad_one_recv.at[image], final_send.at[image], final_recv.at[image]
        )

    def inner_copy():
        return to_partner(
            inner_sums.at[other], inner_recv, final_send.at[images], final_recv.at[images]
        )

    gain_one, bias_one = norm_pack[0:1], norm_pack[1:2]
    gain_two, bias_two = norm_pack[2:3], norm_pack[3:4]

    for image in range(images):
        normed, _, _ = norm_parts(tokens[image].astype(F32), gain_one, bias_one)
        normed_one[me_t, image] = normed.astype(BF)
    greet((("tensor", nt), ("seq", ns)), pltpu.get_barrier_semaphore())
    for image in range(images):
        one_copy(image).start()

    narrow = heads * DH
    pad = jnp.zeros((256 - narrow, width), BF)
    query_low[...] = jnp.concatenate([w_qkv[0].astype(BF), pad], 0)
    key_value_low[0:narrow] = w_qkv[1].astype(BF)
    key_value_low[narrow : 2 * narrow] = w_qkv[2].astype(BF)

    def project(image, carry):
        one_copy(image).wait_recv()
        blocks = [normed_one[half, image] for half in range(2)]
        pairs = jnp.concatenate([dot(block, key_value_low[...], NT) for block in blocks], 0)
        pairs = pairs * cosine[...] + swap_quarters(pairs) * sine[...]
        keys_values[image, me_s] = pairs.astype(BF)
        for copy in pair_copies(image):
            copy.start()
        raw = jnp.concatenate([dot(block, query_low[...], NT) for block in blocks], 0)
        raw = raw * cosine[:, 0:256] + swap_quarters(raw) * sine[:, 0:256]
        raw = raw * (DH ** (-0.5))
        lane = lax.broadcasted_iota(jnp.int32, (1, 128), 1)
        for head in range(heads):
            tile = raw[:, head // 2 * 128 : head // 2 * 128 + 128]
            queries[image * heads + head] = jnp.where(lax.div(lane, DH) == head % 2, tile, 0.0).astype(BF)
        normed_one_all[image] = jnp.concatenate([block.astype(F32) for block in blocks], 0).astype(BF)
        return carry

    lax.fori_loop(0, images, project, 0)

    for load in loads[0:3]:
        load.wait()
    out_low[me_t] = jnp.concatenate([pad, w_out[...].astype(BF)], 0)
    for index in range(2):
        gate_up_low[me_t, index] = w_gate_up[index].astype(BF)
    down_low[me_t] = w_down[...].astype(BF)
    inner_all[me_t] = jnp.zeros_like(inner_all[me_t])
    inner_all[me_t, 0:2] = inner_pack[...]
    for copy in weight_copies():
        copy.start()
    loads[3].wait()
    extra[...] = jnp.zeros_like(extra)
    inner_sums[...] = jnp.zeros_like(inner_sums)

    def half_mask(half):
        lane = lax.broadcasted_iota(jnp.int32, (1, 128), 1)
        return lax.div(lane, DH) == half

    def tile_of(index):
        return pl.ds(pl.multiple_of(index * 128, 128), 128)

    def key_tile(image, index):
        return keys_values[image, :, :, tile_of(index)].reshape(slots, 128)

    def attend(image):
        for copy in pair_copies(image):
            copy.wait_recv()
        bias = jnp.where(keep[pl.ds(image, 1), :] > 0, 0.0, -1e30)
        attended[...] = jnp.zeros_like(attended)

        def head_step(head, carry):
            scores[...] = dot(queries[image * heads + head], key_tile(image, lax.div(head, 2)), NT)
            for start in range(0, seq_rows, CHUNK):
                rows = slice(start, start + CHUNK)
                part = scores[rows] + bias
                part = jnp.exp(part - jnp.max(part, -1, keepdims=True))
                part = part * (1.0 / jnp.sum(part, -1, keepdims=True))
                probs[image * heads + head, rows] = part.astype(BF)
            place = lax.div(head + 1, 2)
            mixed = dot(probs[image * heads + head], key_tile(image, place + 1), NN)
            attended[:, tile_of(place)] += jnp.where(half_mask(lax.rem(head + 1, 2)), mixed, 0.0)
            return carry

        lax.fori_loop(0, heads, head_step, 0)
        attended_low[image] = attended[...].astype(BF)
        attended_in[me_t, image] = attended[own_rows].astype(BF)
        attended_send[image] = attended[other_rows].astype(BF)
        att_copy(image).start()

    def feed(image):
        att_copy(image).wait_recv()
        inputs = tokens[image].astype(F32)
        branch = sum(dot(attended_in[half, image], out_low[half], NN) for half in range(2))
        middle = inputs + branch
        extra[4:5] += column_sums(branch * branch)
        normed, hat_two, inverse_two = norm_parts(middle, gain_two, bias_two)
        rows_two = normed.astype(BF)
        normed_two[me_t, image] = rows_two
        halves = (me_t, other)
        gates = [dot(rows_two, gate_up_low[half, 0], NN) for half in halves]
        ups = [dot(rows_two, gate_up_low[half, 1], NN) for half in halves]
        sigmoids = [1.0 / (1.0 + jnp.exp(-gate)) for gate in gates]
        hiddens = [gate * sigmoid * up for gate, sigmoid, up in zip(gates, sigmoids, ups)]
        mean = sum(jnp.sum(hidden, -1, keepdims=True) for hidden in hiddens) / hidden_all
        centres = [hidden - mean for hidden in hiddens]
        spread = sum(jnp.sum(centre * centre, -1, keepdims=True) for centre in centres) / hidden_all
        inverse_three = lax.rsqrt(spread + EPSILON)
        hats = [centre * inverse_three for centre in centres]
        lows = [
            (hat * inner_all[half, 0:1] + inner_all[half, 1:2]).astype(BF)
            for hat, half in zip(hats, halves)
        ]
        branch = sum(dot(low, down_low[half], NN) for low, half in zip(lows, halves))
        extra[5:6] += column_sums(branch * branch)
        residual[image] = middle + branch
        cotangent = out_grad[image, own_rows] * mask[image, own_rows]
        grad_branch = cotangent.astype(BF)
        grads = [dot(grad_branch, down_low[half], NT) for half in halves]
        for half, grad, hat in zip(halves, grads, hats):
            inner_sums[half, 0:1] += column_sums(grad * hat)
            inner_sums[half, 1:2] += column_sums(grad)
        scaled = [grad * inner_all[half, 0:1] for grad, half in zip(grads, halves)]
        first = sum(jnp.sum(value, -1, keepdims=True) for value in scaled) / hidden_all
        second = (
            sum(jnp.sum(value * hat, -1, keepdims=True) for value, hat in zip(scaled, hats)) / hidden_all
        )
        grad_hiddens = [
            inverse_three * (value - first - hat * second) for value, hat in zip(scaled, hats)
        ]
        gate_rows = [
            (grad * up * (sigmoid + gate * sigmoid * (1.0 - sigmoid))).astype(BF)
            for grad, up, sigmoid, gate in zip(grad_hiddens, ups, sigmoids, gates)
        ]
        up_rows = [
            (grad * gate * sigmoid).astype(BF)
            for grad, gate, sigmoid in zip(grad_hiddens, gates, sigmoids)
        ]
        normed_three[me_t, image] = lows[0]
        normed_three_send[image] = lows[1]
        grad_gate[me_t, image] = gate_rows[0]
        grad_gate_send[image] = gate_rows[1]
        grad_up[me_t, image] = up_rows[0]
        grad_up_send[image] = up_rows[1]
        grad_two = sum(
            dot(gate_row, gate_up_low[half, 0], NT) + dot(up_row, gate_up_low[half, 1], NT)
            for gate_row, up_row, half in zip(gate_rows, up_rows, halves)
        )
        extra[2:3] += column_sums(grad_two * hat_two)
        extra[3:4] += column_sums(grad_two)
        back = cotangent + norm_back(grad_two, hat_two, inverse_two, gain_two)
        grad_middle[image] = back
        low = back.astype(BF)
        grad_middle_low[me_t, image] = low
        grad_attended[me_t, image] = dot(low, out_low[me_t], NT).astype(BF)
        grad_attended_send[image] = dot(low, out_low[other], NT).astype(BF)
        datt_copy(image).start()
        for copy in row_copies(image):
            copy.start()

    def attend_back(image):
        datt_copy(image).wait_recv()
        grad_attended_all[...] = jnp.concatenate(
            [grad_attended[half, image].astype(F32) for half in range(2)], 0
        )
        grad_query[...] = jnp.zeros_like(grad_query)
        grad_pairs[...] = jnp.zeros_like(grad_pairs)

        def head_step(head, carry):
            place = lax.div(head + 1, 2)
            at_key, at_value = lax.div(head, 2), place + 1
            key_half, value_half = half_mask(lax.rem(head, 2)), half_mask(lax.rem(head + 1, 2))
            wide = jnp.where(value_half, grad_attended_all[:, tile_of(place)], 0.0)
            low = wide.astype(BF)
            scores[...] = dot(low, key_tile(image, at_value), NT)
            delta = jnp.sum(wide * attended_low[image, :, tile_of(place)].astype(F32), -1, keepdims=True)
            for start in range(0, seq_rows, CHUNK):
                rows = slice(start, start + CHUNK)
                chance = probs[image * heads + head, rows].astype(F32)
                grad_scores[rows] = (chance * (scores[rows] - delta[rows])).astype(BF)
            grad_query[:, tile_of(at_key)] += jnp.where(
                key_half, dot(grad_scores[...], key_tile(image, at_key), NN), 0.0
            )
            query_t = jnp.transpose(queries[image * heads + head].astype(F32)).astype(BF)
            grad_pairs[tile_of(at_key)] += dot(query_t, grad_scores[...], NN)
            grad_pairs[tile_of(at_value)] += dot(
                jnp.transpose(wide).astype(BF), probs[image * heads + head], NN
            )
            return carry

        lax.fori_loop(0, heads, head_step, 0)
        pairs = jnp.transpose(grad_pairs[...])
        pairs_send[image] = pairs.astype(BF).reshape(ns, seq_rows, width)
        for copy in back_copies(image):
            copy.start()
        raw = grad_query[...] * (DH ** (-0.5))
        raw = raw * cosine[:, 0:256] - swap_quarters(raw) * sine[:, 0:256]
        grad_query_low[image] = raw.astype(BF)

    def stage(step, carry):
        @pl.when(step < images)
        def _():
            attend(step)

        @pl.when(step >= 1)
        def _():
            attend_back(step - 1)

        @pl.when(step == 0)
        def _():
            for copy in weight_copies():
                copy.wait_recv()

        @pl.when(step < images)
        def _():
            feed(step)

        return carry

    lax.fori_loop(0, images + 1, stage, 0)
    inner_copy().start()

    full_out[...] = jnp.zeros_like(full_out)
    full_gate_up[...] = jnp.zeros_like(full_gate_up)
    full_down[...] = jnp.zeros_like(full_down)

    def weights(image, carry):
        for copy in row_copies(image):
            copy.wait_recv()
        for half in range(2):
            place = slice(half * own, half * own + own)
            grad_branch = (out_grad[image, place] * mask[image, place]).astype(BF)
            full_down[...] += dot(normed_three[half, image], grad_branch, TN)
            rows_two = normed_two[half, image]
            full_gate_up[0] += dot(rows_two, grad_gate[half, image], TN)
            full_gate_up[1] += dot(rows_two, grad_up[half, image], TN)
            mixed = attended_low[image].astype(F32)[place].astype(BF)
            full_out[...] += dot(mixed, grad_middle_low[half, image], TN)[256 - narrow :]
        return carry

    lax.fori_loop(0, images, weights, 0)
    for load in loads[4:8]:
        load.wait()
    full_out[...] = full_out[...] * scale + error_out[...]
    full_gate_up[...] = full_gate_up[...] * scale + error_gate_up[...]
    full_down[...] = full_down[...] * scale + error_down[...]

    sum_query[...] = jnp.zeros_like(sum_query)
    sum_pairs[...] = jnp.zeros_like(sum_pairs)

    def finish_pairs(image, carry):
        for copy in back_copies(image):
            copy.wait_recv()
        pairs = pairs_send[image, me_s].astype(F32)
        for step in range(1, ns):
            pairs = pairs + pairs_recv[image, step].astype(F32)
        pairs = pairs * cosine[...] - swap_quarters(pairs) * sine[...]
        pairs = pairs.astype(BF)
        query = grad_query_low[image]
        grad_one[image] = dot(query, query_low[...], NN) + dot(pairs, key_value_low[...], NN)
        final_copy(image).start()
        sum_query[...] += dot(query, normed_one_all[image], TN)
        sum_pairs[...] += dot(pairs, normed_one_all[image], TN)
        return carry

    lax.fori_loop(0, images, finish_pairs, 0)
    full_qkv[0] = sum_query[0:narrow] * scale + error_qkv[0]
    full_qkv[1] = sum_pairs[0:narrow] * scale + error_qkv[1]
    full_qkv[2] = sum_pairs[narrow : 2 * narrow] * scale + error_qkv[2]

    def finish(image, carry):
        final_copy(image).wait_recv()
        grad = grad_one[image, own_rows] + grad_one_recv[image]
        _, hat_one, inverse_one = norm_parts(tokens[image].astype(F32), gain_one, bias_one)
        input_grad[image] = grad_middle[image] + norm_back(grad, hat_one, inverse_one, gain_one)
        extra[0:1] += column_sums(grad * hat_one)
        extra[1:2] += column_sums(grad)
        return carry

    lax.fori_loop(0, images, finish, 0)
    extra[0:4] = extra[0:4] * scale
    inner_copy().wait_recv()
    inner[...] = (inner_sums[me_t] + inner_recv[...]) * scale

    for image in range(images):
        for copy in (
            one_copy(image), *pair_copies(image), att_copy(image), datt_copy(image),
            *row_copies(image), *back_copies(image), final_copy(image),
        ):
            copy.wait_send()
    for copy in (*weight_copies(), inner_copy()):
        copy.wait_send()


def block(mesh_sizes, tokens, keep, mask, cosine, sine, norm_pack, inner_pack, w_qkv, hbm):
    nd, ns, nt = mesh_sizes
    images, own, width = tokens.shape
    seq_rows = 2 * own
    slots = ns * seq_rows
    narrow = w_qkv.shape[1]
    heads = narrow // DH
    wide = inner_pack.shape[1]
    shape = jax.ShapeDtypeStruct
    outs = (
        shape((images, own, width), F32),
        shape((images, own, width), F32),
        shape((3, narrow, width), F32),
        shape((narrow, width), F32),
        shape((2, width, wide), F32),
        shape((wide, width), F32),
        shape((8, width), F32),
        shape((8, wide), F32),
    )
    vmem = pl.BlockSpec(memory_space=pltpu.VMEM)
    hbm_spec = pl.BlockSpec(memory_space=pl.ANY)
    dma = pltpu.SemaphoreType.DMA
    scratch = [
        pltpu.VMEM((2, images, own, width), BF),
        pltpu.VMEM((images, seq_rows, width), BF),
        pltpu.VMEM((images, ns, seq_rows, width), BF),
        pltpu.VMEM((images * heads, seq_rows, 128), BF),
        pltpu.VMEM((images * heads, seq_rows, slots), BF),
        pltpu.VMEM((seq_rows, slots), F32),
        pltpu.VMEM((seq_rows, slots), BF),
        pltpu.VMEM((seq_rows, 256), F32),
        pltpu.VMEM((images, seq_rows, 256), BF),
        pltpu.VMEM((2, images, own, 256), BF),
        pltpu.VMEM((images, own, 256), BF),
        pltpu.VMEM((2, 256, width), BF),
        pltpu.VMEM((2, 2, width, wide), BF),
        pltpu.VMEM((2, wide, width), BF),
        pltpu.VMEM((2, 8, wide), F32),
        pltpu.VMEM((256, width), BF),
        pltpu.VMEM((2 * narrow, width), BF),
        pltpu.VMEM((2, images, own, width), BF),
        pltpu.VMEM((2, images, own, width), BF),
        pltpu.VMEM((images, own, width), F32),
        *[pltpu.VMEM((2, images, own, wide), BF)] * 3,
        *[pltpu.VMEM((images, own, wide), BF)] * 3,
        pltpu.VMEM((2, images, own, 256), BF),
        pltpu.VMEM((images, own, 256), BF),
        pltpu.VMEM((seq_rows, 256), F32),
        pltpu.VMEM((seq_rows, 256), F32),
        pltpu.VMEM((images, seq_rows, 256), BF),
        pltpu.VMEM((width, slots), F32),
        pltpu.VMEM((images, ns, seq_rows, width), BF),
        pltpu.VMEM((images, ns, seq_rows, width), BF),
        pltpu.VMEM((images, seq_rows, width), F32),
        pltpu.VMEM((images, own, width), F32),
        pltpu.VMEM((256, width), F32),
        pltpu.VMEM((2 * narrow, width), F32),
        pltpu.VMEM((2, 8, wide), F32),
        pltpu.VMEM((8, wide), F32),
        *[pltpu.VMEM(array.shape, F32) for array in hbm],
        dma((8,)),
        *[dma((images,))] * 2,
        *[dma((4,))] * 2,
        *[dma((images, ns))] * 2,
        *[dma((images,))] * 4,
        *[dma((images, 5))] * 2,
        *[dma((images, ns))] * 2,
        *[dma((images + 1,))] * 2,
    ]
    return pl.pallas_call(
        functools.partial(block_kernel, mesh_sizes, images),
        out_shape=outs,
        in_specs=[vmem] * 8 + [hbm_spec] * len(hbm),
        out_specs=[vmem] * len(outs),
        scratch_shapes=scratch,
        compiler_params=pltpu.CompilerParams(
            collective_id=1, has_side_effects=True, vmem_limit_bytes=62 * 2**20
        ),
        name="block",
    )(tokens, keep, mask, cosine, sine, norm_pack, inner_pack, w_qkv, *hbm)


def rope_tables(first_slot, count):
    slot_ids = first_slot + jnp.arange(count, dtype=jnp.int32)
    inside = jnp.logical_and(slot_ids >= 1, slot_ids <= GRID * GRID)
    patch = jnp.where(inside, slot_ids - 1, 0)
    row_pos = (patch // GRID).astype(jnp.float32)
    col_pos = (patch % GRID).astype(jnp.float32)
    quarter = DH // 4
    freqs = 10000.0 ** (-jnp.arange(quarter, dtype=jnp.float32) / quarter)
    angles = jnp.concatenate([row_pos[:, None] * freqs, col_pos[:, None] * freqs], -1) * (
        16.0 / GRID
    )
    return (jnp.cos(angles), jnp.sin(angles))


def quarter_lanes(first, second, narrow, rest):
    pairs = jnp.stack(
        [first[:, :QUARTER], second[:, :QUARTER], first[:, QUARTER:], second[:, QUARTER:]], 1
    )
    head = pairs.reshape(first.shape[0], DH)
    keys = jnp.tile(head, (1, narrow // DH))
    return jnp.concatenate([keys, jnp.full_like(keys, rest)], -1)


def per_device(
    tokens,
    out_grad,
    keep_mask,
    w_qkv,
    w_out,
    w_gate_up,
    w_down,
    norm_pack,
    inner_pack,
    moment_qkv,
    moment_out,
    moment_gate_up,
    moment_down,
    moment_norm,
    moment_inner,
    error_qkv,
    error_out,
    error_gate_up,
    error_down,
    basis_qkv,
    basis_out,
    basis_gate_up,
    basis_down,
):
    own_rows, images, width = tokens.shape
    seq_rows = out_grad.shape[0]
    slot_count = keep_mask.shape[0]
    narrow = w_out.shape[0]
    sizes = tuple(lax.axis_size(axis) for axis in ("dp", "seq", "tensor"))
    block_start = lax.axis_index("seq") * seq_rows
    mask = lax.dynamic_slice_in_dim(keep_mask, block_start, seq_rows, 0)
    mask = jnp.transpose(mask).astype(F32)[:, :, None]
    cosine_table, sine_table = rope_tables(block_start, seq_rows)
    cosine = quarter_lanes(cosine_table, cosine_table, narrow, 1.0)
    sine = quarter_lanes(-sine_table, sine_table, narrow, 0.0)

    def turn(array):
        return jnp.swapaxes(array, -1, -2)

    residual, input_grad, *fulls, extra, inner = block(
        sizes,
        jnp.swapaxes(tokens, 0, 1), jnp.transpose(keep_mask), mask, cosine, sine, norm_pack, inner_pack, turn(w_qkv),
        (
            w_out, w_gate_up, w_down, jnp.swapaxes(out_grad, 0, 1),
            turn(error_qkv[0]), error_out[0], error_gate_up[0], error_down[0],
        ),
    )
    bases = tuple(turn(basis) for basis in (basis_qkv, basis_out, basis_gate_up, basis_down))
    parts = factors(sizes, fulls, bases, extra, inner)
    (
        factor_left, factor_qkv, factor_out, factor_gate_up, factor_down,
        new_error_qkv, new_error_out, new_error_gate_up, new_error_down,
        new_moment_qkv, new_moment_out, new_moment_gate_up, new_moment_down, new_moment_norm, new_moment_inner,
        new_w_qkv, new_w_out, new_w_gate_up, new_w_down, new_norm_pack, new_inner_pack,
    ) = update(
        fulls,
        (turn(moment_qkv), moment_out, moment_gate_up, moment_down),
        (turn(w_qkv), w_out, w_gate_up, w_down),
        parts,
        (norm_pack, moment_norm, inner_pack, moment_inner),
    )
    squares = jnp.sum(parts[3][4:6], -1)
    branch_rms = jnp.sqrt(squares / (slot_count * images * lax.axis_size("dp") * width))
    return (
        jnp.swapaxes(residual, 0, 1), jnp.swapaxes(input_grad, 0, 1),
        *(turn(factor) for factor in (factor_left, factor_qkv, factor_out, factor_gate_up, factor_down)),
        turn(new_error_qkv)[None], new_error_out[None], new_error_gate_up[None], new_error_down[None],
        turn(new_moment_qkv), new_moment_out, new_moment_gate_up, new_moment_down, new_moment_norm, new_moment_inner,
        turn(new_w_qkv), new_w_out, new_w_gate_up, new_w_down, new_norm_pack, new_inner_pack,
        branch_rms,
    )


def solution(mesh):
    placed = (
        P(("seq", "tensor"), "dp", None),
        P("seq", "dp", None),
        P(None, "dp"),
        P(None, None, "tensor"),
        P("tensor", None),
        P(None, None, "tensor"),
        P("tensor", None),
        P(),
        P(None, "tensor"),
        P(None, None, "tensor"),
        P("tensor", None),
        P(None, None, "tensor"),
        P("tensor", None),
        P(),
        P(None, "tensor"),
        P(("dp", "seq"), None, None, "tensor"),
        P(("dp", "seq"), "tensor", None),
        P(("dp", "seq"), None, None, "tensor"),
        P(("dp", "seq"), "tensor", None),
        P(None, "tensor", None),
        P("tensor", None),
        P(None, "tensor", None),
        P("tensor", None),
    )
    return jax.shard_map(
        per_device,
        mesh=mesh,
        in_specs=placed,
        out_specs=(
            P(("seq", "tensor"), "dp", None),
            P(("seq", "tensor"), "dp", None),
            P(),
            P(None, "tensor", None),
            P("tensor", None),
            P(None, "tensor", None),
            P("tensor", None),
            P(("dp", "seq"), None, None, "tensor"),
            P(("dp", "seq"), "tensor", None),
            P(("dp", "seq"), None, None, "tensor"),
            P(("dp", "seq"), "tensor", None),
            P(None, None, "tensor"),
            P("tensor", None),
            P(None, None, "tensor"),
            P("tensor", None),
            P(),
            P(None, "tensor"),
            P(None, None, "tensor"),
            P("tensor", None),
            P(None, None, "tensor"),
            P("tensor", None),
            P(),
            P(None, "tensor"),
            P(),
        ),
        check_vma=False,
    )
```

```python
import functools
import math

import jax
import jax.numpy as jnp
from jax import lax
from jax.experimental import pallas as pl
from jax.experimental.pallas import tpu as pltpu
from jax.sharding import PartitionSpec as P

DH = 64
FF = 1024
GRID = 32
RANK = 8
QUARTER = DH // 4
CHUNK = 16
LIMIT = 62


EPSILON = 1e-06
MOMENTUM = 0.9
STEP_RATE = 0.5
MESH = pl.DeviceIdType.MESH
BF = jnp.bfloat16
F32 = jnp.float32


def split(value):
    high = value.astype(BF)
    return high, (value - high.astype(F32)).astype(BF)


def dot(left, right, dims):
    return lax.dot_general(left, right, (dims, ((), ())), preferred_element_type=F32)


NN = ((1,), (0,))
NT = ((1,), (1,))
TN = ((0,), (0,))


def fine_dot(left, right, dims):
    left_high, left_low = split(left)
    right_high, right_low = split(right)
    return (
        dot(left_high, right_high, dims)
        + dot(left_high, right_low, dims)
        + dot(left_low, right_high, dims)
    )


def gram_schmidt(stack):
    rows = lax.broadcasted_iota(jnp.int32, (1, RANK, 1), 1)
    for index in range(RANK):
        column = stack[:, index : index + 1, :]
        products = jnp.sum(stack * column, -1, keepdims=True)
        scale = lax.rsqrt(products[:, index : index + 1, :] + EPSILON)
        done = column * scale
        rest = stack - (products * scale) * done
        stack = jnp.where(rows < index, stack, jnp.where(rows == index, done, rest))
    return stack


def exchange(axis, size, buffers, sends, receives):
    me = lax.axis_index(axis)
    copies = []
    for step in range(1, size):
        peer = lax.rem(me + step, size)
        for number, buffer in enumerate(buffers):
            copy = pltpu.make_async_remote_copy(
                src_ref=buffer.at[me],
                dst_ref=buffer.at[me],
                send_sem=sends.at[number, step],
                recv_sem=receives.at[number, step],
                device_id={axis: peer},
                device_id_type=MESH,
            )
            copy.start()
            copies.append(copy)
    return copies


def arrive(copies):
    for copy in copies:
        copy.wait()


def total(buffer, size):
    value = buffer[0]
    for index in range(1, size):
        value = value + buffer[index]
    return value


def greet(axes, barrier):
    for axis, size in axes:
        me = lax.axis_index(axis)
        for step in range(1, size):
            pl.semaphore_signal(
                barrier, inc=1, device_id={axis: lax.rem(me + step, size)}, device_id_type=MESH
            )


def triple_first(rows):
    high, low = split(rows)
    return jnp.concatenate([high.astype(F32), high.astype(F32), low.astype(F32)], 0)


def triple_second(rows):
    high, low = split(rows)
    return jnp.concatenate([high.astype(F32), low.astype(F32), high.astype(F32)], 0)


def update_kernel(*refs):
    (
        full_qkv, full_out, full_gate_up, full_down,
        moment_qkv, moment_out, moment_gate_up, moment_down,
        w_qkv, w_out, w_gate_up, w_down,
        left_rows, left_rows_fine, left_cols_fine, extra_sum,
        narrow_rows, narrow_cols_fine, wide_rows, wide_rows_fine, down_cols_fine, inner_sum,
        norm_pack, moment_norm, inner_pack, moment_inner,
        factor_left, factor_qkv, factor_out, factor_gate_up, factor_down,
        error_qkv, error_out, error_gate_up, error_down,
        new_moment_qkv, new_moment_out, new_moment_gate_up, new_moment_down, new_moment_norm, new_moment_inner,
        new_w_qkv, new_w_out, new_w_gate_up, new_w_down, new_norm_pack, new_inner_pack,
    ) = refs

    def put(approx, full, moment, weight, error, new_moment, new_weight):
        error[...] = full[...] - approx
        fresh = MOMENTUM * moment[...] + approx
        new_moment[...] = fresh
        new_weight[...] = weight[...] - STEP_RATE * fresh

    for index in range(3):
        put(
            dot(narrow_cols_fine[index], left_rows_fine[0], NN),
            *(ref.at[index] for ref in (full_qkv, moment_qkv, w_qkv, error_qkv, new_moment_qkv, new_w_qkv)),
        )
    put(
        dot(narrow_cols_fine[3], left_rows_fine[1], NN),
        full_out, moment_out, w_out, error_out, new_moment_out, new_w_out,
    )
    for index in range(2):
        put(
            dot(left_cols_fine[index], wide_rows_fine[index], NN),
            *(ref.at[index] for ref in (full_gate_up, moment_gate_up, w_gate_up, error_gate_up, new_moment_gate_up, new_w_gate_up)),
        )
    put(
        dot(down_cols_fine[...], left_rows_fine[4], NN),
        full_down, moment_down, w_down, error_down, new_moment_down, new_w_down,
    )

    @pl.when(pl.program_id(0) == 0)
    def _():
        factor_left[...] = left_rows[...]
        factor_qkv[...] = narrow_rows[0:3]
        factor_out[...] = narrow_rows[3]
        factor_gate_up[...] = wide_rows[0:2]
        factor_down[...] = wide_rows[2]
        fresh = MOMENTUM * moment_norm[...] + extra_sum[0:4]
        new_moment_norm[...] = fresh
        new_norm_pack[...] = norm_pack[...] - STEP_RATE * fresh
        fresh = MOMENTUM * moment_inner[...] + inner_sum[0:2]
        new_moment_inner[...] = fresh
        new_inner_pack[...] = inner_pack[...] - STEP_RATE * fresh


def update(fulls, moments, weights, parts, norms):
    steps = 4
    _, narrow, width = fulls[0].shape
    wide = fulls[2].shape[-1]
    part = width // steps

    def whole(array):
        zeros = (0,) * array.ndim
        return pl.BlockSpec(array.shape, lambda step, zeros=zeros: zeros)

    matrices = [
        pl.BlockSpec((3, narrow // steps, width), lambda step: (0, step, 0)),
        pl.BlockSpec((narrow // steps, width), lambda step: (step, 0)),
        pl.BlockSpec((2, part, wide), lambda step: (0, step, 0)),
        pl.BlockSpec((wide // steps, width), lambda step: (step, 0)),
    ]
    specs = [whole(array) for array in parts]
    specs[2] = pl.BlockSpec((2, part, 3 * RANK), lambda step: (0, step, 0))
    specs[5] = pl.BlockSpec((4, narrow // steps, 3 * RANK), lambda step: (0, step, 0))
    specs[8] = pl.BlockSpec((wide // steps, 3 * RANK), lambda step: (step, 0))
    shape = jax.ShapeDtypeStruct
    small = [
        shape((5, RANK, width), F32),
        shape((3, RANK, narrow), F32),
        shape((RANK, narrow), F32),
        shape((2, RANK, wide), F32),
        shape((RANK, wide), F32),
    ]
    like = [shape(array.shape, F32) for array in fulls]
    norm, inner = shape((4, width), F32), shape((2, wide), F32)
    return pl.pallas_call(
        update_kernel,
        grid=(steps,),
        out_shape=[*small, *like, *like, norm, inner, *like, norm, inner],
        in_specs=[*matrices * 3, *specs, *(whole(array) for array in norms)],
        out_specs=[
            *(whole(array) for array in small),
            *matrices * 2,
            whole(norm),
            whole(inner),
            *matrices,
            whole(norm),
            whole(inner),
        ],
        compiler_params=pltpu.CompilerParams(vmem_limit_bytes=LIMIT * 2**20),
        name="update",
    )(*fulls, *moments, *weights, *parts, *norms)


def swap_quarters(tile):
    lane = lax.broadcasted_iota(jnp.int32, (1, 128), 1)
    low = lax.rem(lax.div(lane, QUARTER), 2) == 0
    return jnp.where(low, pltpu.roll(tile, 128 - QUARTER, 1), pltpu.roll(tile, QUARTER, 1))


def turn_pairs(pairs, cosine, sine):
    keys = lax.broadcasted_iota(jnp.int32, (1, 128), 1) < DH
    first, second, third = (pairs[:, start : start + 128] for start in (0, 128, 256))
    first = first * cosine + swap_quarters(first) * sine
    second = jnp.where(keys, second * cosine + swap_quarters(second) * sine, second)
    return jnp.concatenate([first, second, third], -1)


def turn_queries(raw, cosine, sine):
    tiles = (raw[:, start : start + 128] for start in (0, 128))
    return jnp.concatenate([tile * cosine + swap_quarters(tile) * sine for tile in tiles], -1)


def angle_tables(first_slot, count):
    slots = first_slot + lax.broadcasted_iota(jnp.int32, (count, 128), 0)
    place = lax.rem(lax.broadcasted_iota(jnp.int32, (count, 128), 1), DH)
    inside = jnp.logical_and(slots >= 1, slots <= GRID * GRID)
    patch = jnp.where(inside, slots - 1, 0)
    quarter = lax.div(place, QUARTER)
    position = jnp.where(quarter < 2, lax.div(patch, GRID), lax.rem(patch, GRID)).astype(F32)
    power = lax.rem(place, QUARTER).astype(F32)
    angles = position * jnp.exp(power * (-math.log(10000.0) / QUARTER)) * (16.0 / GRID)
    sine = jnp.sin(angles)
    return jnp.cos(angles), jnp.where(lax.rem(quarter, 2) == 0, -sine, sine)


def norm_parts(values, gain, bias):
    centre = values - jnp.mean(values, -1, keepdims=True)
    spread = jnp.mean(centre * centre, -1, keepdims=True)
    inverse = lax.rsqrt(spread + EPSILON)
    normed = centre * inverse
    return (normed * gain + bias, normed, inverse)


def norm_back(grad, normed, inverse, gain):
    scaled = grad * gain
    return inverse * (
        scaled
        - jnp.mean(scaled, -1, keepdims=True)
        - normed * jnp.mean(scaled * normed, -1, keepdims=True)
    )


def column_sums(value):
    return jnp.sum(value, 0, keepdims=True)


def block_kernel(sizes, images, *refs):
    (
        keep, norm_pack, inner_pack, basis_qkv, basis_out, basis_gate_up, basis_down,
        tokens_hbm, w_qkv_hbm, w_out_hbm, w_gate_up_hbm, w_down_hbm, out_grad_hbm,
        error_qkv_hbm, error_out_hbm, error_gate_up_hbm, error_down_hbm,
        residual, input_grad, full_qkv, full_out, full_gate_up, full_down,
        left_rows, left_rows_fine, left_cols_fine, extra_sum,
        narrow_rows, narrow_cols_fine, wide_rows, wide_rows_fine, down_cols_fine, inner_sum,
        normed_one, normed_one_all, keys_values, queries, probs, scores, grad_scores,
        attended, attended_low, attended_in, attended_send,
        out_low, gate_up_low, down_low, inner_all, query_low, key_value_low,
        normed_two, grad_middle_low, grad_middle, normed_three, grad_gate, grad_up,
        normed_three_send, grad_gate_send, grad_up_send,
        grad_attended, grad_attended_send, grad_attended_all, grad_query, grad_query_low, grad_pairs,
        pairs_send, pairs_recv, grad_one, grad_one_recv, sum_query, sum_pairs, inner_sums, inner_recv,
        tokens, w_qkv, w_out, w_gate_up, w_down, out_grad, mask, cosine, sine, extra, kept_rows,
        early_t, early_d, early_s, late_t, late_s, late_d, norm_t, norm_s, norm_d,
        thin_d, thin_s, broad_d, broad_s, slim_s, slim_d,
        local_sems, one_send, one_recv, weight_send, weight_recv, pair_send, pair_recv,
        att_send, att_recv, datt_send, datt_recv, rows_send, rows_recv, back_send, back_recv,
        final_send, final_recv, low_send, low_recv,
    ) = refs
    nd, ns, nt = sizes
    me_t, me_s = lax.axis_index("tensor"), lax.axis_index("seq")
    other = 1 - me_t
    me_d = lax.axis_index("dp")
    own, width = tokens.shape[1], tokens.shape[2]
    seq_rows = 2 * own
    slots = ns * seq_rows
    heads = w_qkv.shape[1] // DH
    hidden_all = 2 * w_down.shape[0]
    scale = (images * seq_rows) ** (-0.5)
    own_rows = pl.ds(pl.multiple_of(me_t * own, 8), own)
    other_rows = pl.ds(pl.multiple_of(other * own, 8), own)

    barrier = pltpu.get_barrier_semaphore()
    greet((("tensor", nt), ("seq", ns), ("dp", nd)), barrier)
    loads = [
        pltpu.make_async_copy(source, target, local_sems.at[number])
        for number, (source, target) in enumerate(
            (
                (tokens_hbm, tokens), (w_qkv_hbm, w_qkv),
                (w_out_hbm, w_out), (w_gate_up_hbm, w_gate_up), (w_down_hbm, w_down), (out_grad_hbm, out_grad),
                (error_qkv_hbm, full_qkv), (error_out_hbm, full_out),
                (error_gate_up_hbm, full_gate_up), (error_down_hbm, full_down),
            )
        )
    ]
    for load in loads:
        load.start()

    def to_partner(source, target, send, receive):
        return pltpu.make_async_remote_copy(
            src_ref=source, dst_ref=target, send_sem=send, recv_sem=receive,
            device_id={"tensor": other}, device_id_type=MESH,
        )

    def to_seq(source, target, send, receive, step):
        return pltpu.make_async_remote_copy(
            src_ref=source, dst_ref=target, send_sem=send, recv_sem=receive,
            device_id={"seq": lax.rem(me_s + step, ns)}, device_id_type=MESH,
        )

    def one_copy(image):
        block = normed_one.at[me_t, image]
        return to_partner(block, block, one_send.at[image], one_recv.at[image])

    def weight_copies():
        return [
            to_partner(ref.at[me_t], ref.at[me_t], weight_send.at[number], weight_recv.at[number])
            for number, ref in enumerate((out_low, gate_up_low, down_low, inner_all))
        ]

    def pair_copies(image):
        block = keys_values.at[image, me_s]
        return [
            to_seq(block, block, pair_send.at[image, step], pair_recv.at[image, step], step)
            for step in range(1, ns)
        ]

    def att_copy(image):
        return to_partner(
            attended_send.at[image], attended_in.at[me_t, image], att_send.at[image], att_recv.at[image]
        )

    def datt_copy(image):
        return to_partner(
            grad_attended_send.at[image], grad_attended.at[me_t, image], datt_send.at[image], datt_recv.at[image]
        )

    def row_copies(image):
        moves = (
            (normed_two.at[me_t, image], normed_two),
            (grad_middle_low.at[me_t, image], grad_middle_low),
            (normed_three_send.at[image], normed_three),
            (grad_gate_send.at[image], grad_gate),
            (grad_up_send.at[image], grad_up),
        )
        return [
            to_partner(source, target.at[me_t, image], rows_send.at[image, number], rows_recv.at[image, number])
            for number, (source, target) in enumerate(moves)
        ]

    def back_copies(image):
        return [
            to_seq(
                pairs_send.at[image, lax.rem(me_s + step, ns)], pairs_recv.at[image, step],
                back_send.at[image, step], back_recv.at[image, step], step,
            )
            for step in range(1, ns)
        ]

    def final_copy(image):
        return to_partner(
            grad_one.at[image, other_rows], grad_one_recv.at[image], final_send.at[image], final_recv.at[image]
        )

    def inner_copy():
        return to_partner(
            inner_sums.at[other], inner_recv, final_send.at[images], final_recv.at[images]
        )

    gain_one, bias_one = norm_pack[0:1], norm_pack[1:2]
    gain_two, bias_two = norm_pack[2:3], norm_pack[3:4]

    cosine[...], sine[...] = angle_tables(me_s * seq_rows, seq_rows)
    kept = jnp.concatenate([keep[...].astype(F32), jnp.zeros((8 - images, slots), F32)], 0)
    kept_rows[...] = jnp.transpose(kept)
    kept = kept_rows[pl.ds(pl.multiple_of(me_s * seq_rows, 8), seq_rows)]
    for image in range(images):
        mask[image] = kept[:, image : image + 1]
    loads[0].wait()
    for image in range(images):
        normed, _, _ = norm_parts(tokens[image].astype(F32), gain_one, bias_one)
        normed_one[me_t, image] = normed.astype(BF)
    pl.semaphore_wait(barrier, (nt - 1) + (ns - 1) + (nd - 1))
    for image in range(images):
        one_copy(image).start()
    loads[1].wait()

    narrow = heads * DH
    pad = jnp.zeros((256 - narrow, width), BF)
    query_low[...] = jnp.concatenate([w_qkv[0].astype(BF), pad], 0)
    key_value_low[0:narrow] = w_qkv[1].astype(BF)
    key_value_low[narrow : 2 * narrow] = w_qkv[2].astype(BF)

    def project(image, carry):
        one_copy(image).wait_recv()
        blocks = [normed_one[half, image] for half in range(2)]
        pairs = jnp.concatenate([dot(block, key_value_low[...], NT) for block in blocks], 0)
        pairs = turn_pairs(pairs, cosine[...], sine[...])
        keys_values[image, me_s] = pairs.astype(BF)
        for copy in pair_copies(image):
            copy.start()
        raw = jnp.concatenate([dot(block, query_low[...], NT) for block in blocks], 0)
        raw = turn_queries(raw, cosine[...], sine[...]) * (DH ** (-0.5))
        lane = lax.broadcasted_iota(jnp.int32, (1, 128), 1)
        for head in range(heads):
            tile = raw[:, head // 2 * 128 : head // 2 * 128 + 128]
            queries[image * heads + head] = jnp.where(lax.div(lane, DH) == head % 2, tile, 0.0).astype(BF)
        normed_one_all[image] = jnp.concatenate([block.astype(F32) for block in blocks], 0).astype(BF)
        return carry

    lax.fori_loop(0, images, project, 0)

    for load in loads[2:5]:
        load.wait()
    out_low[me_t] = jnp.concatenate([pad, w_out[...].astype(BF)], 0)
    for index in range(2):
        gate_up_low[me_t, index] = w_gate_up[index].astype(BF)
    down_low[me_t] = w_down[...].astype(BF)
    inner_all[me_t] = jnp.zeros_like(inner_all[me_t])
    inner_all[me_t, 0:2] = inner_pack[...]
    for copy in weight_copies():
        copy.start()
    loads[5].wait()
    extra[...] = jnp.zeros_like(extra)
    inner_sums[...] = jnp.zeros_like(inner_sums)

    def half_mask(half):
        lane = lax.broadcasted_iota(jnp.int32, (1, 128), 1)
        return lax.div(lane, DH) == half

    def tile_of(index):
        return pl.ds(pl.multiple_of(index * 128, 128), 128)

    def key_tile(image, index):
        return keys_values[image, :, :, tile_of(index)].reshape(slots, 128)

    def attend(image):
        for copy in pair_copies(image):
            copy.wait_recv()
        bias = jnp.where(keep[pl.ds(image, 1), :] > 0, 0.0, -1e30)
        attended[...] = jnp.zeros_like(attended)

        def head_step(head, carry):
            scores[...] = dot(queries[image * heads + head], key_tile(image, lax.div(head, 2)), NT)
            for start in range(0, seq_rows, CHUNK):
                rows = slice(start, start + CHUNK)
                part = scores[rows] + bias
                part = jnp.exp(part - jnp.max(part, -1, keepdims=True))
                part = part * (1.0 / jnp.sum(part, -1, keepdims=True))
                probs[image * heads + head, rows] = part.astype(BF)
            place = lax.div(head + 1, 2)
            mixed = dot(probs[image * heads + head], key_tile(image, place + 1), NN)
            attended[:, tile_of(place)] += jnp.where(half_mask(lax.rem(head + 1, 2)), mixed, 0.0)
            return carry

        lax.fori_loop(0, heads, head_step, 0)
        attended_low[image] = attended[...].astype(BF)
        attended_in[me_t, image] = attended[own_rows].astype(BF)
        attended_send[image] = attended[other_rows].astype(BF)
        att_copy(image).start()

    def feed(image):
        att_copy(image).wait_recv()
        inputs = tokens[image].astype(F32)
        branch = sum(dot(attended_in[half, image], out_low[half], NN) for half in range(2))
        middle = inputs + branch
        extra[4:5] += column_sums(branch * branch)
        normed, hat_two, inverse_two = norm_parts(middle, gain_two, bias_two)
        rows_two = normed.astype(BF)
        normed_two[me_t, image] = rows_two
        halves = (me_t, other)
        gates = [dot(rows_two, gate_up_low[half, 0], NN) for half in halves]
        ups = [dot(rows_two, gate_up_low[half, 1], NN) for half in halves]
        sigmoids = [1.0 / (1.0 + jnp.exp(-gate)) for gate in gates]
        hiddens = [gate * sigmoid * up for gate, sigmoid, up in zip(gates, sigmoids, ups)]
        mean = sum(jnp.sum(hidden, -1, keepdims=True) for hidden in hiddens) / hidden_all
        centres = [hidden - mean for hidden in hiddens]
        spread = sum(jnp.sum(centre * centre, -1, keepdims=True) for centre in centres) / hidden_all
        inverse_three = lax.rsqrt(spread + EPSILON)
        hats = [centre * inverse_three for centre in centres]
        lows = [
            (hat * inner_all[half, 0:1] + inner_all[half, 1:2]).astype(BF)
            for hat, half in zip(hats, halves)
        ]
        branch = sum(dot(low, down_low[half], NN) for low, half in zip(lows, halves))
        extra[5:6] += column_sums(branch * branch)
        residual[image] = middle + branch
        cotangent = out_grad[image, own_rows] * mask[image, own_rows]
        grad_branch = cotangent.astype(BF)
        grads = [dot(grad_branch, down_low[half], NT) for half in halves]
        for half, grad, hat in zip(halves, grads, hats):
            inner_sums[half, 0:1] += column_sums(grad * hat)
            inner_sums[half, 1:2] += column_sums(grad)
        scaled = [grad * inner_all[half, 0:1] for grad, half in zip(grads, halves)]
        first = sum(jnp.sum(value, -1, keepdims=True) for value in scaled) / hidden_all
        second = (
            sum(jnp.sum(value * hat, -1, keepdims=True) for value, hat in zip(scaled, hats)) / hidden_all
        )
        grad_hiddens = [
            inverse_three * (value - first - hat * second) for value, hat in zip(scaled, hats)
        ]
        gate_rows = [
            (grad * up * (sigmoid + gate * sigmoid * (1.0 - sigmoid))).astype(BF)
            for grad, up, sigmoid, gate in zip(grad_hiddens, ups, sigmoids, gates)
        ]
        up_rows = [
            (grad * gate * sigmoid).astype(BF)
            for grad, gate, sigmoid in zip(grad_hiddens, gates, sigmoids)
        ]
        normed_three[me_t, image] = lows[0]
        normed_three_send[image] = lows[1]
        grad_gate[me_t, image] = gate_rows[0]
        grad_gate_send[image] = gate_rows[1]
        grad_up[me_t, image] = up_rows[0]
        grad_up_send[image] = up_rows[1]
        grad_two = sum(
            dot(gate_row, gate_up_low[half, 0], NT) + dot(up_row, gate_up_low[half, 1], NT)
            for gate_row, up_row, half in zip(gate_rows, up_rows, halves)
        )
        extra[2:3] += column_sums(grad_two * hat_two)
        extra[3:4] += column_sums(grad_two)
        back = cotangent + norm_back(grad_two, hat_two, inverse_two, gain_two)
        grad_middle[image] = back
        low = back.astype(BF)
        grad_middle_low[me_t, image] = low
        grad_attended[me_t, image] = dot(low, out_low[me_t], NT).astype(BF)
        grad_attended_send[image] = dot(low, out_low[other], NT).astype(BF)
        datt_copy(image).start()
        for copy in row_copies(image):
            copy.start()

    def attend_back(image):
        datt_copy(image).wait_recv()
        grad_attended_all[...] = jnp.concatenate(
            [grad_attended[half, image].astype(F32) for half in range(2)], 0
        )
        grad_query[...] = jnp.zeros_like(grad_query)
        grad_pairs[...] = jnp.zeros_like(grad_pairs)

        def head_step(head, carry):
            place = lax.div(head + 1, 2)
            at_key, at_value = lax.div(head, 2), place + 1
            key_half, value_half = half_mask(lax.rem(head, 2)), half_mask(lax.rem(head + 1, 2))
            wide = jnp.where(value_half, grad_attended_all[:, tile_of(place)], 0.0)
            low = wide.astype(BF)
            scores[...] = dot(low, key_tile(image, at_value), NT)
            delta = jnp.sum(wide * attended_low[image, :, tile_of(place)].astype(F32), -1, keepdims=True)
            for start in range(0, seq_rows, CHUNK):
                rows = slice(start, start + CHUNK)
                chance = probs[image * heads + head, rows].astype(F32)
                grad_scores[rows] = (chance * (scores[rows] - delta[rows])).astype(BF)
            grad_query[:, tile_of(at_key)] += jnp.where(
                key_half, dot(grad_scores[...], key_tile(image, at_key), NN), 0.0
            )
            query_t = jnp.transpose(queries[image * heads + head].astype(F32)).astype(BF)
            grad_pairs[tile_of(at_key)] += dot(query_t, grad_scores[...], NN)
            grad_pairs[tile_of(at_value)] += dot(
                jnp.transpose(wide).astype(BF), probs[image * heads + head], NN
            )
            return carry

        lax.fori_loop(0, heads, head_step, 0)
        pairs = jnp.transpose(grad_pairs[...])
        pairs_send[image] = pairs.astype(BF).reshape(ns, seq_rows, width)
        for copy in back_copies(image):
            copy.start()
        raw = grad_query[...] * (DH ** (-0.5))
        raw = turn_queries(raw, cosine[...], -sine[...])
        grad_query_low[image] = raw.astype(BF)

    def stage(step, carry):
        @pl.when(step < images)
        def _():
            attend(step)

        @pl.when(step >= 1)
        def _():
            attend_back(step - 1)

        @pl.when(step == 0)
        def _():
            for copy in weight_copies():
                copy.wait_recv()

        @pl.when(step < images)
        def _():
            feed(step)

        return carry

    lax.fori_loop(0, images + 1, stage, 0)
    inner_copy().start()

    for load in loads[7:10]:
        load.wait()

    def weights(image, carry):
        for copy in row_copies(image):
            copy.wait_recv()
        for half in range(2):
            place = slice(half * own, half * own + own)
            grad_branch = (out_grad[image, place] * mask[image, place]).astype(BF)
            full_down[...] += dot(normed_three[half, image], grad_branch, TN) * scale
            rows_two = normed_two[half, image]
            full_gate_up[0] += dot(rows_two, grad_gate[half, image], TN) * scale
            full_gate_up[1] += dot(rows_two, grad_up[half, image], TN) * scale
            mixed = attended_low[image].astype(F32)[place].astype(BF)
            full_out[...] += dot(mixed, grad_middle_low[half, image], TN)[256 - narrow :] * scale
        return carry

    lax.fori_loop(0, images, weights, 0)

    def low_exchange(axis, size, buffers, number):
        return exchange(axis, size, buffers, low_send.at[number], low_recv.at[number])

    share = 1.0 / (ns * nd)
    early = early_t.at[me_t]
    early[0:8] = fine_dot(basis_out[...], full_out[...], NN)
    for index in range(2):
        early[8 + 8 * index : 16 + 8 * index] = fine_dot(
            basis_gate_up[index], full_gate_up[index], NT
        )
    early[24:32] = fine_dot(basis_down[...], full_down[...], NN)
    early[32:40] = extra[...]
    moves = low_exchange("tensor", nt, (early_t,), 0)

    sum_query[...] = jnp.zeros_like(sum_query)
    sum_pairs[...] = jnp.zeros_like(sum_pairs)

    def finish_pairs(image):
        for copy in back_copies(image):
            copy.wait_recv()
        pairs = pairs_send[image, me_s].astype(F32)
        for step in range(1, ns):
            pairs = pairs + pairs_recv[image, step].astype(F32)
        pairs = turn_pairs(pairs, cosine[...], -sine[...]).astype(BF)
        query = grad_query_low[image]
        grad_one[image] = dot(query, query_low[...], NN) + dot(pairs, key_value_low[...], NN)
        final_copy(image).start()
        sum_query[...] += dot(query, normed_one_all[image], TN)
        sum_pairs[...] += dot(pairs, normed_one_all[image], TN)

    finish_pairs(0)
    arrive(moves)
    early_d[me_d] = total(early_t, nt)
    early_moves = low_exchange("dp", nd, (early_d,), 1)

    def rest_pairs(image, carry):
        finish_pairs(image)
        return carry

    lax.fori_loop(1, images, rest_pairs, 0)
    loads[6].wait()
    full_qkv[0] += sum_query[0:narrow] * scale
    full_qkv[1] += sum_pairs[0:narrow] * scale
    full_qkv[2] += sum_pairs[narrow : 2 * narrow] * scale
    late_t[me_t] = sum(fine_dot(basis_qkv[index], full_qkv[index], NN) for index in range(3))
    late_moves = low_exchange("tensor", nt, (late_t,), 2)

    norm_t[me_t] = jnp.zeros_like(norm_t[me_t])

    def finish(image, carry):
        final_copy(image).wait_recv()
        grad = grad_one[image, own_rows] + grad_one_recv[image]
        _, hat_one, inverse_one = norm_parts(tokens[image].astype(F32), gain_one, bias_one)
        input_grad[image] = grad_middle[image] + norm_back(grad, hat_one, inverse_one, gain_one)
        norm_t[me_t, 0:1] += column_sums(grad * hat_one)
        norm_t[me_t, 1:2] += column_sums(grad)
        return carry

    def finalize_left(index, rows):
        left_rows[index] = rows
        triple = triple_first(rows)
        left_rows_fine[index] = triple.astype(BF)
        if index in (2, 3):
            left_cols_fine[index - 2] = jnp.transpose(triple).astype(BF)

    arrive(late_moves)
    late_s[me_s] = total(late_t, nt)
    late_moves = low_exchange("seq", ns, (late_s,), 3)
    lax.fori_loop(0, images, finish, 0)
    norm_moves = low_exchange("tensor", nt, (norm_t,), 4)
    arrive(early_moves)
    early_s[me_s] = total(early_d, nd)
    early_moves = low_exchange("seq", ns, (early_s,), 5)
    arrive(late_moves)
    late_d[me_d] = total(late_s, ns)
    late_moves = low_exchange("dp", nd, (late_d,), 6)
    arrive(early_moves)
    summed = total(early_s, ns)
    extra_sum[2:4] = summed[34:36] * (share * scale)
    extra_sum[4:6] = summed[36:38]
    extra_sum[6:8] = jnp.zeros_like(extra_sum[6:8])
    left = gram_schmidt(summed[0:32].reshape(4, RANK, width))
    for index in range(4):
        finalize_left(index + 1, left[index])
    thin_d[me_d] = fine_dot(left[0], full_out[...], NT)
    for index in range(2):
        broad_d[me_d, 8 * index : 8 * index + 8] = fine_dot(left[1 + index], full_gate_up[index], NN)
    broad_d[me_d, 16:24] = fine_dot(left[3], full_down[...], NT)
    inner_copy().wait_recv()
    broad_d[me_d, 24:32] = (inner_sums[me_t] + inner_recv[...]) * scale
    early_moves = low_exchange("dp", nd, (thin_d, broad_d), 7)
    arrive(norm_moves)
    norm_s[me_s] = total(norm_t, nt) * scale
    arrive(late_moves)
    left = gram_schmidt(total(late_d, nd).reshape(1, RANK, width))[0]
    for index in range(3):
        slim_s[me_s, 8 * index : 8 * index + 8] = fine_dot(left, full_qkv[index], NT)
    late_moves = low_exchange("seq", ns, (slim_s, norm_s), 8)
    finalize_left(0, left)
    arrive(early_moves)
    thin_s[me_s] = total(thin_d, nd)
    broad_s[me_s] = total(broad_d, nd)
    early_moves = low_exchange("seq", ns, (thin_s, broad_s), 9)
    arrive(late_moves)
    slim_d[me_d] = total(slim_s, ns)
    norm_d[me_d] = total(norm_s, ns)
    late_moves = low_exchange("dp", nd, (slim_d, norm_d), 10)

    def finalize_narrow(index, rows):
        narrow_rows[index] = rows
        narrow_cols_fine[index] = jnp.transpose(triple_second(rows)).astype(BF)

    arrive(early_moves)
    finalize_narrow(3, total(thin_s, ns) * share)
    broad = total(broad_s, ns) * share
    inner_sum[...] = broad[24:32]
    for index in range(3):
        part = broad[8 * index : 8 * index + 8]
        wide_rows[index] = part
        if index < 2:
            wide_rows_fine[index] = triple_second(part).astype(BF)
        else:
            down_cols_fine[...] = jnp.transpose(triple_second(part)).astype(BF)
    arrive(late_moves)
    slim = total(slim_d, nd) * share
    for index in range(3):
        finalize_narrow(index, slim[8 * index : 8 * index + 8])
    extra_sum[0:2] = total(norm_d, nd)[0:2] * share

    for image in range(images):
        for copy in (
            one_copy(image), *pair_copies(image), att_copy(image), datt_copy(image),
            *row_copies(image), *back_copies(image), final_copy(image),
        ):
            copy.wait_send()
    for copy in (*weight_copies(), inner_copy()):
        copy.wait_send()


def block(mesh_sizes, small, hbm):
    nd, ns, nt = mesh_sizes
    images, own, width = hbm[0].shape
    seq_rows = 2 * own
    slots = ns * seq_rows
    narrow = hbm[1].shape[1]
    heads = narrow // DH
    wide = small[2].shape[1]
    shape = jax.ShapeDtypeStruct
    outs = (
        shape((images, own, width), F32),
        shape((images, own, width), F32),
        shape((3, narrow, width), F32),
        shape((narrow, width), F32),
        shape((2, width, wide), F32),
        shape((wide, width), F32),
        shape((5, RANK, width), F32),
        shape((5, 3 * RANK, width), BF),
        shape((2, width, 3 * RANK), BF),
        shape((8, width), F32),
        shape((4, RANK, narrow), F32),
        shape((4, narrow, 3 * RANK), BF),
        shape((3, RANK, wide), F32),
        shape((2, 3 * RANK, wide), BF),
        shape((wide, 3 * RANK), BF),
        shape((8, wide), F32),
    )
    vmem = pl.BlockSpec(memory_space=pltpu.VMEM)
    hbm_spec = pl.BlockSpec(memory_space=pl.ANY)
    dma = pltpu.SemaphoreType.DMA
    scratch = [
        pltpu.VMEM((2, images, own, width), BF),
        pltpu.VMEM((images, seq_rows, width), BF),
        pltpu.VMEM((images, ns, seq_rows, width), BF),
        pltpu.VMEM((images * heads, seq_rows, 128), BF),
        pltpu.VMEM((images * heads, seq_rows, slots), BF),
        pltpu.VMEM((seq_rows, slots), F32),
        pltpu.VMEM((seq_rows, slots), BF),
        pltpu.VMEM((seq_rows, 256), F32),
        pltpu.VMEM((images, seq_rows, 256), BF),
        pltpu.VMEM((2, images, own, 256), BF),
        pltpu.VMEM((images, own, 256), BF),
        pltpu.VMEM((2, 256, width), BF),
        pltpu.VMEM((2, 2, width, wide), BF),
        pltpu.VMEM((2, wide, width), BF),
        pltpu.VMEM((2, 8, wide), F32),
        pltpu.VMEM((256, width), BF),
        pltpu.VMEM((2 * narrow, width), BF),
        pltpu.VMEM((2, images, own, width), BF),
        pltpu.VMEM((2, images, own, width), BF),
        pltpu.VMEM((images, own, width), F32),
        *[pltpu.VMEM((2, images, own, wide), BF)] * 3,
        *[pltpu.VMEM((images, own, wide), BF)] * 3,
        pltpu.VMEM((2, images, own, 256), BF),
        pltpu.VMEM((images, own, 256), BF),
        pltpu.VMEM((seq_rows, 256), F32),
        pltpu.VMEM((seq_rows, 256), F32),
        pltpu.VMEM((images, seq_rows, 256), BF),
        pltpu.VMEM((width, slots), F32),
        pltpu.VMEM((images, ns, seq_rows, width), BF),
        pltpu.VMEM((images, ns, seq_rows, width), BF),
        pltpu.VMEM((images, seq_rows, width), F32),
        pltpu.VMEM((images, own, width), F32),
        pltpu.VMEM((256, width), F32),
        pltpu.VMEM((2 * narrow, width), F32),
        pltpu.VMEM((2, 8, wide), F32),
        pltpu.VMEM((8, wide), F32),
        *[pltpu.VMEM(array.shape, array.dtype) for array in hbm[0:6]],
        pltpu.VMEM((images, seq_rows, 1), F32),
        pltpu.VMEM((seq_rows, 128), F32),
        pltpu.VMEM((seq_rows, 128), F32),
        pltpu.VMEM((8, width), F32),
        pltpu.VMEM((slots, 8), F32),
        *[pltpu.VMEM((size, 40, width), F32) for size in (nt, nd, ns)],
        *[pltpu.VMEM((size, 8, width), F32) for size in (nt, ns, nd)],
        *[pltpu.VMEM((size, 8, width), F32) for size in (nt, ns, nd)],
        *[pltpu.VMEM((size, 8, narrow), F32) for size in (nd, ns)],
        *[pltpu.VMEM((size, 32, wide), F32) for size in (nd, ns)],
        *[pltpu.VMEM((size, 24, narrow), F32) for size in (ns, nd)],
        dma((10,)),
        *[dma((images,))] * 2,
        *[dma((4,))] * 2,
        *[dma((images, ns))] * 2,
        *[dma((images,))] * 4,
        *[dma((images, 5))] * 2,
        *[dma((images, ns))] * 2,
        *[dma((images + 1,))] * 2,
        *[dma((11, 2, max(mesh_sizes)))] * 2,
    ]
    return pl.pallas_call(
        functools.partial(block_kernel, mesh_sizes, images),
        out_shape=outs,
        in_specs=[vmem] * len(small) + [hbm_spec] * len(hbm),
        out_specs=[vmem] * len(outs),
        scratch_shapes=scratch,
        compiler_params=pltpu.CompilerParams(
            collective_id=0, has_side_effects=True, vmem_limit_bytes=LIMIT * 2**20
        ),
        name="block",
    )(*small, *hbm)


def per_device(
    tokens,
    out_grad,
    keep_mask,
    w_qkv,
    w_out,
    w_gate_up,
    w_down,
    norm_pack,
    inner_pack,
    moment_qkv,
    moment_out,
    moment_gate_up,
    moment_down,
    moment_norm,
    moment_inner,
    error_qkv,
    error_out,
    error_gate_up,
    error_down,
    basis_qkv,
    basis_out,
    basis_gate_up,
    basis_down,
):
    own_rows, images, width = tokens.shape
    slot_count = keep_mask.shape[0]
    sizes = tuple(lax.axis_size(axis) for axis in ("dp", "seq", "tensor"))

    def turn(array):
        return jnp.swapaxes(array, -1, -2)

    residual, input_grad, *rest = block(
        sizes,
        (
            jnp.transpose(keep_mask), norm_pack, inner_pack,
            *(turn(basis) for basis in (basis_qkv, basis_out, basis_gate_up, basis_down)),
        ),
        (
            jnp.swapaxes(tokens, 0, 1), turn(w_qkv), w_out, w_gate_up, w_down, jnp.swapaxes(out_grad, 0, 1),
            turn(error_qkv[0]), error_out[0], error_gate_up[0], error_down[0],
        ),
    )
    fulls, parts = rest[0:4], rest[4:]
    (
        factor_left, factor_qkv, factor_out, factor_gate_up, factor_down,
        new_error_qkv, new_error_out, new_error_gate_up, new_error_down,
        new_moment_qkv, new_moment_out, new_moment_gate_up, new_moment_down, new_moment_norm, new_moment_inner,
        new_w_qkv, new_w_out, new_w_gate_up, new_w_down, new_norm_pack, new_inner_pack,
    ) = update(
        fulls,
        (turn(moment_qkv), moment_out, moment_gate_up, moment_down),
        (turn(w_qkv), w_out, w_gate_up, w_down),
        parts,
        (norm_pack, moment_norm, inner_pack, moment_inner),
    )
    squares = jnp.sum(parts[3][4:6], -1)
    branch_rms = jnp.sqrt(squares / (slot_count * images * lax.axis_size("dp") * width))
    return (
        jnp.swapaxes(residual, 0, 1), jnp.swapaxes(input_grad, 0, 1),
        *(turn(factor) for factor in (factor_left, factor_qkv, factor_out, factor_gate_up, factor_down)),
        turn(new_error_qkv)[None], new_error_out[None], new_error_gate_up[None], new_error_down[None],
        turn(new_moment_qkv), new_moment_out, new_moment_gate_up, new_moment_down, new_moment_norm, new_moment_inner,
        turn(new_w_qkv), new_w_out, new_w_gate_up, new_w_down, new_norm_pack, new_inner_pack,
        branch_rms,
    )


def solution(mesh):
    placed = (
        P(("seq", "tensor"), "dp", None),
        P("seq", "dp", None),
        P(None, "dp"),
        P(None, None, "tensor"),
        P("tensor", None),
        P(None, None, "tensor"),
        P("tensor", None),
        P(),
        P(None, "tensor"),
        P(None, None, "tensor"),
        P("tensor", None),
        P(None, None, "tensor"),
        P("tensor", None),
        P(),
        P(None, "tensor"),
        P(("dp", "seq"), None, None, "tensor"),
        P(("dp", "seq"), "tensor", None),
        P(("dp", "seq"), None, None, "tensor"),
        P(("dp", "seq"), "tensor", None),
        P(None, "tensor", None),
        P("tensor", None),
        P(None, "tensor", None),
        P("tensor", None),
    )
    return jax.shard_map(
        per_device,
        mesh=mesh,
        in_specs=placed,
        out_specs=(
            P(("seq", "tensor"), "dp", None),
            P(("seq", "tensor"), "dp", None),
            P(),
            P(None, "tensor", None),
            P("tensor", None),
            P(None, "tensor", None),
            P("tensor", None),
            P(("dp", "seq"), None, None, "tensor"),
            P(("dp", "seq"), "tensor", None),
            P(("dp", "seq"), None, None, "tensor"),
            P(("dp", "seq"), "tensor", None),
            P(None, None, "tensor"),
            P("tensor", None),
            P(None, None, "tensor"),
            P("tensor", None),
            P(),
            P(None, "tensor"),
            P(None, None, "tensor"),
            P("tensor", None),
            P(None, None, "tensor"),
            P("tensor", None),
            P(),
            P(None, "tensor"),
            P(),
        ),
        check_vma=False,
    )
```

```python
import functools
import math

import jax
import jax.numpy as jnp
from jax import lax
from jax.experimental import pallas as pl
from jax.experimental.pallas import tpu as pltpu
from jax.sharding import PartitionSpec as P

DH = 64
FF = 1024
GRID = 32
RANK = 8
QUARTER = DH // 4
CHUNK = 16
LIMIT = 43


EPSILON = 1e-06
MOMENTUM = 0.9
STEP_RATE = 0.5
MESH = pl.DeviceIdType.MESH
BF = jnp.bfloat16
F32 = jnp.float32


def split(value):
    high = value.astype(BF)
    return high, (value - high.astype(F32)).astype(BF)


def dot(left, right, dims):
    return lax.dot_general(left, right, (dims, ((), ())), preferred_element_type=F32)


NN = ((1,), (0,))
NT = ((1,), (1,))
TN = ((0,), (0,))


def fine_dot(left, right, dims):
    left_high, left_low = split(left)
    right_high, right_low = split(right)
    both = jnp.concatenate([left_high.astype(F32), left_low.astype(F32)], 0).astype(BF)
    rows = dot(both, right_high, dims)
    return rows[0:RANK] + rows[RANK:] + dot(left_high, right_low, dims)


def gram_schmidt(stack):
    rows = lax.broadcasted_iota(jnp.int32, (1, RANK, 1), 1)
    for index in range(RANK):
        column = stack[:, index : index + 1, :]
        products = jnp.sum(stack * column, -1, keepdims=True)
        scale = lax.rsqrt(products[:, index : index + 1, :] + EPSILON)
        done = column * scale
        rest = stack - (products * scale) * done
        stack = jnp.where(rows < index, stack, jnp.where(rows == index, done, rest))
    return stack


def exchange(axis, size, buffers, sends, receives):
    me = lax.axis_index(axis)
    copies = []
    for step in range(1, size):
        peer = lax.rem(me + step, size)
        for number, buffer in enumerate(buffers):
            copy = pltpu.make_async_remote_copy(
                src_ref=buffer.at[me],
                dst_ref=buffer.at[me],
                send_sem=sends.at[number, step],
                recv_sem=receives.at[number, step],
                device_id={axis: peer},
                device_id_type=MESH,
            )
            copy.start()
            copies.append(copy)
    return copies


def scatter(axis, size, pieces, inbox, sends, receives):
    me = lax.axis_index(axis)
    inbox[me] = pieces[me]
    copies = []
    for step in range(1, size):
        peer = lax.rem(me + step, size)
        copy = pltpu.make_async_remote_copy(
            src_ref=pieces.at[peer],
            dst_ref=inbox.at[me],
            send_sem=sends.at[0, step],
            recv_sem=receives.at[0, step],
            device_id={axis: peer},
            device_id_type=MESH,
        )
        copy.start()
        copies.append(copy)
    return copies


def arrive(copies):
    for copy in copies:
        copy.wait()


def total(buffer, size):
    value = buffer[0]
    for index in range(1, size):
        value = value + buffer[index]
    return value


def greet(axes, barrier):
    for axis, size in axes:
        me = lax.axis_index(axis)
        for step in range(1, size):
            pl.semaphore_signal(
                barrier, inc=1, device_id={axis: lax.rem(me + step, size)}, device_id_type=MESH
            )


def triple_first(rows):
    high, low = split(rows)
    return jnp.concatenate([high.astype(F32), high.astype(F32), low.astype(F32)], 0)


def triple_second(rows):
    high, low = split(rows)
    return jnp.concatenate([high.astype(F32), low.astype(F32), high.astype(F32)], 0)


def store_kernel(count, total_rows, *refs):
    sources, squares = refs[:count], refs[count]
    targets, branch_rms, sems = refs[count + 1 : 2 * count + 1], refs[2 * count + 1], refs[2 * count + 2]
    copies = [
        pltpu.make_async_copy(source, target, sems.at[number])
        for number, (source, target) in enumerate(zip(sources, targets))
    ]
    for copy in copies:
        copy.start()
    roots = jnp.sqrt(jnp.sum(squares[...], -1, keepdims=True) / total_rows)
    for index in range(2):
        branch_rms[index] = roots[index, 0]
    for copy in copies:
        copy.wait()


def store(arrays, squares, total_rows):
    vmem = pl.BlockSpec(memory_space=pltpu.VMEM)
    count = len(arrays)
    return pl.pallas_call(
        functools.partial(store_kernel, count, total_rows),
        out_shape=[*(jax.ShapeDtypeStruct(array.shape, F32) for array in arrays), jax.ShapeDtypeStruct((2,), F32)],
        in_specs=[vmem] * (count + 1),
        out_specs=[*[pl.BlockSpec(memory_space=pltpu.HBM)] * count, pl.BlockSpec(memory_space=pltpu.SMEM)],
        scratch_shapes=[pltpu.SemaphoreType.DMA((count,))],
        compiler_params=pltpu.CompilerParams(vmem_limit_bytes=2**20),
        name="store",
    )(*arrays, squares)


def swap_quarters(tile):
    lane = lax.broadcasted_iota(jnp.int32, (1, 128), 1)
    low = lax.rem(lax.div(lane, QUARTER), 2) == 0
    return jnp.where(low, pltpu.roll(tile, 128 - QUARTER, 1), pltpu.roll(tile, QUARTER, 1))


def turn_pairs(pairs, cosine, sine):
    keys = lax.broadcasted_iota(jnp.int32, (1, 128), 1) < DH
    first, second, third = (pairs[:, start : start + 128] for start in (0, 128, 256))
    first = first * cosine + swap_quarters(first) * sine
    second = jnp.where(keys, second * cosine + swap_quarters(second) * sine, second)
    return jnp.concatenate([first, second, third], -1)


def turn_queries(raw, cosine, sine):
    tiles = (raw[:, start : start + 128] for start in (0, 128))
    return jnp.concatenate([tile * cosine + swap_quarters(tile) * sine for tile in tiles], -1)


def angle_tables(first_slot, count):
    slots = first_slot + lax.broadcasted_iota(jnp.int32, (count, 128), 0)
    place = lax.rem(lax.broadcasted_iota(jnp.int32, (count, 128), 1), DH)
    inside = jnp.logical_and(slots >= 1, slots <= GRID * GRID)
    patch = jnp.where(inside, slots - 1, 0)
    quarter = lax.div(place, QUARTER)
    position = jnp.where(quarter < 2, lax.div(patch, GRID), lax.rem(patch, GRID)).astype(F32)
    power = lax.rem(place, QUARTER).astype(F32)
    angles = position * jnp.exp(power * (-math.log(10000.0) / QUARTER)) * (16.0 / GRID)
    sine = jnp.sin(angles)
    return jnp.cos(angles), jnp.where(lax.rem(quarter, 2) == 0, -sine, sine)


def norm_parts(values, gain, bias):
    centre = values - jnp.mean(values, -1, keepdims=True)
    spread = jnp.mean(centre * centre, -1, keepdims=True)
    inverse = lax.rsqrt(spread + EPSILON)
    normed = centre * inverse
    return (normed * gain + bias, normed, inverse)


def norm_back(grad, normed, inverse, gain):
    scaled = grad * gain
    return inverse * (
        scaled
        - jnp.mean(scaled, -1, keepdims=True)
        - normed * jnp.mean(scaled * normed, -1, keepdims=True)
    )


def column_sums(value):
    return jnp.sum(value, 0, keepdims=True)


def block_kernel(sizes, images, *refs):
    (
        keep, norm_pack, inner_pack, moment_norm, moment_inner, basis_qkv, basis_out, basis_gate_up, basis_down,
        tokens_hbm, w_qkv_hbm, w_out_hbm, w_gate_up_hbm, w_down_hbm, out_grad_hbm,
        error_qkv_hbm, error_out_hbm, error_gate_up_hbm, error_down_hbm,
        moment_qkv_hbm, moment_out_hbm, moment_gate_up_hbm, moment_down_hbm,
        residual, input_grad, factor_left, factor_qkv, factor_out, factor_gate_up, factor_down,
        full_qkv, full_out, full_gate_up, full_down,
        moment_qkv, moment_out, moment_gate_up, moment_down, new_moment_norm, new_moment_inner,
        w_qkv, w_out, w_gate_up, w_down, new_norm_pack, new_inner_pack, squares,
        normed_one, normed_one_all, keys_values, queries, probs, scores, grad_scores,
        attended, attended_low, attended_in, attended_send,
        out_low, gate_up_low, down_low, inner_all, query_low, key_value_low,
        normed_two, grad_middle_low, grad_middle, normed_three, grad_gate, grad_up,
        normed_three_send, grad_gate_send, grad_up_send,
        grad_attended, grad_attended_send, grad_attended_all, grad_query, grad_query_low, grad_pairs,
        pairs_send, pairs_x, pairs_y, relay_x, relay_y, grad_one, grad_one_recv, sum_query, sum_pairs, inner_sums, inner_recv,
        tokens, out_grad, mask, cosine, sine, extra, kept_rows,
        early_t, early_all, early_in, early_d, early_left, late_t, late_s, late_d, norm_t, norm_s, norm_d,
        right_all, right_in, right_d, right_sum, slim_s, slim_d, thin_s, thin_d,
        local_sems, one_send, one_recv, weight_send, weight_recv, pair_send, pair_recv,
        att_send, att_recv, datt_send, datt_recv, rows_send, rows_recv, back_send, back_recv,
        final_send, final_recv, low_send, low_recv,
    ) = refs
    nd, ns, nt = sizes
    me_t, me_s = lax.axis_index("tensor"), lax.axis_index("seq")
    other = 1 - me_t
    near_x = me_s + 1 - 2 * lax.rem(me_s, 2)
    near_y = lax.rem(me_s + 2, 4)
    far = 3 - me_s
    me_d = lax.axis_index("dp")
    own, width = tokens.shape[1], tokens.shape[2]
    seq_rows = 2 * own
    slots = ns * seq_rows
    heads = w_qkv.shape[1] // DH
    wide = w_down.shape[0]
    hidden_all = 2 * wide
    scale = (images * seq_rows) ** (-0.5)
    top = (own + 15) // 16 * 16
    upper, lower = slice(0, top), slice(top, seq_rows)
    own_rows = pl.ds(pl.multiple_of(me_t * own, 8), own)
    other_rows = pl.ds(pl.multiple_of(other * own, 8), own)

    barrier = pltpu.get_barrier_semaphore()
    greet((("tensor", nt), ("seq", ns), ("dp", nd)), barrier)
    loads = [
        pltpu.make_async_copy(source, target, local_sems.at[number])
        for number, (source, target) in enumerate(
            (
                (tokens_hbm, tokens), (w_qkv_hbm, w_qkv),
                (w_out_hbm, w_out), (w_gate_up_hbm, w_gate_up), (w_down_hbm, w_down), (out_grad_hbm, out_grad),
                (error_qkv_hbm, full_qkv), (error_out_hbm, full_out),
                (error_gate_up_hbm, full_gate_up), (error_down_hbm, full_down),
                (moment_qkv_hbm, moment_qkv), (moment_out_hbm, moment_out),
                (moment_gate_up_hbm, moment_gate_up), (moment_down_hbm, moment_down),
            )
        )
    ]
    for load in loads:
        load.start()

    def to_partner(source, target, send, receive):
        return pltpu.make_async_remote_copy(
            src_ref=source, dst_ref=target, send_sem=send, recv_sem=receive,
            device_id={"tensor": other}, device_id_type=MESH,
        )

    def to_seq(source, target, send, receive, peer):
        return pltpu.make_async_remote_copy(
            src_ref=source, dst_ref=target, send_sem=send, recv_sem=receive,
            device_id={"seq": peer}, device_id_type=MESH,
        )

    def one_copy(image):
        block = normed_one.at[me_t, image]
        return to_partner(block, block, one_send.at[image], one_recv.at[image])

    def weight_copies():
        return [
            to_partner(ref.at[me_t], ref.at[me_t], weight_send.at[number], weight_recv.at[number])
            for number, ref in enumerate((out_low, gate_up_low, down_low, inner_all))
        ]

    def pair_copy(image, tile, kind):
        place, peer = ((me_s, near_x), (me_s, near_y), (near_x, near_y), (near_y, near_x))[kind]
        block = keys_values.at[image, tile, place]
        if kind >= 2:
            block = block.at[(upper, lower)[kind - 2]]
        return to_seq(block, block, pair_send.at[image, tile, kind], pair_recv.at[image, tile, kind], peer)

    def send_pairs(image, tile):
        for kind in range(2):
            pair_copy(image, tile, kind).start()

    def forward_pairs(image, tile):
        for kind in range(2):
            pair_copy(image, tile, kind).wait_recv()
            pair_copy(image, tile, 2 + kind).start()

    def await_pairs(image, tile):
        for kind in range(2, 4):
            pair_copy(image, tile, kind).wait_recv()

    def att_copy(image):
        return to_partner(
            attended_send.at[image], attended_in.at[me_t, image], att_send.at[image], att_recv.at[image]
        )

    def datt_copy(image):
        return to_partner(
            grad_attended_send.at[image], grad_attended.at[me_t, image], datt_send.at[image], datt_recv.at[image]
        )

    def row_copies(image):
        moves = (
            (normed_two.at[me_t, image], normed_two),
            (grad_middle_low.at[me_t, image], grad_middle_low),
            (normed_three_send.at[image], normed_three),
            (grad_gate_send.at[image], grad_gate),
            (grad_up_send.at[image], grad_up),
        )
        return [
            to_partner(source, target.at[me_t, image], rows_send.at[image, number], rows_recv.at[image, number])
            for number, (source, target) in enumerate(moves)
        ]

    def back_copy(image, kind):
        place, rows, target, there, peer = (
            (far, upper, relay_x, slice(0, top), near_x),
            (far, lower, relay_y, slice(0, seq_rows - top), near_y),
            (near_x, upper, pairs_x, upper, near_x),
            (near_y, lower, pairs_y, lower, near_y),
            (near_x, lower, pairs_x, lower, near_x),
            (near_y, upper, pairs_y, upper, near_y),
        )[kind]
        return to_seq(
            pairs_send.at[image, place, rows], target.at[image, there],
            back_send.at[image, kind], back_recv.at[image, kind], peer,
        )

    def relay_back(image):
        for place, rows, inbox, arrival, onward in ((near_y, upper, relay_x, 0, 5), (near_x, lower, relay_y, 1, 4)):
            back_copy(image, arrival).wait_recv()
            value = pairs_send[image, place, rows].astype(F32) + inbox[image].astype(F32)
            pairs_send[image, place, rows] = value.astype(BF)
            back_copy(image, onward).start()

    def final_copy(image):
        return to_partner(
            grad_one.at[image, other_rows], grad_one_recv.at[image], final_send.at[image], final_recv.at[image]
        )

    def inner_copy():
        return to_partner(
            inner_sums.at[other], inner_recv, final_send.at[images], final_recv.at[images]
        )

    gain_one, bias_one = norm_pack[0:1], norm_pack[1:2]
    gain_two, bias_two = norm_pack[2:3], norm_pack[3:4]

    cosine[...], sine[...] = angle_tables(me_s * seq_rows, seq_rows)
    kept = jnp.concatenate([keep[...].astype(F32), jnp.zeros((8 - images, slots), F32)], 0)
    kept_rows[...] = jnp.transpose(kept)
    kept = kept_rows[pl.ds(pl.multiple_of(me_s * seq_rows, 8), seq_rows)]
    for image in range(images):
        mask[image] = kept[:, image : image + 1]
    loads[0].wait()
    for image in range(images):
        normed, _, _ = norm_parts(tokens[image].astype(F32), gain_one, bias_one)
        normed_one[me_t, image] = normed.astype(BF)
    pl.semaphore_wait(barrier, (nt - 1) + (ns - 1) + (nd - 1))
    for image in range(images):
        one_copy(image).start()
    loads[1].wait()

    narrow = heads * DH
    pad = jnp.zeros((256 - narrow, width), BF)
    query_low[...] = jnp.concatenate([w_qkv[0].astype(BF), pad], 0)
    key_value_low[0:narrow] = w_qkv[1].astype(BF)
    key_value_low[narrow : 2 * narrow] = w_qkv[2].astype(BF)

    def project(image, carry):
        one_copy(image).wait_recv()
        blocks = [normed_one[half, image] for half in range(2)]
        pairs = jnp.concatenate([dot(block, key_value_low[...], NT) for block in blocks], 0)
        pairs = turn_pairs(pairs, cosine[...], sine[...])
        for tile in range(3):
            keys_values[image, tile, me_s] = pairs[:, 128 * tile : 128 * tile + 128].astype(BF)

        @pl.when(image == 0)
        def _():
            for tile in range(3):
                send_pairs(image, tile)

        raw = jnp.concatenate([dot(block, query_low[...], NT) for block in blocks], 0)
        raw = turn_queries(raw, cosine[...], sine[...]) * (DH ** (-0.5))
        lane = lax.broadcasted_iota(jnp.int32, (1, 128), 1)
        for head in range(heads):
            tile = raw[:, head // 2 * 128 : head // 2 * 128 + 128]
            queries[image * heads + head] = jnp.where(lax.div(lane, DH) == head % 2, tile, 0.0).astype(BF)
        normed_one_all[image] = jnp.concatenate([block.astype(F32) for block in blocks], 0).astype(BF)
        return carry

    lax.fori_loop(0, images, project, 0)

    for load in loads[2:5]:
        load.wait()
    out_low[me_t] = jnp.concatenate([pad, w_out[...].astype(BF)], 0)
    for index in range(2):
        gate_up_low[me_t, index] = w_gate_up[index].astype(BF)
    down_low[me_t] = w_down[...].astype(BF)
    inner_all[me_t] = jnp.zeros_like(inner_all[me_t])
    inner_all[me_t, 0:2] = inner_pack[...]
    for copy in weight_copies():
        copy.start()
    loads[5].wait()
    extra[...] = jnp.zeros_like(extra)
    inner_sums[...] = jnp.zeros_like(inner_sums)

    def halves_of(lower, upper):
        lane = lax.broadcasted_iota(jnp.int32, (1, 128), 1)
        return jnp.where(lane < DH, lower, upper)

    def half_of(value, half):
        return halves_of(value, 0.0) if half == 0 else halves_of(0.0, value)

    def key_tile(image, index):
        return keys_values[image, index].reshape(slots, 128)

    def attend(image):
        @pl.when(image == 0)
        def _():
            forward_pairs(0, 0)
            forward_pairs(0, 1)
            send_pairs(1, 0)
            forward_pairs(0, 2)
            send_pairs(1, 1)
            send_pairs(1, 2)

        bias = jnp.where(keep[pl.ds(image, 1), :] > 0, 0.0, -1e30)

        def score(head):
            scores[head % 2] = dot(queries[image * heads + head], key_tile(image, head // 2), NT)

        def chances(head):
            for start in range(0, seq_rows, CHUNK):
                rows = slice(start, start + CHUNK)
                part = scores[head % 2, rows] + bias
                part = jnp.exp(part - jnp.max(part, -1, keepdims=True))
                part = part * (1.0 / jnp.sum(part, -1, keepdims=True))
                probs[image * heads + head, rows] = part.astype(BF)

        def mix(head):
            return dot(probs[image * heads + head], key_tile(image, 1 + (head + 1) // 2), NN)

        await_pairs(image, 0)
        score(0)
        score(1)
        chances(0)
        await_pairs(image, 1)
        score(2)
        mixed = [mix(0)]
        chances(1)
        await_pairs(image, 2)
        mixed.append(mix(1))
        chances(2)
        mixed.append(mix(2))
        attended[:, 0:128] = half_of(mixed[0], 1)
        attended[:, 128:256] = halves_of(mixed[1], mixed[2])
        attended_low[image] = attended[...].astype(BF)
        attended_in[me_t, image] = attended[own_rows].astype(BF)
        attended_send[image] = attended[other_rows].astype(BF)
        att_copy(image).start()

        @pl.when(image == 0)
        def _():
            forward_pairs(1, 0)
            forward_pairs(1, 1)

        @pl.when(image == 1)
        def _():
            forward_pairs(2, 0)

        @pl.when(image == 2)
        def _():
            relay_back(0)

    def feed(image):
        att_copy(image).wait_recv()
        inputs = tokens[image].astype(F32)
        branch = sum(dot(attended_in[half, image], out_low[half], NN) for half in range(2))
        middle = inputs + branch
        extra[4:5] += column_sums(branch * branch)
        normed, hat_two, inverse_two = norm_parts(middle, gain_two, bias_two)
        rows_two = normed.astype(BF)
        normed_two[me_t, image] = rows_two
        halves = (me_t, other)
        gates = [dot(rows_two, gate_up_low[half, 0], NN) for half in halves]
        ups = [dot(rows_two, gate_up_low[half, 1], NN) for half in halves]
        sigmoids = [1.0 / (1.0 + jnp.exp(-gate)) for gate in gates]
        hiddens = [gate * sigmoid * up for gate, sigmoid, up in zip(gates, sigmoids, ups)]
        mean = sum(jnp.sum(hidden, -1, keepdims=True) for hidden in hiddens) / hidden_all
        centres = [hidden - mean for hidden in hiddens]
        spread = sum(jnp.sum(centre * centre, -1, keepdims=True) for centre in centres) / hidden_all
        inverse_three = lax.rsqrt(spread + EPSILON)
        hats = [centre * inverse_three for centre in centres]
        lows = [
            (hat * inner_all[half, 0:1] + inner_all[half, 1:2]).astype(BF)
            for hat, half in zip(hats, halves)
        ]
        branch = sum(dot(low, down_low[half], NN) for low, half in zip(lows, halves))
        extra[5:6] += column_sums(branch * branch)
        residual[image] = middle + branch

        @pl.when(image == 0)
        def _():
            forward_pairs(1, 2)
            for tile in range(3):
                send_pairs(2, tile)

        cotangent = out_grad[image, own_rows] * mask[image, own_rows]
        grad_branch = cotangent.astype(BF)
        grads = [dot(grad_branch, down_low[half], NT) for half in halves]
        for half, grad, hat in zip(halves, grads, hats):
            inner_sums[half, 0:1] += column_sums(grad * hat)
            inner_sums[half, 1:2] += column_sums(grad)
        scaled = [grad * inner_all[half, 0:1] for grad, half in zip(grads, halves)]
        first = sum(jnp.sum(value, -1, keepdims=True) for value in scaled) / hidden_all
        second = (
            sum(jnp.sum(value * hat, -1, keepdims=True) for value, hat in zip(scaled, hats)) / hidden_all
        )
        grad_hiddens = [
            inverse_three * (value - first - hat * second) for value, hat in zip(scaled, hats)
        ]
        gate_rows = [
            (grad * up * (sigmoid + gate * sigmoid * (1.0 - sigmoid))).astype(BF)
            for grad, up, sigmoid, gate in zip(grad_hiddens, ups, sigmoids, gates)
        ]
        up_rows = [
            (grad * gate * sigmoid).astype(BF)
            for grad, gate, sigmoid in zip(grad_hiddens, gates, sigmoids)
        ]
        normed_three[me_t, image] = lows[0]
        normed_three_send[image] = lows[1]
        grad_gate[me_t, image] = gate_rows[0]
        grad_gate_send[image] = gate_rows[1]
        grad_up[me_t, image] = up_rows[0]
        grad_up_send[image] = up_rows[1]
        grad_two = sum(
            dot(gate_row, gate_up_low[half, 0], NT) + dot(up_row, gate_up_low[half, 1], NT)
            for gate_row, up_row, half in zip(gate_rows, up_rows, halves)
        )
        extra[2:3] += column_sums(grad_two * hat_two)
        extra[3:4] += column_sums(grad_two)
        back = cotangent + norm_back(grad_two, hat_two, inverse_two, gain_two)
        grad_middle[image] = back
        low = back.astype(BF)
        grad_middle_low[me_t, image] = low
        grad_attended[me_t, image] = dot(low, out_low[me_t], NT).astype(BF)
        grad_attended_send[image] = dot(low, out_low[other], NT).astype(BF)
        datt_copy(image).start()
        for copy in row_copies(image):
            copy.start()

    def attend_back(image):
        datt_copy(image).wait_recv()
        grad_attended_all[...] = jnp.concatenate(
            [grad_attended[half, image].astype(F32) for half in range(2)], 0
        )
        wides = [half_of(grad_attended_all[:, 0:128], 1)]
        wides += [half_of(grad_attended_all[:, 128:256], half) for half in range(2)]
        lows = [wide.astype(BF) for wide in wides]
        mixed = attended_low[image].astype(F32)
        deltas = [
            jnp.sum(wide * mixed[:, tile * 128 : tile * 128 + 128], -1, keepdims=True)
            for wide, tile in zip(wides, (0, 1, 1))
        ]

        def grad_chance(head):
            scores[head % 2] = dot(lows[head], key_tile(image, 1 + (head + 1) // 2), NT)

        def grad_score(head):
            for start in range(0, seq_rows, CHUNK):
                rows = slice(start, start + CHUNK)
                chance = probs[image * heads + head, rows].astype(F32)
                grad_scores[head, rows] = (chance * (scores[head % 2, rows] - deltas[head][rows])).astype(BF)

        def pair_rows(place, wide, half, right):
            rows = jnp.transpose(wide)[half * DH : half * DH + DH].astype(BF)
            grad_pairs[place * DH : place * DH + DH] = dot(rows, right, NN)

        def value_grad(head):
            pair_rows(heads + head, wides[head], (head + 1) % 2, probs[image * heads + head])

        def key_grad(head):
            wide = queries[image * heads + head].astype(F32)
            pair_rows(head, wide, head % 2, grad_scores[head])

        def query_grad(head):
            return dot(grad_scores[head], key_tile(image, head // 2), NN)

        grad_chance(0)
        grad_chance(1)
        value_grad(0)
        grad_score(0)
        grad_chance(2)
        value_grad(1)
        grad_score(1)
        query_grads = [query_grad(0)]
        key_grad(0)
        value_grad(2)
        grad_score(2)
        query_grads.append(query_grad(1))
        key_grad(1)
        query_grads.append(query_grad(2))
        key_grad(2)
        grad_query[:, 0:128] = halves_of(query_grads[0], query_grads[1])
        grad_query[:, 128:256] = half_of(query_grads[2], 0)
        pairs = jnp.transpose(grad_pairs[...])
        pairs_send[image] = pairs.astype(BF).reshape(ns, seq_rows, width)

        @pl.when(image == 0)
        def _():
            forward_pairs(2, 1)
            forward_pairs(2, 2)

        for kind in range(4):
            back_copy(image, kind).start()
        raw = grad_query[...] * (DH ** (-0.5))
        raw = turn_queries(raw, cosine[...], -sine[...])
        grad_query_low[image] = raw.astype(BF)

    def weights(image):
        for copy in row_copies(image):
            copy.wait_recv()
        for half in range(2):
            place = slice(half * own, half * own + own)
            grad_branch = (out_grad[image, place] * mask[image, place]).astype(BF)
            full_down[...] += dot(normed_three[half, image], grad_branch, TN) * scale
            rows_two = normed_two[half, image]
            full_gate_up[0] += dot(rows_two, grad_gate[half, image], TN) * scale
            full_gate_up[1] += dot(rows_two, grad_up[half, image], TN) * scale
            mixed = attended_low[image].astype(F32)[place].astype(BF)
            full_out[...] += dot(mixed, grad_middle_low[half, image], TN)[256 - narrow :] * scale

    def stage(step, carry):
        @pl.when(step < images)
        def _():
            attend(step)

        @pl.when(step == images)
        def _():
            for load in loads[7:10]:
                load.wait()
            lax.fori_loop(0, images - 1, lambda image, rest: weights(image) or rest, 0)
            relay_back(1)

        @pl.when(step >= 1)
        def _():
            attend_back(step - 1)

        @pl.when(step == 0)
        def _():
            for copy in weight_copies():
                copy.wait_recv()

        @pl.when(step < images)
        def _():
            feed(step)

        return carry

    lax.fori_loop(0, images + 1, stage, 0)
    inner_copy().start()

    weights(images - 1)

    def low_exchange(axis, size, buffers, number):
        return exchange(axis, size, buffers, low_send.at[number], low_recv.at[number])

    def low_scatter(pieces, inbox, number):
        return scatter("seq", ns, pieces, inbox, low_send.at[number], low_recv.at[number])

    share = 1.0 / (ns * nd)
    early = early_t.at[me_t]
    early[0] = fine_dot(basis_out[...], full_out[...], NN)
    for index in range(2):
        early[1 + index] = fine_dot(basis_gate_up[index], full_gate_up[index], NT)
    early[3] = fine_dot(basis_down[...], full_down[...], NN)
    early_moves = low_exchange("tensor", nt, (early_t,), 0)

    sum_query[...] = jnp.zeros_like(sum_query)
    sum_pairs[...] = jnp.zeros_like(sum_pairs)

    def finish_pairs(image):
        for kind in range(2, 6):
            back_copy(image, kind).wait_recv()
        pairs = pairs_send[image, me_s].astype(F32)
        pairs = pairs + pairs_x[image].astype(F32) + pairs_y[image].astype(F32)
        pairs = turn_pairs(pairs, cosine[...], -sine[...]).astype(BF)
        query = grad_query_low[image]
        grad_one[image] = dot(query, query_low[...], NN) + dot(pairs, key_value_low[...], NN)
        final_copy(image).start()
        sum_query[...] += dot(query, normed_one_all[image], TN)
        sum_pairs[...] += dot(pairs, normed_one_all[image], TN)

    finish_pairs(0)
    arrive(early_moves)
    early_all[...] = total(early_t, nt)
    early_moves = low_scatter(early_all, early_in, 1)
    relay_back(images - 1)
    finish_pairs(1)
    arrive(early_moves)
    early_d[me_d] = total(early_in, ns)
    early_moves = low_exchange("dp", nd, (early_d,), 2)
    finish_pairs(2)
    loads[6].wait()
    full_qkv[0] += sum_query[0:narrow] * scale
    full_qkv[1] += sum_pairs[0:narrow] * scale
    full_qkv[2] += sum_pairs[narrow : 2 * narrow] * scale
    late_t[me_t] = sum(fine_dot(basis_qkv[index], full_qkv[index], NN) for index in range(3))
    late_moves = low_exchange("tensor", nt, (late_t,), 3)

    norm_t[me_t] = extra[...]

    def finish(image, carry):
        final_copy(image).wait_recv()
        grad = grad_one[image, own_rows] + grad_one_recv[image]
        _, hat_one, inverse_one = norm_parts(tokens[image].astype(F32), gain_one, bias_one)
        input_grad[image] = grad_middle[image] + norm_back(grad, hat_one, inverse_one, gain_one)
        norm_t[me_t, 0:1] += column_sums(grad * hat_one)
        norm_t[me_t, 1:2] += column_sums(grad)
        return carry

    def settle(left, right, full, moment, weight):
        approx = dot(triple_second(right).astype(BF), triple_first(left).astype(BF), TN)
        full[...] = full[...] - approx
        fresh = MOMENTUM * moment[...] + approx
        moment[...] = fresh
        weight[...] = weight[...] - STEP_RATE * fresh

    def orthonormal(rows):
        return gram_schmidt(rows.reshape(1, RANK, width))[0]

    arrive(late_moves)
    late_s[me_s] = total(late_t, nt)
    late_moves = low_exchange("seq", ns, (late_s,), 4)
    arrive(early_moves)
    early_left[me_s] = orthonormal(total(early_d, nd))
    early_moves = low_exchange("seq", ns, (early_left,), 5)
    lax.fori_loop(0, images, finish, 0)
    norm_moves = low_exchange("tensor", nt, (norm_t,), 6)
    arrive(late_moves)
    late_d[me_d] = total(late_s, ns)
    late_moves = low_exchange("dp", nd, (late_d,), 7)
    arrive(early_moves)
    right_all[0, :, 0:narrow] = fine_dot(early_left[0], full_out[...], NT)
    right_all[0, :, narrow:] = jnp.zeros((RANK, wide - narrow), F32)
    for index in range(2):
        right_all[1 + index] = fine_dot(early_left[1 + index], full_gate_up[index], NN)
    right_all[3] = fine_dot(early_left[3], full_down[...], NT)
    early_moves = low_scatter(right_all, right_in, 8)
    for index in range(4):
        factor_left[1 + index] = early_left[index]
    inner_copy().wait_recv()
    thin_s[me_s] = (inner_sums[me_t] + inner_recv[...]) * scale
    arrive(norm_moves)
    norm_s[me_s] = total(norm_t, nt)
    arrive(early_moves)
    right_d[me_d] = total(right_in, ns)
    early_moves = low_exchange("dp", nd, (right_d,), 9)
    arrive(late_moves)
    left = orthonormal(total(late_d, nd))
    for index in range(3):
        slim_s[me_s, 8 * index : 8 * index + 8] = fine_dot(left, full_qkv[index], NT)
    late_moves = low_exchange("seq", ns, (slim_s, norm_s, thin_s), 10)
    factor_left[0] = left
    for load in loads[10:14]:
        load.wait()
    arrive(late_moves)
    slim_d[me_d] = total(slim_s, ns)
    norm_d[me_d] = total(norm_s, ns)
    thin_d[me_d] = total(thin_s, ns)
    late_moves = low_exchange("dp", nd, (slim_d, norm_d, thin_d), 11)
    arrive(early_moves)
    right_sum[me_s] = total(right_d, nd) * share
    early_moves = low_exchange("seq", ns, (right_sum,), 12)
    arrive(early_moves)
    right = right_sum[0, :, 0:narrow]
    factor_out[...] = right
    settle(early_left[0], right, full_out, moment_out, w_out)
    for index in range(2):
        right = right_sum[1 + index]
        factor_gate_up[index] = right
        left_triple, right_triple = triple_first(early_left[1 + index]), triple_second(right)
        approx = dot(left_triple.astype(BF), right_triple.astype(BF), TN)
        full_gate_up[index] = full_gate_up[index] - approx
        fresh = MOMENTUM * moment_gate_up[index] + approx
        moment_gate_up[index] = fresh
        w_gate_up[index] = w_gate_up[index] - STEP_RATE * fresh
    factor_down[...] = right_sum[3]
    settle(early_left[3], right_sum[3], full_down, moment_down, w_down)
    arrive(late_moves)
    slim = total(slim_d, nd) * share
    for index in range(3):
        right = slim[8 * index : 8 * index + 8]
        factor_qkv[index] = right
        settle(left, right, full_qkv.at[index], moment_qkv.at[index], w_qkv.at[index])
    norms = total(norm_d, nd)
    squares[...] = norms[4:6]
    fresh = MOMENTUM * moment_norm[...] + norms[0:4] * (share * scale)
    new_moment_norm[...] = fresh
    new_norm_pack[...] = norm_pack[...] - STEP_RATE * fresh
    fresh = MOMENTUM * moment_inner[...] + total(thin_d, nd)[0:2] * share
    new_moment_inner[...] = fresh
    new_inner_pack[...] = inner_pack[...] - STEP_RATE * fresh

    for image in range(images):
        for copy in (
            one_copy(image), att_copy(image), datt_copy(image), *row_copies(image), final_copy(image),
            *(pair_copy(image, tile, kind) for tile in range(3) for kind in range(4)),
            *(back_copy(image, kind) for kind in range(6)),
        ):
            copy.wait_send()
    for copy in (*weight_copies(), inner_copy()):
        copy.wait_send()


def block(mesh_sizes, small, hbm):
    nd, ns, nt = mesh_sizes
    images, own, width = hbm[0].shape
    seq_rows = 2 * own
    slots = ns * seq_rows
    top = (own + 15) // 16 * 16
    narrow = hbm[1].shape[1]
    heads = narrow // DH
    wide = small[2].shape[1]
    shape = jax.ShapeDtypeStruct
    matrices = ((3, narrow, width), (narrow, width), (2, width, wide), (wide, width))
    shapes = (
        (images, own, width), (images, own, width),
        (5, RANK, width), (3, RANK, narrow), (RANK, narrow), (2, RANK, wide), (RANK, wide),
        *matrices, *matrices, (4, width), (2, wide), *matrices, (4, width), (2, wide), (2, width),
    )
    outs = [pltpu.VMEM(dims, F32) for dims in shapes]
    vmem = pl.BlockSpec(memory_space=pltpu.VMEM)
    hbm_spec = pl.BlockSpec(memory_space=pltpu.HBM)
    dma = pltpu.SemaphoreType.DMA
    scratch = [
        pltpu.VMEM((2, images, own, width), BF),
        pltpu.VMEM((images, seq_rows, width), BF),
        pltpu.VMEM((images, 3, ns, seq_rows, 128), BF),
        pltpu.VMEM((images * heads, seq_rows, 128), BF),
        pltpu.VMEM((images * heads, seq_rows, slots), BF),
        pltpu.VMEM((2, seq_rows, slots), F32),
        pltpu.VMEM((heads, seq_rows, slots), BF),
        pltpu.VMEM((seq_rows, 256), F32),
        pltpu.VMEM((images, seq_rows, 256), BF),
        pltpu.VMEM((2, images, own, 256), BF),
        pltpu.VMEM((images, own, 256), BF),
        pltpu.VMEM((2, 256, width), BF),
        pltpu.VMEM((2, 2, width, wide), BF),
        pltpu.VMEM((2, wide, width), BF),
        pltpu.VMEM((2, 8, wide), F32),
        pltpu.VMEM((256, width), BF),
        pltpu.VMEM((2 * narrow, width), BF),
        pltpu.VMEM((2, images, own, width), BF),
        pltpu.VMEM((2, images, own, width), BF),
        pltpu.VMEM((images, own, width), F32),
        *[pltpu.VMEM((2, images, own, wide), BF)] * 3,
        *[pltpu.VMEM((images, own, wide), BF)] * 3,
        pltpu.VMEM((2, images, own, 256), BF),
        pltpu.VMEM((images, own, 256), BF),
        pltpu.VMEM((seq_rows, 256), F32),
        pltpu.VMEM((seq_rows, 256), F32),
        pltpu.VMEM((images, seq_rows, 256), BF),
        pltpu.VMEM((width, slots), F32),
        pltpu.VMEM((images, ns, seq_rows, width), BF),
        *[pltpu.VMEM((images, seq_rows, width), BF)] * 2,
        pltpu.VMEM((images, top, width), BF),
        pltpu.VMEM((images, seq_rows - top, width), BF),
        pltpu.VMEM((images, seq_rows, width), F32),
        pltpu.VMEM((images, own, width), F32),
        pltpu.VMEM((256, width), F32),
        pltpu.VMEM((2 * narrow, width), F32),
        pltpu.VMEM((2, 8, wide), F32),
        pltpu.VMEM((8, wide), F32),
        pltpu.VMEM(hbm[0].shape, BF),
        pltpu.VMEM(hbm[5].shape, F32),
        pltpu.VMEM((images, seq_rows, 1), F32),
        pltpu.VMEM((seq_rows, 128), F32),
        pltpu.VMEM((seq_rows, 128), F32),
        pltpu.VMEM((8, width), F32),
        pltpu.VMEM((slots, 8), F32),
        pltpu.VMEM((nt, 4, RANK, width), F32),
        pltpu.VMEM((4, RANK, width), F32),
        *[pltpu.VMEM((size, RANK, width), F32) for size in (ns, nd, ns)],
        *[pltpu.VMEM((size, RANK, width), F32) for size in (nt, ns, nd)],
        *[pltpu.VMEM((size, RANK, width), F32) for size in (nt, ns, nd)],
        *[pltpu.VMEM((size, RANK, wide), F32) for size in (4, ns, nd, ns)],
        *[pltpu.VMEM((size, 3 * RANK, narrow), F32) for size in (ns, nd)],
        *[pltpu.VMEM((size, RANK, wide), F32) for size in (ns, nd)],
        dma((14,)),
        *[dma((images,))] * 2,
        *[dma((4,))] * 2,
        *[dma((images, 3, 4))] * 2,
        *[dma((images,))] * 4,
        *[dma((images, 5))] * 2,
        *[dma((images, 6))] * 2,
        *[dma((images + 1,))] * 2,
        *[dma((13, 3, max(mesh_sizes)))] * 2,
    ]
    return pl.pallas_call(
        functools.partial(block_kernel, mesh_sizes, images),
        out_shape=outs,
        in_specs=[vmem] * len(small) + [hbm_spec] * len(hbm),
        out_specs=[vmem] * len(outs),
        scratch_shapes=scratch,
        compiler_params=pltpu.CompilerParams(
            collective_id=0, has_side_effects=True, vmem_limit_bytes=(LIMIT + nd // 8) * 2**20
        ),
        name="block",
    )(*small, *hbm)


def per_device(
    tokens,
    out_grad,
    keep_mask,
    w_qkv,
    w_out,
    w_gate_up,
    w_down,
    norm_pack,
    inner_pack,
    moment_qkv,
    moment_out,
    moment_gate_up,
    moment_down,
    moment_norm,
    moment_inner,
    error_qkv,
    error_out,
    error_gate_up,
    error_down,
    basis_qkv,
    basis_out,
    basis_gate_up,
    basis_down,
):
    own_rows, images, width = tokens.shape
    slot_count = keep_mask.shape[0]
    sizes = tuple(lax.axis_size(axis) for axis in ("dp", "seq", "tensor"))

    def turn(array):
        return jnp.swapaxes(array, -1, -2)

    *arrays, squares = block(
        sizes,
        (
            jnp.transpose(keep_mask), norm_pack, inner_pack, moment_norm, moment_inner,
            *(turn(basis) for basis in (basis_qkv, basis_out, basis_gate_up, basis_down)),
        ),
        (
            jnp.swapaxes(tokens, 0, 1), turn(w_qkv), w_out, w_gate_up, w_down, jnp.swapaxes(out_grad, 0, 1),
            turn(error_qkv[0]), error_out[0], error_gate_up[0], error_down[0],
            turn(moment_qkv), moment_out, moment_gate_up, moment_down,
        ),
    )
    (
        residual, input_grad, factor_left, factor_qkv, factor_out, factor_gate_up, factor_down,
        new_error_qkv, new_error_out, new_error_gate_up, new_error_down,
        new_moment_qkv, new_moment_out, new_moment_gate_up, new_moment_down, new_moment_norm, new_moment_inner,
        new_w_qkv, new_w_out, new_w_gate_up, new_w_down, new_norm_pack, new_inner_pack,
        branch_rms,
    ) = store(arrays, squares, float(slot_count * images * lax.axis_size("dp") * width))
    return (
        jnp.swapaxes(residual, 0, 1), jnp.swapaxes(input_grad, 0, 1),
        *(turn(factor) for factor in (factor_left, factor_qkv, factor_out, factor_gate_up, factor_down)),
        turn(new_error_qkv)[None], new_error_out[None], new_error_gate_up[None], new_error_down[None],
        turn(new_moment_qkv), new_moment_out, new_moment_gate_up, new_moment_down, new_moment_norm, new_moment_inner,
        turn(new_w_qkv), new_w_out, new_w_gate_up, new_w_down, new_norm_pack, new_inner_pack,
        branch_rms,
    )


def solution(mesh):
    placed = (
        P(("seq", "tensor"), "dp", None),
        P("seq", "dp", None),
        P(None, "dp"),
        P(None, None, "tensor"),
        P("tensor", None),
        P(None, None, "tensor"),
        P("tensor", None),
        P(),
        P(None, "tensor"),
        P(None, None, "tensor"),
        P("tensor", None),
        P(None, None, "tensor"),
        P("tensor", None),
        P(),
        P(None, "tensor"),
        P(("dp", "seq"), None, None, "tensor"),
        P(("dp", "seq"), "tensor", None),
        P(("dp", "seq"), None, None, "tensor"),
        P(("dp", "seq"), "tensor", None),
        P(None, "tensor", None),
        P("tensor", None),
        P(None, "tensor", None),
        P("tensor", None),
    )
    return jax.shard_map(
        per_device,
        mesh=mesh,
        in_specs=placed,
        out_specs=(
            P(("seq", "tensor"), "dp", None),
            P(("seq", "tensor"), "dp", None),
            P(),
            P(None, "tensor", None),
            P("tensor", None),
            P(None, "tensor", None),
            P("tensor", None),
            P(("dp", "seq"), None, None, "tensor"),
            P(("dp", "seq"), "tensor", None),
            P(("dp", "seq"), None, None, "tensor"),
            P(("dp", "seq"), "tensor", None),
            P(None, None, "tensor"),
            P("tensor", None),
            P(None, None, "tensor"),
            P("tensor", None),
            P(),
            P(None, "tensor"),
            P(None, None, "tensor"),
            P("tensor", None),
            P(None, None, "tensor"),
            P("tensor", None),
            P(),
            P(None, "tensor"),
            P(),
        ),
        check_vma=False,
    )
```

```python
import functools
import math

import jax
import jax.numpy as jnp
from jax import lax
from jax.experimental import pallas as pl
from jax.experimental.pallas import tpu as pltpu
from jax.sharding import PartitionSpec as P

DH = 64
FF = 1024
GRID = 32
RANK = 8
QUARTER = DH // 4
CHUNK = 16
LIMIT = 46


EPSILON = 1e-06
MOMENTUM = 0.9
STEP_RATE = 0.5
MESH = pl.DeviceIdType.MESH
BF = jnp.bfloat16
F32 = jnp.float32


def split(value):
    high = value.astype(BF)
    return high, (value - high.astype(F32)).astype(BF)


def dot(left, right, dims):
    return lax.dot_general(left, right, (dims, ((), ())), preferred_element_type=F32)


NN = ((1,), (0,))
NT = ((1,), (1,))
TN = ((0,), (0,))


def two_rows(rows):
    high, low = split(rows)
    return jnp.concatenate([high.astype(F32), low.astype(F32)], 0).astype(BF)


def fold(rows):
    return rows[0:RANK] + rows[RANK:]


def fine_dot(left, right, dims):
    right_high, right_low = split(right)
    return fold(dot(two_rows(left), right_high, dims)) + dot(left.astype(BF), right_low, dims)


def gram_schmidt(stack):
    rows = lax.broadcasted_iota(jnp.int32, (1, RANK, 1), 1)
    for index in range(RANK):
        column = stack[:, index : index + 1, :]
        products = jnp.sum(stack * column, -1, keepdims=True)
        scale = lax.rsqrt(products[:, index : index + 1, :] + EPSILON)
        done = column * scale
        rest = stack - (products * scale) * done
        stack = jnp.where(rows < index, stack, jnp.where(rows == index, done, rest))
    return stack


def exchange(axis, size, buffers, sends, receives, base):
    me = lax.axis_index(axis)
    copies = []
    for step in range(1, size):
        peer = lax.rem(me + step, size)
        for buffer in buffers:
            place = base + len(copies)
            copy = pltpu.make_async_remote_copy(
                src_ref=buffer.at[me],
                dst_ref=buffer.at[me],
                send_sem=sends.at[place],
                recv_sem=receives.at[place],
                device_id={axis: peer},
                device_id_type=MESH,
            )
            copy.start()
            copies.append(copy)
    return copies


def scatter(axis, size, pieces, inbox, sends, receives, base):
    me = lax.axis_index(axis)
    inbox[me] = pieces[me]
    copies = []
    for step in range(1, size):
        peer = lax.rem(me + step, size)
        copy = pltpu.make_async_remote_copy(
            src_ref=pieces.at[peer],
            dst_ref=inbox.at[me],
            send_sem=sends.at[base + step - 1],
            recv_sem=receives.at[base + step - 1],
            device_id={axis: peer},
            device_id_type=MESH,
        )
        copy.start()
        copies.append(copy)
    return copies


def arrive(copies):
    for copy in copies:
        copy.wait()


def total(buffer, size):
    value = buffer[0]
    for index in range(1, size):
        value = value + buffer[index]
    return value


def greet(axes, barrier):
    for axis, size in axes:
        me = lax.axis_index(axis)
        for step in range(1, size):
            pl.semaphore_signal(
                barrier, inc=1, device_id={axis: lax.rem(me + step, size)}, device_id_type=MESH
            )


def triple_first(rows):
    high, low = split(rows)
    return jnp.concatenate([high.astype(F32), high.astype(F32), low.astype(F32)], 0)


def triple_second(rows):
    high, low = split(rows)
    return jnp.concatenate([high.astype(F32), low.astype(F32), high.astype(F32)], 0)


def store_kernel(total_rows, plain, *refs):
    sources, rest = refs[:plain], refs[plain:]
    squares, factor_left, factor_qkv, factor_out, factor_gate_up, factor_down = rest[:6]
    fulls, moments, weights = rest[6:10], rest[10:14], rest[14:18]
    targets, rest = rest[18 : 18 + plain], rest[18 + plain :]
    results, branch_rms, fresh, sems = rest[:12], rest[12], rest[13:25], rest[25]
    copies = [
        pltpu.make_async_copy(source, target, sems.at[number])
        for number, (source, target) in enumerate(zip(sources, targets))
    ]
    for copy in copies:
        copy.start()

    def settle(number, approx, pick):
        full, moment, weight = (pick(group[number]) for group in (fulls, moments, weights))
        places = (number, 4 + number, 8 + number)
        error_to, moment_to, weight_to = (pick(fresh[place]) for place in places)
        error_to[...] = full[...] - approx
        momentum = MOMENTUM * moment[...] + approx
        moment_to[...] = momentum
        weight_to[...] = weight[...] - STEP_RATE * momentum
        for place in places:
            copy = pltpu.make_async_copy(pick(fresh[place]), pick(results[place]), sems.at[len(copies)])
            copy.start()
            copies.append(copy)

    def product(rows, columns):
        return dot(rows.astype(BF), columns.astype(BF), TN)

    lefts = [triple_first(factor_left[index]) for index in range(5)]
    for index in range(2):
        settle(2, product(lefts[2 + index], triple_second(factor_gate_up[index])), lambda ref: ref.at[index])
    settle(3, product(triple_second(factor_down[...]), lefts[4]), lambda ref: ref)
    settle(1, product(triple_second(factor_out[...]), lefts[1]), lambda ref: ref)
    for index in range(3):
        settle(0, product(triple_second(factor_qkv[index]), lefts[0]), lambda ref: ref.at[index])
    roots = jnp.sqrt(jnp.sum(squares[...], -1, keepdims=True) / total_rows)
    for index in range(2):
        branch_rms[index] = roots[index, 0]
    for copy in copies:
        copy.wait()


def store(plain, squares, factors, fulls, moments, weights, total_rows):
    vmem = pl.BlockSpec(memory_space=pltpu.VMEM)
    matrices = [*fulls, *moments, *weights]
    shapes = [jax.ShapeDtypeStruct(array.shape, F32) for array in (*plain, *factors, *matrices)]
    count = len(plain) + len(factors)
    return pl.pallas_call(
        functools.partial(store_kernel, total_rows, count),
        out_shape=[*shapes, jax.ShapeDtypeStruct((2,), F32)],
        in_specs=[vmem] * (count + 1 + len(factors) + 12),
        out_specs=[*[pl.BlockSpec(memory_space=pltpu.HBM)] * len(shapes), pl.BlockSpec(memory_space=pltpu.SMEM)],
        scratch_shapes=[
            *[pltpu.VMEM(array.shape, F32) for array in matrices],
            pltpu.SemaphoreType.DMA((count + 21,)),
        ],
        compiler_params=pltpu.CompilerParams(vmem_limit_bytes=24 * 2**20),
        name="store",
    )(*plain, *factors, squares, *factors, *matrices)


def swap_quarters(tile):
    lane = lax.broadcasted_iota(jnp.int32, (1, 128), 1)
    low = lax.rem(lax.div(lane, QUARTER), 2) == 0
    return jnp.where(low, pltpu.roll(tile, 128 - QUARTER, 1), pltpu.roll(tile, QUARTER, 1))


def turn_pairs(pairs, cosine, sine):
    keys = lax.broadcasted_iota(jnp.int32, (1, 128), 1) < DH
    first, second, third = (pairs[:, start : start + 128] for start in (0, 128, 256))
    first = first * cosine + swap_quarters(first) * sine
    second = jnp.where(keys, second * cosine + swap_quarters(second) * sine, second)
    return jnp.concatenate([first, second, third], -1)


def turn_queries(raw, cosine, sine):
    tiles = (raw[:, start : start + 128] for start in (0, 128))
    return jnp.concatenate([tile * cosine + swap_quarters(tile) * sine for tile in tiles], -1)


def angle_tables(first_slot, count):
    slots = first_slot + lax.broadcasted_iota(jnp.int32, (count, 128), 0)
    place = lax.rem(lax.broadcasted_iota(jnp.int32, (count, 128), 1), DH)
    inside = jnp.logical_and(slots >= 1, slots <= GRID * GRID)
    patch = jnp.where(inside, slots - 1, 0)
    quarter = lax.div(place, QUARTER)
    position = jnp.where(quarter < 2, lax.div(patch, GRID), lax.rem(patch, GRID)).astype(F32)
    power = lax.rem(place, QUARTER).astype(F32)
    angles = position * jnp.exp(power * (-math.log(10000.0) / QUARTER)) * (16.0 / GRID)
    sine = jnp.sin(angles)
    return jnp.cos(angles), jnp.where(lax.rem(quarter, 2) == 0, -sine, sine)


def norm_parts(values, gain, bias):
    centre = values - jnp.mean(values, -1, keepdims=True)
    spread = jnp.mean(centre * centre, -1, keepdims=True)
    inverse = lax.rsqrt(spread + EPSILON)
    normed = centre * inverse
    return (normed * gain + bias, normed, inverse)


def norm_back(grad, normed, inverse, gain):
    scaled = grad * gain
    return inverse * (
        scaled
        - jnp.mean(scaled, -1, keepdims=True)
        - normed * jnp.mean(scaled * normed, -1, keepdims=True)
    )


def column_sums(value):
    return jnp.sum(value, 0, keepdims=True)


def block_kernel(sizes, images, *refs):
    (
        keep, norm_pack, inner_pack, moment_norm, moment_inner, basis_qkv, basis_out, basis_gate_up, basis_down,
        tokens_hbm, w_qkv_hbm, w_out_hbm, w_gate_up_hbm, w_down_hbm, out_grad_hbm,
        error_qkv_hbm, error_out_hbm, error_gate_up_hbm, error_down_hbm,
        moment_qkv_hbm, moment_out_hbm, moment_gate_up_hbm, moment_down_hbm,
        residual, input_grad, factor_left, factor_qkv, factor_out, factor_gate_up, factor_down,
        full_qkv, full_out, full_gate_up, full_down,
        moment_qkv, moment_out, moment_gate_up, moment_down, new_moment_norm, new_moment_inner,
        w_qkv, w_out, w_gate_up, w_down, new_norm_pack, new_inner_pack, squares,
        normed_one, normed_one_all, keys_values, queries, probs, scores, grad_scores,
        attended, attended_low, attended_in, attended_send,
        out_low, gate_up_low, down_low, inner_all, query_low, key_value_low,
        slim_rows, grad_middle, wide_rows, wide_rows_send, grad_down, queries_t,
        grad_attended, grad_attended_send, grad_attended_all, grad_query, grad_query_low, grad_pairs,
        *rest,
    ) = refs
    pairs_send, pairs_x, pairs_y, relay_x, relay_y = rest[0:5]
    ( grad_one, grad_one_recv, sum_query, sum_pairs, inner_sums, inner_recv,
        tokens, out_grad, mask, cosine, sine, extra, kept_rows, late_sum, thin_query, thin_pairs,
        early_t, early_all, early_in, early_d, early_left, late_t, late_s, late_d, norm_t, norm_s, norm_d,
        right_all, right_in, right_d, right_sum, slim_s, slim_d, tiny_s, tiny_d,
        local_sems, one_send, one_recv, weight_send, weight_recv, pair_send, pair_recv,
        att_send, att_recv, datt_send, datt_recv, rows_send, rows_recv, back_send, back_recv,
        final_send, final_recv, low_send, low_recv,
    ) = rest[5:]
    nd, ns, nt = sizes
    me_t, me_s = lax.axis_index("tensor"), lax.axis_index("seq")
    other = 1 - me_t
    near_x = me_s + 1 - 2 * lax.rem(me_s, 2)
    near_y = lax.rem(me_s + 2, 4)
    far = 3 - me_s
    me_d = lax.axis_index("dp")
    own, width = tokens.shape[1], tokens.shape[2]
    seq_rows = 2 * own
    slots = ns * seq_rows
    heads = w_qkv.shape[1] // DH
    wide = w_down.shape[0]
    hidden_all = 2 * wide
    scale = (images * seq_rows) ** (-0.5)
    top = (own + 15) // 16 * 16
    upper, lower = slice(0, top), slice(top, seq_rows)
    own_rows = pl.ds(pl.multiple_of(me_t * own, 8), own)
    other_rows = pl.ds(pl.multiple_of(other * own, 8), own)

    barrier = pltpu.get_barrier_semaphore()
    greet((("tensor", nt), ("seq", ns), ("dp", nd)), barrier)
    loads = [
        pltpu.make_async_copy(source, target, local_sems.at[number])
        for number, (source, target) in enumerate(
            (
                (tokens_hbm, tokens), (w_qkv_hbm, w_qkv),
                (w_out_hbm, w_out), (w_gate_up_hbm, w_gate_up), (w_down_hbm, w_down), (out_grad_hbm, out_grad),
                (error_qkv_hbm, full_qkv), (error_out_hbm, full_out),
                (error_gate_up_hbm, full_gate_up), (error_down_hbm, full_down),
                (moment_qkv_hbm, moment_qkv), (moment_out_hbm, moment_out),
                (moment_gate_up_hbm, moment_gate_up), (moment_down_hbm, moment_down),
            )
        )
    ]
    for load in loads:
        load.start()

    def to_partner(source, target, send, receive):
        return pltpu.make_async_remote_copy(
            src_ref=source, dst_ref=target, send_sem=send, recv_sem=receive,
            device_id={"tensor": other}, device_id_type=MESH,
        )

    def to_seq(source, target, send, receive, peer):
        return pltpu.make_async_remote_copy(
            src_ref=source, dst_ref=target, send_sem=send, recv_sem=receive,
            device_id={"seq": peer}, device_id_type=MESH,
        )

    def one_copy(image):
        block = normed_one.at[me_t, image]
        return to_partner(block, block, one_send.at[image], one_recv.at[image])

    def weight_copies():
        return [
            to_partner(ref.at[me_t], ref.at[me_t], weight_send.at[number], weight_recv.at[number])
            for number, ref in enumerate((out_low, gate_up_low, down_low, inner_all))
        ]

    def pair_copy(image, tile, kind):
        place, peer = ((me_s, near_x), (me_s, near_y), (near_x, near_y), (near_y, near_x))[kind]
        block = keys_values.at[image, tile, place]
        if kind >= 2:
            block = block.at[(upper, lower)[kind - 2]]
        return to_seq(block, block, pair_send.at[image, tile, kind], pair_recv.at[image, tile, kind], peer)

    def send_pairs(image, tile):
        for kind in range(2):
            pair_copy(image, tile, kind).start()

    def forward_pairs(image, tile):
        for kind in range(2):
            pair_copy(image, tile, kind).wait_recv()
            pair_copy(image, tile, 2 + kind).start()

    def await_pairs(image, tile):
        for kind in range(2, 4):
            pair_copy(image, tile, kind).wait_recv()

    def att_copy(image):
        return to_partner(
            attended_send.at[image], attended_in.at[me_t, image], att_send.at[image], att_recv.at[image]
        )

    def datt_copy(image):
        return to_partner(
            grad_attended_send.at[image], grad_attended.at[me_t, image], datt_send.at[image], datt_recv.at[image]
        )

    def row_copies(image):
        moves = ((slim_rows.at[me_t, image], slim_rows), (wide_rows_send.at[image], wide_rows))
        return [
            to_partner(source, target.at[me_t, image], rows_send.at[image, number], rows_recv.at[image, number])
            for number, (source, target) in enumerate(moves)
        ]

    def back_copy(image, kind):
        place, rows, target, there, peer = (
            (far, upper, relay_x, slice(0, top), near_x),
            (far, lower, relay_y, slice(0, seq_rows - top), near_y),
            (near_x, upper, pairs_x, upper, near_x),
            (near_y, lower, pairs_y, lower, near_y),
            (near_x, lower, pairs_x, lower, near_x),
            (near_y, upper, pairs_y, upper, near_y),
        )[kind]
        return to_seq(
            pairs_send.at[image, place, rows], target.at[image, there],
            back_send.at[image, kind], back_recv.at[image, kind], peer,
        )

    def relay_back(image):
        for place, rows, inbox, arrival, onward in ((near_y, upper, relay_x, 0, 5), (near_x, lower, relay_y, 1, 4)):
            back_copy(image, arrival).wait_recv()
            value = pairs_send[image, place, rows].astype(F32) + inbox[image].astype(F32)
            pairs_send[image, place, rows] = value.astype(BF)
            back_copy(image, onward).start()

    def final_copy(image):
        return to_partner(
            grad_one.at[image, other_rows], grad_one_recv.at[image], final_send.at[image], final_recv.at[image]
        )

    def inner_copy():
        return to_partner(
            inner_sums.at[other], inner_recv, final_send.at[images], final_recv.at[images]
        )

    gain_one, bias_one = norm_pack[0:1], norm_pack[1:2]
    gain_two, bias_two = norm_pack[2:3], norm_pack[3:4]

    cosine[...], sine[...] = angle_tables(me_s * seq_rows, seq_rows)
    loads[0].wait()
    for image in range(images):
        normed, _, _ = norm_parts(tokens[image].astype(F32), gain_one, bias_one)
        normed_one[me_t, image] = normed.astype(BF)
        if image == 0:
            pl.semaphore_wait(barrier, (nt - 1) + (ns - 1) + (nd - 1))
        one_copy(image).start()
    loads[1].wait()

    narrow = heads * DH
    pad = jnp.zeros((256 - narrow, width), BF)
    query_low[...] = jnp.concatenate([w_qkv[0].astype(BF), pad], 0)
    key_value_low[0:narrow] = w_qkv[1].astype(BF)
    key_value_low[narrow : 2 * narrow] = w_qkv[2].astype(BF)

    def project(image, carry):
        one_copy(image).wait_recv()
        blocks = [normed_one[half, image] for half in range(2)]
        pairs = jnp.concatenate([dot(block, key_value_low[...], NT) for block in blocks], 0)
        pairs = turn_pairs(pairs, cosine[...], sine[...])
        for tile in range(3):
            keys_values[image, tile, me_s] = pairs[:, 128 * tile : 128 * tile + 128].astype(BF)

        @pl.when(image == 0)
        def _():
            for tile in range(3):
                send_pairs(image, tile)

        raw = jnp.concatenate([dot(block, query_low[...], NT) for block in blocks], 0)
        raw = turn_queries(raw, cosine[...], sine[...]) * (DH ** (-0.5))
        lane = lax.broadcasted_iota(jnp.int32, (1, 128), 1)
        for head in range(heads):
            tile = raw[:, head // 2 * 128 : head // 2 * 128 + 128]
            queries[image * heads + head] = jnp.where(lax.div(lane, DH) == head % 2, tile, 0.0).astype(BF)
        normed_one_all[image] = jnp.concatenate([block.astype(F32) for block in blocks], 0).astype(BF)
        return carry

    lax.fori_loop(0, images, project, 0)

    for load in loads[2:5]:
        load.wait()
    out_low[me_t] = jnp.concatenate([pad, w_out[...].astype(BF)], 0)
    for index in range(2):
        gate_up_low[me_t, index] = w_gate_up[index].astype(BF)
    down_low[me_t] = w_down[...].astype(BF)
    inner_all[me_t] = jnp.zeros_like(inner_all[me_t])
    inner_all[me_t, 0:2] = inner_pack[...]
    for copy in weight_copies():
        copy.start()
    kept = jnp.concatenate([keep[...].astype(F32), jnp.zeros((8 - images, slots), F32)], 0)
    kept_rows[...] = jnp.transpose(kept)
    kept = kept_rows[pl.ds(pl.multiple_of(me_s * seq_rows, 8), seq_rows)]
    for image in range(images):
        mask[image] = kept[:, image : image + 1]
    loads[5].wait()
    loads[6].wait()
    late_sum[...] = sum(fine_dot(basis_qkv[index], full_qkv[index], NN) for index in range(3))
    gap = jnp.zeros((RANK, 256 - narrow), F32)
    thin_query[...] = two_rows(jnp.concatenate([basis_qkv[0], gap], -1))
    thin_pairs[...] = two_rows(jnp.concatenate([basis_qkv[1], basis_qkv[2]], -1))
    extra[...] = jnp.zeros_like(extra)
    inner_sums[...] = jnp.zeros_like(inner_sums)

    def halves_of(lower, upper):
        lane = lax.broadcasted_iota(jnp.int32, (1, 128), 1)
        return jnp.where(lane < DH, lower, upper)

    def half_of(value, half):
        return halves_of(value, 0.0) if half == 0 else halves_of(0.0, value)

    def key_tile(image, index):
        return keys_values[image, index].reshape(slots, 128)

    def attend(image):
        @pl.when(image == 0)
        def _():
            forward_pairs(0, 0)
            forward_pairs(0, 1)
            forward_pairs(0, 2)
            for tile in range(3):
                send_pairs(1, tile)
            for copy in weight_copies():
                copy.wait_recv()

            def ahead(place, carry):
                cotangent = out_grad[place, own_rows] * mask[place, own_rows]
                for index, half in enumerate((me_t, other)):
                    grad_down[place, index] = dot(cotangent.astype(BF), down_low[half], NT)
                for head in range(heads):
                    turned = jnp.transpose(queries[place * heads + head].astype(F32))
                    start = head % 2 * DH
                    queries_t[place * heads + head] = turned[start : start + DH].astype(BF)
                return carry

            lax.fori_loop(0, images, ahead, 0)

        bias = jnp.where(keep[pl.ds(image, 1), :] > 0, 0.0, -1e30)

        def score(head):
            scores[head % 2] = dot(queries[image * heads + head], key_tile(image, head // 2), NT)

        def chances(head):
            for start in range(0, seq_rows, CHUNK):
                rows = slice(start, start + CHUNK)
                part = scores[head % 2, rows] + bias
                part = jnp.exp(part - jnp.max(part, -1, keepdims=True))
                part = part * (1.0 / jnp.sum(part, -1, keepdims=True))
                probs[image * heads + head, rows] = part.astype(BF)

        def mix(head):
            return dot(probs[image * heads + head], key_tile(image, 1 + (head + 1) // 2), NN)

        await_pairs(image, 0)
        score(0)
        score(1)
        chances(0)
        await_pairs(image, 1)
        score(2)
        mixed = [mix(0)]
        chances(1)
        await_pairs(image, 2)
        mixed.append(mix(1))
        chances(2)
        mixed.append(mix(2))
        attended[:, 0:128] = half_of(mixed[0], 1)
        attended[:, 128:256] = halves_of(mixed[1], mixed[2])
        attended_low[image] = attended[...].astype(BF)
        attended_in[me_t, image] = attended[own_rows].astype(BF)
        attended_send[image] = attended[other_rows].astype(BF)
        att_copy(image).start()

        @pl.when(image == 0)
        def _():
            forward_pairs(1, 0)

        @pl.when(image == 1)
        def _():
            forward_pairs(2, 0)

        @pl.when(image == 2)
        def _():
            relay_back(0)

    def feed(image):
        att_copy(image).wait_recv()
        inputs = tokens[image].astype(F32)
        branch = sum(dot(attended_in[half, image], out_low[half], NN) for half in range(2))
        middle = inputs + branch
        extra[4:5] += column_sums(branch * branch)
        normed, hat_two, inverse_two = norm_parts(middle, gain_two, bias_two)
        rows_two = normed.astype(BF)
        slim_rows[me_t, image, :, 0:width] = rows_two
        halves = (me_t, other)
        gates = [dot(rows_two, gate_up_low[half, 0], NN) for half in halves]
        ups = [dot(rows_two, gate_up_low[half, 1], NN) for half in halves]
        sigmoids = [1.0 / (1.0 + jnp.exp(-gate)) for gate in gates]
        hiddens = [gate * sigmoid * up for gate, sigmoid, up in zip(gates, sigmoids, ups)]
        mean = sum(jnp.sum(hidden, -1, keepdims=True) for hidden in hiddens) / hidden_all
        centres = [hidden - mean for hidden in hiddens]
        spread = sum(jnp.sum(centre * centre, -1, keepdims=True) for centre in centres) / hidden_all
        inverse_three = lax.rsqrt(spread + EPSILON)
        hats = [centre * inverse_three for centre in centres]
        lows = [
            (hat * inner_all[half, 0:1] + inner_all[half, 1:2]).astype(BF)
            for hat, half in zip(hats, halves)
        ]
        branch = sum(dot(low, down_low[half], NN) for low, half in zip(lows, halves))
        extra[5:6] += column_sums(branch * branch)
        residual[image] = middle + branch

        @pl.when(image == 0)
        def _():
            forward_pairs(1, 1)
            forward_pairs(1, 2)
            for tile in range(3):
                send_pairs(2, tile)

        cotangent = out_grad[image, own_rows] * mask[image, own_rows]
        grads = [grad_down[image, index] for index in range(2)]
        for half, grad, hat in zip(halves, grads, hats):
            inner_sums[half, 0:1] += column_sums(grad * hat)
            inner_sums[half, 1:2] += column_sums(grad)
        scaled = [grad * inner_all[half, 0:1] for grad, half in zip(grads, halves)]
        first = sum(jnp.sum(value, -1, keepdims=True) for value in scaled) / hidden_all
        second = (
            sum(jnp.sum(value * hat, -1, keepdims=True) for value, hat in zip(scaled, hats)) / hidden_all
        )
        grad_hiddens = [
            inverse_three * (value - first - hat * second) for value, hat in zip(scaled, hats)
        ]
        gate_rows = [
            (grad * up * (sigmoid + gate * sigmoid * (1.0 - sigmoid))).astype(BF)
            for grad, up, sigmoid, gate in zip(grad_hiddens, ups, sigmoids, gates)
        ]
        up_rows = [
            (grad * gate * sigmoid).astype(BF)
            for grad, gate, sigmoid in zip(grad_hiddens, gates, sigmoids)
        ]
        for number, pair in enumerate((lows, gate_rows, up_rows)):
            wide_rows[me_t, image, :, number * wide : number * wide + wide] = pair[0]
            wide_rows_send[image, :, number * wide : number * wide + wide] = pair[1]
        grad_two = sum(
            dot(gate_row, gate_up_low[half, 0], NT) + dot(up_row, gate_up_low[half, 1], NT)
            for gate_row, up_row, half in zip(gate_rows, up_rows, halves)
        )
        extra[2:3] += column_sums(grad_two * hat_two)
        extra[3:4] += column_sums(grad_two)
        back = cotangent + norm_back(grad_two, hat_two, inverse_two, gain_two)
        grad_middle[image] = back
        low = back.astype(BF)
        slim_rows[me_t, image, :, width:] = low
        grad_attended[me_t, image] = dot(low, out_low[me_t], NT).astype(BF)
        grad_attended_send[image] = dot(low, out_low[other], NT).astype(BF)
        datt_copy(image).start()
        for copy in row_copies(image):
            copy.start()

    def attend_back(image):
        datt_copy(image).wait_recv()
        grad_attended_all[...] = jnp.concatenate(
            [grad_attended[half, image].astype(F32) for half in range(2)], 0
        )
        wides = [half_of(grad_attended_all[:, 0:128], 1)]
        wides += [half_of(grad_attended_all[:, 128:256], half) for half in range(2)]
        lows = [wide.astype(BF) for wide in wides]
        mixed = attended_low[image].astype(F32)
        deltas = [
            jnp.sum(wide * mixed[:, tile * 128 : tile * 128 + 128], -1, keepdims=True)
            for wide, tile in zip(wides, (0, 1, 1))
        ]

        def grad_chance(head):
            scores[head % 2] = dot(lows[head], key_tile(image, 1 + (head + 1) // 2), NT)

        def grad_score(head):
            for start in range(0, seq_rows, CHUNK):
                rows = slice(start, start + CHUNK)
                chance = probs[image * heads + head, rows].astype(F32)
                grad_scores[head, rows] = (chance * (scores[head % 2, rows] - deltas[head][rows])).astype(BF)

        def value_grad(head):
            start = (head + 1) % 2 * DH
            rows = jnp.transpose(wides[head])[start : start + DH].astype(BF)
            place = (heads + head) * DH
            grad_pairs[place : place + DH] = dot(rows, probs[image * heads + head], NN)

        def key_grad(head):
            place = head * DH
            grad_pairs[place : place + DH] = dot(queries_t[image * heads + head], grad_scores[head], NN)

        def query_grad(head):
            return dot(grad_scores[head], key_tile(image, head // 2), NN)

        grad_chance(0)
        grad_chance(1)
        value_grad(0)
        grad_score(0)
        grad_chance(2)
        value_grad(1)
        grad_score(1)
        query_grads = [query_grad(0)]
        key_grad(0)
        value_grad(2)
        grad_score(2)
        query_grads.append(query_grad(1))
        key_grad(1)
        query_grads.append(query_grad(2))
        key_grad(2)
        grad_query[:, 0:128] = halves_of(query_grads[0], query_grads[1])
        grad_query[:, 128:256] = half_of(query_grads[2], 0)

        pairs_send[image] = jnp.transpose(grad_pairs[...]).astype(BF).reshape(ns, seq_rows, width)

        @pl.when(image == 0)
        def _():
            forward_pairs(2, 1)
            forward_pairs(2, 2)

        for kind in range(4):
            back_copy(image, kind).start()
        raw = grad_query[...] * (DH ** (-0.5))
        raw = turn_queries(raw, cosine[...], -sine[...])
        grad_query_low[image] = raw.astype(BF)

    def weights(image):
        for copy in row_copies(image):
            copy.wait_recv()
        for half in range(2):
            place = slice(half * own, half * own + own)
            grad_branch = (out_grad[image, place] * mask[image, place]).astype(BF)
            normed_three, grad_gate, grad_up = (
                wide_rows[half, image, :, number * wide : number * wide + wide] for number in range(3)
            )
            full_down[...] += dot(normed_three, grad_branch, TN) * scale
            rows_two, low = slim_rows[half, image, :, 0:width], slim_rows[half, image, :, width:]
            full_gate_up[0] += dot(rows_two, grad_gate, TN) * scale
            full_gate_up[1] += dot(rows_two, grad_up, TN) * scale
            mixed = attended_low[image].astype(F32)[place].astype(BF)
            full_out[...] += dot(mixed, low, TN)[256 - narrow :] * scale

    def stage(step, carry):
        @pl.when(step < images)
        def _():
            attend(step)

        @pl.when(step == images)
        def _():
            for load in loads[7:10]:
                load.wait()
            lax.fori_loop(0, images - 1, lambda image, rest: weights(image) or rest, 0)
            relay_back(1)

        @pl.when(step >= 1)
        def _():
            attend_back(step - 1)

        @pl.when(step < images)
        def _():
            feed(step)

        return carry

    lax.fori_loop(0, images + 1, stage, 0)
    inner_copy().start()

    weights(images - 1)

    taken = []

    def take(count):
        taken.append(count)
        return sum(taken) - count

    def low_exchange(axis, size, buffers):
        base = take((size - 1) * len(buffers))
        return exchange(axis, size, buffers, low_send, low_recv, base)

    def low_scatter(pieces, inbox):
        return scatter("seq", ns, pieces, inbox, low_send, low_recv, take(ns - 1))

    share = 1.0 / (ns * nd)
    early = early_t.at[me_t]
    early[0] = fine_dot(basis_out[...], full_out[...], NN)
    for index in range(2):
        early[1 + index] = fine_dot(basis_gate_up[index], full_gate_up[index], NT)
    early[3] = fine_dot(basis_down[...], full_down[...], NN)
    early[4] = extra[...]
    early_moves = low_exchange("tensor", nt, (early_t,))

    sum_query[...] = jnp.zeros_like(sum_query)
    sum_pairs[...] = jnp.zeros_like(sum_pairs)

    def pairs_of(image):
        for kind in range(2, 6):
            back_copy(image, kind).wait_recv()
        pairs = pairs_send[image, me_s].astype(F32)
        pairs = pairs + pairs_x[image].astype(F32) + pairs_y[image].astype(F32)
        pairs = turn_pairs(pairs, cosine[...], -sine[...]).astype(BF)
        rows = dot(thin_query[...], grad_query_low[image], NT) + dot(thin_pairs[...], pairs, NT)
        late_sum[...] += fold(dot(two_rows(fold(rows)), normed_one_all[image], NN)) * scale
        return pairs

    def finish_pairs(image, pairs):
        query = grad_query_low[image]
        grad_one[image] = dot(query, query_low[...], NN) + dot(pairs, key_value_low[...], NN)
        final_copy(image).start()
        sum_query[...] += dot(query, normed_one_all[image], TN)
        sum_pairs[...] += dot(pairs, normed_one_all[image], TN)

    finish_pairs(0, pairs_of(0))
    arrive(early_moves)
    summed = total(early_t, nt)
    early_all[...] = summed[0:4]
    early_moves = low_scatter(early_all, early_in)
    inner_copy().wait_recv()
    tiny_s[me_s] = jnp.zeros_like(tiny_s[me_s])
    tiny_s[me_s, 0:2] = ((inner_sums[me_t] + inner_recv[...]) * scale)[0:2]
    tiny_s[me_s, 2:6, 0:width] = summed[4, 2:6]
    tiny_moves = low_exchange("seq", ns, (tiny_s,))
    relay_back(images - 1)
    finish_pairs(1, pairs_of(1))
    arrive(early_moves)
    early_d[me_d] = total(early_in, ns)
    early_moves = low_exchange("dp", nd, (early_d,))
    arrive(tiny_moves)
    tiny_d[me_d] = total(tiny_s, ns)
    tiny_moves = low_exchange("dp", nd, (tiny_d,))
    pairs = pairs_of(images - 1)
    late_t[me_t] = late_sum[...]
    late_moves = low_exchange("tensor", nt, (late_t,))
    finish_pairs(images - 1, pairs)
    arrive(late_moves)
    late_s[me_s] = total(late_t, nt)
    late_moves = low_exchange("seq", ns, (late_s,))
    full_qkv[0] += sum_query[0:narrow] * scale
    full_qkv[1] += sum_pairs[0:narrow] * scale
    full_qkv[2] += sum_pairs[narrow : 2 * narrow] * scale

    norm_t[me_t] = jnp.zeros_like(norm_t[me_t])

    def finish(image, carry):
        final_copy(image).wait_recv()
        grad = grad_one[image, own_rows] + grad_one_recv[image]
        _, hat_one, inverse_one = norm_parts(tokens[image].astype(F32), gain_one, bias_one)
        input_grad[image] = grad_middle[image] + norm_back(grad, hat_one, inverse_one, gain_one)
        norm_t[me_t, 0:1] += column_sums(grad * hat_one)
        norm_t[me_t, 1:2] += column_sums(grad)
        return carry

    def orthonormal(rows):
        return gram_schmidt(rows.reshape(1, RANK, width))[0]

    arrive(early_moves)
    early_left[me_s] = orthonormal(total(early_d, nd))
    early_moves = low_exchange("seq", ns, (early_left,))
    arrive(late_moves)
    late_d[me_d] = total(late_s, ns)
    late_moves = low_exchange("dp", nd, (late_d,))
    lax.fori_loop(0, images, finish, 0)
    norm_moves = low_exchange("tensor", nt, (norm_t,))
    arrive(early_moves)
    right_all[0, :, 0:narrow] = fine_dot(early_left[0], full_out[...], NT)
    right_all[0, :, narrow:] = jnp.zeros((RANK, wide - narrow), F32)
    for index in range(2):
        right_all[1 + index] = fine_dot(early_left[1 + index], full_gate_up[index], NN)
    right_all[3] = fine_dot(early_left[3], full_down[...], NT)
    early_moves = low_scatter(right_all, right_in)
    for index in range(4):
        factor_left[1 + index] = early_left[index]
    arrive(norm_moves)
    norm_s[me_s] = total(norm_t, nt)[0:2]
    arrive(late_moves)
    left = orthonormal(total(late_d, nd))
    for index in range(3):
        slim_s[me_s, 8 * index : 8 * index + 8] = fine_dot(left, full_qkv[index], NT)
    late_moves = low_exchange("seq", ns, (slim_s, norm_s))
    factor_left[0] = left
    arrive(early_moves)
    right_d[me_d] = total(right_in, ns)
    early_moves = low_exchange("dp", nd, (right_d,))
    for load in loads[10:14]:
        load.wait()
    arrive(tiny_moves)
    tiny = total(tiny_d, nd)
    squares[...] = tiny[4:6, 0:width]
    arrive(late_moves)
    slim_d[me_d] = total(slim_s, ns)
    norm_d[me_d] = total(norm_s, ns)
    late_moves = low_exchange("dp", nd, (slim_d, norm_d))
    fresh = MOMENTUM * moment_norm[2:4] + tiny[2:4, 0:width] * (share * scale)
    new_moment_norm[2:4] = fresh
    new_norm_pack[2:4] = norm_pack[2:4] - STEP_RATE * fresh
    fresh = MOMENTUM * moment_inner[...] + tiny[0:2] * share
    new_moment_inner[...] = fresh
    new_inner_pack[...] = inner_pack[...] - STEP_RATE * fresh
    arrive(early_moves)
    right_sum[me_s] = total(right_d, nd) * share
    early_moves = low_exchange("seq", ns, (right_sum,))
    arrive(early_moves)
    factor_out[...] = right_sum[0, :, 0:narrow]
    for index in range(2):
        factor_gate_up[index] = right_sum[1 + index]
    factor_down[...] = right_sum[3]
    arrive(late_moves)
    slim = total(slim_d, nd) * share
    for index in range(3):
        factor_qkv[index] = slim[8 * index : 8 * index + 8]
    fresh = MOMENTUM * moment_norm[0:2] + total(norm_d, nd) * (share * scale)
    new_moment_norm[0:2] = fresh
    new_norm_pack[0:2] = norm_pack[0:2] - STEP_RATE * fresh

    for image in range(images):
        for copy in (
            one_copy(image), att_copy(image), datt_copy(image), *row_copies(image), final_copy(image),
            *(pair_copy(image, tile, kind) for tile in range(3) for kind in range(4)),
            *(back_copy(image, kind) for kind in range(6)),
        ):
            copy.wait_send()
    for copy in (*weight_copies(), inner_copy()):
        copy.wait_send()


def block(mesh_sizes, small, hbm):
    nd, ns, nt = mesh_sizes
    images, own, width = hbm[0].shape
    seq_rows = 2 * own
    slots = ns * seq_rows
    top = (own + 15) // 16 * 16
    narrow = hbm[1].shape[1]
    heads = narrow // DH
    wide = small[2].shape[1]
    shape = jax.ShapeDtypeStruct
    matrices = ((3, narrow, width), (narrow, width), (2, width, wide), (wide, width))
    shapes = (
        (images, own, width), (images, own, width),
        (5, RANK, width), (3, RANK, narrow), (RANK, narrow), (2, RANK, wide), (RANK, wide),
        *matrices, *matrices, (4, width), (2, wide), *matrices, (4, width), (2, wide), (2, width),
    )
    outs = [pltpu.VMEM(dims, F32) for dims in shapes]
    vmem = pl.BlockSpec(memory_space=pltpu.VMEM)
    hbm_spec = pl.BlockSpec(memory_space=pltpu.HBM)
    dma = pltpu.SemaphoreType.DMA
    scratch = [
        pltpu.VMEM((2, images, own, width), BF),
        pltpu.VMEM((images, seq_rows, width), BF),
        pltpu.VMEM((images, 3, ns, seq_rows, 128), BF),
        pltpu.VMEM((images * heads, seq_rows, 128), BF),
        pltpu.VMEM((images * heads, seq_rows, slots), BF),
        pltpu.VMEM((2, seq_rows, slots), F32),
        pltpu.VMEM((heads, seq_rows, slots), BF),
        pltpu.VMEM((seq_rows, 256), F32),
        pltpu.VMEM((images, seq_rows, 256), BF),
        pltpu.VMEM((2, images, own, 256), BF),
        pltpu.VMEM((images, own, 256), BF),
        pltpu.VMEM((2, 256, width), BF),
        pltpu.VMEM((2, 2, width, wide), BF),
        pltpu.VMEM((2, wide, width), BF),
        pltpu.VMEM((2, 8, wide), F32),
        pltpu.VMEM((256, width), BF),
        pltpu.VMEM((2 * narrow, width), BF),
        pltpu.VMEM((2, images, own, 2 * width), BF),
        pltpu.VMEM((images, own, width), F32),
        pltpu.VMEM((2, images, own, 3 * wide), BF),
        pltpu.VMEM((images, own, 3 * wide), BF),
        pltpu.VMEM((images, 2, own, wide), F32),
        pltpu.VMEM((images * heads, DH, seq_rows), BF),
        pltpu.VMEM((2, images, own, 256), BF),
        pltpu.VMEM((images, own, 256), BF),
        pltpu.VMEM((seq_rows, 256), F32),
        pltpu.VMEM((seq_rows, 256), F32),
        pltpu.VMEM((images, seq_rows, 256), BF),
        pltpu.VMEM((width, slots), F32),
        *[
            pltpu.VMEM((images, *rows, width), BF)
            for rows in ((ns, seq_rows), (seq_rows,), (seq_rows,), (top,), (seq_rows - top,))
        ],
        pltpu.VMEM((images, seq_rows, width), F32),
        pltpu.VMEM((images, own, width), F32),
        pltpu.VMEM((256, width), F32),
        pltpu.VMEM((2 * narrow, width), F32),
        pltpu.VMEM((2, 8, wide), F32),
        pltpu.VMEM((8, wide), F32),
        pltpu.VMEM(hbm[0].shape, BF),
        pltpu.VMEM(hbm[5].shape, F32),
        pltpu.VMEM((images, seq_rows, 1), F32),
        pltpu.VMEM((seq_rows, 128), F32),
        pltpu.VMEM((seq_rows, 128), F32),
        pltpu.VMEM((8, width), F32),
        pltpu.VMEM((slots, 8), F32),
        pltpu.VMEM((RANK, width), F32),
        pltpu.VMEM((2 * RANK, 256), BF),
        pltpu.VMEM((2 * RANK, 2 * narrow), BF),
        pltpu.VMEM((nt, 5, RANK, width), F32),
        pltpu.VMEM((4, RANK, width), F32),
        *[pltpu.VMEM((size, RANK, width), F32) for size in (ns, nd, ns)],
        *[pltpu.VMEM((size, RANK, width), F32) for size in (nt, ns, nd)],
        pltpu.VMEM((nt, RANK, width), F32),
        *[pltpu.VMEM((size, 2, width), F32) for size in (ns, nd)],
        *[pltpu.VMEM((size, RANK, wide), F32) for size in (4, ns, nd, ns)],
        *[pltpu.VMEM((size, 3 * RANK, narrow), F32) for size in (ns, nd)],
        *[pltpu.VMEM((size, RANK, wide), F32) for size in (ns, nd)],
        dma((14,)),
        *[dma((images,))] * 2,
        *[dma((4,))] * 2,
        *[dma((images, 3, 4))] * 2,
        *[dma((images,))] * 4,
        *[dma((images, 2))] * 2,
        *[dma((images, 6))] * 2,
        *[dma((images + 1,))] * 2,
        *[dma((3 * (nt - 1) + 8 * (ns - 1) + 6 * (nd - 1),))] * 2,
    ]
    return pl.pallas_call(
        functools.partial(block_kernel, mesh_sizes, images),
        out_shape=outs,
        in_specs=[vmem] * len(small) + [hbm_spec] * len(hbm),
        out_specs=[vmem] * len(outs),
        scratch_shapes=scratch,
        compiler_params=pltpu.CompilerParams(
            collective_id=0, has_side_effects=True, vmem_limit_bytes=(LIMIT + nd // 8) * 2**20
        ),
        name="block",
    )(*small, *hbm)


def per_device(
    tokens,
    out_grad,
    keep_mask,
    w_qkv,
    w_out,
    w_gate_up,
    w_down,
    norm_pack,
    inner_pack,
    moment_qkv,
    moment_out,
    moment_gate_up,
    moment_down,
    moment_norm,
    moment_inner,
    error_qkv,
    error_out,
    error_gate_up,
    error_down,
    basis_qkv,
    basis_out,
    basis_gate_up,
    basis_down,
):
    own_rows, images, width = tokens.shape
    slot_count = keep_mask.shape[0]
    sizes = tuple(lax.axis_size(axis) for axis in ("dp", "seq", "tensor"))

    def turn(array):
        return jnp.swapaxes(array, -1, -2)

    results = block(
        sizes,
        (
            jnp.transpose(keep_mask), norm_pack, inner_pack, moment_norm, moment_inner,
            *(turn(basis) for basis in (basis_qkv, basis_out, basis_gate_up, basis_down)),
        ),
        (
            jnp.swapaxes(tokens, 0, 1), turn(w_qkv), w_out, w_gate_up, w_down, jnp.swapaxes(out_grad, 0, 1),
            turn(error_qkv[0]), error_out[0], error_gate_up[0], error_down[0],
            turn(moment_qkv), moment_out, moment_gate_up, moment_down,
        ),
    )
    grads, lows, fulls, moments = results[0:2], results[2:7], results[7:11], results[11:15]
    (
        residual, input_grad, new_moment_norm, new_moment_inner, new_norm_pack, new_inner_pack,
        factor_left, factor_qkv, factor_out, factor_gate_up, factor_down,
        new_error_qkv, new_error_out, new_error_gate_up, new_error_down,
        new_moment_qkv, new_moment_out, new_moment_gate_up, new_moment_down,
        new_w_qkv, new_w_out, new_w_gate_up, new_w_down,
        branch_rms,
    ) = store(
        (*grads, *results[15:17], *results[21:23]), results[23], lows, fulls, moments, results[17:21],
        float(slot_count * images * lax.axis_size("dp") * width),
    )
    return (
        jnp.swapaxes(residual, 0, 1), jnp.swapaxes(input_grad, 0, 1),
        *(turn(factor) for factor in (factor_left, factor_qkv, factor_out, factor_gate_up, factor_down)),
        turn(new_error_qkv)[None], new_error_out[None], new_error_gate_up[None], new_error_down[None],
        turn(new_moment_qkv), new_moment_out, new_moment_gate_up, new_moment_down, new_moment_norm, new_moment_inner,
        turn(new_w_qkv), new_w_out, new_w_gate_up, new_w_down, new_norm_pack, new_inner_pack,
        branch_rms,
    )


def solution(mesh):
    placed = (
        P(("seq", "tensor"), "dp", None),
        P("seq", "dp", None),
        P(None, "dp"),
        P(None, None, "tensor"),
        P("tensor", None),
        P(None, None, "tensor"),
        P("tensor", None),
        P(),
        P(None, "tensor"),
        P(None, None, "tensor"),
        P("tensor", None),
        P(None, None, "tensor"),
        P("tensor", None),
        P(),
        P(None, "tensor"),
        P(("dp", "seq"), None, None, "tensor"),
        P(("dp", "seq"), "tensor", None),
        P(("dp", "seq"), None, None, "tensor"),
        P(("dp", "seq"), "tensor", None),
        P(None, "tensor", None),
        P("tensor", None),
        P(None, "tensor", None),
        P("tensor", None),
    )
    return jax.shard_map(
        per_device,
        mesh=mesh,
        in_specs=placed,
        out_specs=(
            P(("seq", "tensor"), "dp", None),
            P(("seq", "tensor"), "dp", None),
            P(),
            P(None, "tensor", None),
            P("tensor", None),
            P(None, "tensor", None),
            P("tensor", None),
            P(("dp", "seq"), None, None, "tensor"),
            P(("dp", "seq"), "tensor", None),
            P(("dp", "seq"), None, None, "tensor"),
            P(("dp", "seq"), "tensor", None),
            P(None, None, "tensor"),
            P("tensor", None),
            P(None, None, "tensor"),
            P("tensor", None),
            P(),
            P(None, "tensor"),
            P(None, None, "tensor"),
            P("tensor", None),
            P(None, None, "tensor"),
            P("tensor", None),
            P(),
            P(None, "tensor"),
            P(),
        ),
        check_vma=False,
    )
```

```python
import functools
import math

import jax
import jax.numpy as jnp
from jax import lax
from jax.experimental import pallas as pl
from jax.experimental.pallas import tpu as pltpu
from jax.sharding import PartitionSpec as P

DH = 64
FF = 1024
GRID = 32
RANK = 8
QUARTER = DH // 4
CHUNK = 16
LIMIT = 46


EPSILON = 1e-06
MOMENTUM = 0.9
STEP_RATE = 0.5
MESH = pl.DeviceIdType.MESH
BF = jnp.bfloat16
F32 = jnp.float32


def split(value):
    high = value.astype(BF)
    return high, (value - high.astype(F32)).astype(BF)


def dot(left, right, dims):
    return lax.dot_general(left, right, (dims, ((), ())), preferred_element_type=F32)


NN = ((1,), (0,))
NT = ((1,), (1,))
TN = ((0,), (0,))


def two_rows(rows):
    high, low = split(rows)
    return jnp.concatenate([high.astype(F32), low.astype(F32)], 0).astype(BF)


def fold(rows):
    return rows[0:RANK] + rows[RANK:]


def fine_dot(left, right, dims):
    right_high, right_low = split(right)
    return fold(dot(two_rows(left), right_high, dims)) + dot(left.astype(BF), right_low, dims)


def gram_schmidt(stack):
    rows = lax.broadcasted_iota(jnp.int32, (1, RANK, 1), 1)
    for index in range(RANK):
        column = stack[:, index : index + 1, :]
        products = jnp.sum(stack * column, -1, keepdims=True)
        scale = lax.rsqrt(products[:, index : index + 1, :] + EPSILON)
        done = column * scale
        rest = stack - (products * scale) * done
        stack = jnp.where(rows < index, stack, jnp.where(rows == index, done, rest))
    return stack


class Moves:
    def __init__(self, span, send, receive, device):
        self.whole = pltpu.make_async_remote_copy(
            src_ref=span, dst_ref=span, send_sem=send, recv_sem=receive, device_id=device, device_id_type=MESH
        )

    def arrive(self):
        self.whole.wait()


def exchange(axes, sizes, buffer, send, receive, pieces=None):
    count = math.prod(sizes)
    place = 0
    for axis, size in zip(axes, sizes):
        place = place * size + lax.axis_index(axis)
    for step in range(1, count):
        peer = lax.rem(place + step, count)
        device, rest = {}, peer
        for axis, size in reversed(tuple(zip(axes, sizes))):
            device[axis] = lax.rem(rest, size)
            rest = lax.div(rest, size)
        pltpu.make_async_remote_copy(
            src_ref=buffer.at[place] if pieces is None else pieces.at[peer],
            dst_ref=buffer.at[place],
            send_sem=send,
            recv_sem=receive,
            device_id=device,
            device_id_type=MESH,
        ).start()
    return Moves(buffer.at[0 : count - 1], send, receive, device)


def arrive(moves):
    for move in moves:
        move.arrive()


def total(buffer, size):
    value = buffer[0].astype(F32)
    for index in range(1, size):
        value = value + buffer[index].astype(F32)
    return value


def greet(axes, barrier):
    for axis, size in axes:
        me = lax.axis_index(axis)
        for step in range(1, size):
            pl.semaphore_signal(
                barrier, inc=1, device_id={axis: lax.rem(me + step, size)}, device_id_type=MESH
            )


def triple_first(rows):
    high, low = split(rows)
    return jnp.concatenate([high.astype(F32), high.astype(F32), low.astype(F32)], 0)


def triple_second(rows):
    high, low = split(rows)
    return jnp.concatenate([high.astype(F32), low.astype(F32), high.astype(F32)], 0)


def store_kernel(total_rows, plain, *refs):
    sources, rest = refs[:plain], refs[plain:]
    squares, factor_left, factor_qkv, factor_out, factor_gate_up, factor_down = rest[:6]
    fulls, moments, weights = rest[6:10], rest[10:14], rest[14:18]
    targets, rest = rest[18 : 18 + plain], rest[18 + plain :]
    results, branch_rms, fresh, sems = rest[:12], rest[12], rest[13:25], rest[25]
    copies = [
        pltpu.make_async_copy(source, target, sems.at[number])
        for number, (source, target) in enumerate(zip(sources, targets))
    ]
    for copy in copies:
        copy.start()

    def settle(number, approx, pick):
        full, moment, weight = (pick(group[number]) for group in (fulls, moments, weights))
        places = (number, 4 + number, 8 + number)
        error_to, moment_to, weight_to = (pick(fresh[place]) for place in places)
        error_to[...] = full[...] - approx
        momentum = MOMENTUM * moment[...] + approx
        moment_to[...] = momentum
        weight_to[...] = weight[...] - STEP_RATE * momentum
        for place in places:
            copy = pltpu.make_async_copy(pick(fresh[place]), pick(results[place]), sems.at[len(copies)])
            copy.start()
            copies.append(copy)

    def product(rows, columns):
        return dot(rows.astype(BF), columns.astype(BF), TN)

    lefts = [triple_first(factor_left[index]) for index in range(5)]
    for index in range(2):
        settle(2, product(lefts[2 + index], triple_second(factor_gate_up[index])), lambda ref: ref.at[index])
    settle(3, product(triple_second(factor_down[...]), lefts[4]), lambda ref: ref)
    settle(1, product(triple_second(factor_out[...]), lefts[1]), lambda ref: ref)
    for index in range(3):
        settle(0, product(triple_second(factor_qkv[index]), lefts[0]), lambda ref: ref.at[index])
    roots = jnp.sqrt(jnp.sum(squares[...], -1, keepdims=True) / total_rows)
    for index in range(2):
        branch_rms[index] = roots[index, 0]
    for copy in copies:
        copy.wait()


def store(plain, squares, factors, fulls, moments, weights, total_rows):
    vmem = pl.BlockSpec(memory_space=pltpu.VMEM)
    matrices = [*fulls, *moments, *weights]
    shapes = [jax.ShapeDtypeStruct(array.shape, F32) for array in (*plain, *factors, *matrices)]
    count = len(plain) + len(factors)
    return pl.pallas_call(
        functools.partial(store_kernel, total_rows, count),
        out_shape=[*shapes, jax.ShapeDtypeStruct((2,), F32)],
        in_specs=[vmem] * (count + 1 + len(factors) + 12),
        out_specs=[*[pl.BlockSpec(memory_space=pltpu.HBM)] * len(shapes), pl.BlockSpec(memory_space=pltpu.SMEM)],
        scratch_shapes=[
            *[pltpu.VMEM(array.shape, F32) for array in matrices],
            pltpu.SemaphoreType.DMA((count + 21,)),
        ],
        compiler_params=pltpu.CompilerParams(vmem_limit_bytes=24 * 2**20),
        name="store",
    )(*plain, *factors, squares, *factors, *matrices)


def swap_quarters(tile):
    lane = lax.broadcasted_iota(jnp.int32, (1, 128), 1)
    low = lax.rem(lax.div(lane, QUARTER), 2) == 0
    return jnp.where(low, pltpu.roll(tile, 128 - QUARTER, 1), pltpu.roll(tile, QUARTER, 1))


def turn_pairs(pairs, cosine, sine):
    keys = lax.broadcasted_iota(jnp.int32, (1, 128), 1) < DH
    first, second, third = (pairs[:, start : start + 128] for start in (0, 128, 256))
    first = first * cosine + swap_quarters(first) * sine
    second = jnp.where(keys, second * cosine + swap_quarters(second) * sine, second)
    return jnp.concatenate([first, second, third], -1)


def turn_queries(raw, cosine, sine):
    tiles = (raw[:, start : start + 128] for start in (0, 128))
    return jnp.concatenate([tile * cosine + swap_quarters(tile) * sine for tile in tiles], -1)


def angle_tables(first_slot, count):
    slots = first_slot + lax.broadcasted_iota(jnp.int32, (count, 128), 0)
    place = lax.rem(lax.broadcasted_iota(jnp.int32, (count, 128), 1), DH)
    inside = jnp.logical_and(slots >= 1, slots <= GRID * GRID)
    patch = jnp.where(inside, slots - 1, 0)
    quarter = lax.div(place, QUARTER)
    position = jnp.where(quarter < 2, lax.div(patch, GRID), lax.rem(patch, GRID)).astype(F32)
    power = lax.rem(place, QUARTER).astype(F32)
    angles = position * jnp.exp(power * (-math.log(10000.0) / QUARTER)) * (16.0 / GRID)
    sine = jnp.sin(angles)
    return jnp.cos(angles), jnp.where(lax.rem(quarter, 2) == 0, -sine, sine)


def norm_parts(values, gain, bias):
    centre = values - jnp.mean(values, -1, keepdims=True)
    spread = jnp.mean(centre * centre, -1, keepdims=True)
    inverse = lax.rsqrt(spread + EPSILON)
    normed = centre * inverse
    return (normed * gain + bias, normed, inverse)


def norm_back(grad, normed, inverse, gain):
    scaled = grad * gain
    return inverse * (
        scaled
        - jnp.mean(scaled, -1, keepdims=True)
        - normed * jnp.mean(scaled * normed, -1, keepdims=True)
    )


def column_sums(value):
    return jnp.sum(value, 0, keepdims=True)


def block_kernel(sizes, images, *refs):
    (
        keep, norm_pack, inner_pack, moment_norm, moment_inner, basis_qkv, basis_out, basis_gate_up, basis_down,
        tokens_hbm, w_qkv_hbm, w_out_hbm, w_gate_up_hbm, w_down_hbm, out_grad_hbm,
        error_qkv_hbm, error_out_hbm, error_gate_up_hbm, error_down_hbm,
        moment_qkv_hbm, moment_out_hbm, moment_gate_up_hbm, moment_down_hbm,
        residual, input_grad, factor_left, factor_qkv, factor_out, factor_gate_up, factor_down,
        full_qkv, full_out, full_gate_up, full_down,
        moment_qkv, moment_out, moment_gate_up, moment_down, new_moment_norm, new_moment_inner,
        w_qkv, w_out, w_gate_up, w_down, new_norm_pack, new_inner_pack, squares,
        normed_one, normed_one_all, keys_values, queries, probs, scores, grad_scores,
        attended, attended_low, attended_in, attended_send,
        out_low, gate_up_low, down_low, inner_all, query_low, key_value_low,
        slim_rows, grad_middle, wide_rows, wide_rows_send, grad_down, queries_t,
        grad_attended, grad_attended_send, grad_attended_all, grad_query, grad_query_low, grad_pairs,
        *rest,
    ) = refs
    pairs_send, pairs_x, pairs_y, relay_x, relay_y = rest[0:5]
    ( grad_one, grad_one_recv, sum_query, sum_pairs, inner_sums, inner_recv,
        tokens, out_grad, mask, cosine, sine, extra, kept_rows, late_sum, thin_query, thin_pairs,
        early_t, early_all, early_in, early_d, early_left, late_s, late_d, norm_t, norm_s, norm_d,
        right_all, right_in, right_d, right_sum, slim_s, slim_d, tiny_s, tiny_d,
        local_sems, one_send, one_recv, weight_send, weight_recv, pair_send, pair_recv,
        att_send, att_recv, datt_send, datt_recv, rows_send, rows_recv, back_send, back_recv,
        final_send, final_recv, low_send, low_recv,
    ) = rest[5:]
    nd, ns, nt = sizes
    me_t, me_s = lax.axis_index("tensor"), lax.axis_index("seq")
    other = 1 - me_t
    near_x = me_s + 1 - 2 * lax.rem(me_s, 2)
    near_y = lax.rem(me_s + 2, 4)
    far = 3 - me_s
    me_d = lax.axis_index("dp")
    own, width = tokens.shape[1], tokens.shape[2]
    seq_rows = 2 * own
    slots = ns * seq_rows
    heads = w_qkv.shape[1] // DH
    wide = w_down.shape[0]
    hidden_all = 2 * wide
    scale = (images * seq_rows) ** (-0.5)
    top = (own + 15) // 16 * 16
    upper, lower = slice(0, top), slice(top, seq_rows)
    own_rows = pl.ds(pl.multiple_of(me_t * own, 8), own)
    other_rows = pl.ds(pl.multiple_of(other * own, 8), own)

    barrier = pltpu.get_barrier_semaphore()
    greet((("tensor", nt), ("seq", ns), ("dp", nd)), barrier)
    loads = [
        pltpu.make_async_copy(source, target, local_sems.at[number])
        for number, (source, target) in enumerate(
            (
                (tokens_hbm, tokens), (w_qkv_hbm, w_qkv),
                (w_out_hbm, w_out), (w_gate_up_hbm, w_gate_up), (w_down_hbm, w_down), (out_grad_hbm, out_grad),
                (error_qkv_hbm, full_qkv), (error_out_hbm, full_out),
                (error_gate_up_hbm, full_gate_up), (error_down_hbm, full_down),
                (moment_qkv_hbm, moment_qkv), (moment_out_hbm, moment_out),
                (moment_gate_up_hbm, moment_gate_up), (moment_down_hbm, moment_down),
            )
        )
    ]
    for load in loads[0:2]:
        load.start()

    def to_partner(source, target, send, receive):
        return pltpu.make_async_remote_copy(
            src_ref=source, dst_ref=target, send_sem=send, recv_sem=receive,
            device_id={"tensor": other}, device_id_type=MESH,
        )

    def to_seq(source, target, send, receive, peer):
        return pltpu.make_async_remote_copy(
            src_ref=source, dst_ref=target, send_sem=send, recv_sem=receive,
            device_id={"seq": peer}, device_id_type=MESH,
        )

    def one_copy(image):
        block = normed_one.at[me_t, image]
        return to_partner(block, block, one_send.at[image], one_recv.at[image])

    def weight_copies():
        return [
            to_partner(ref.at[me_t], ref.at[me_t], weight_send.at[number], weight_recv.at[number])
            for number, ref in enumerate((out_low, gate_up_low, down_low, inner_all))
        ]

    def pair_copy(image, tile, kind):
        place, peer = ((me_s, near_x), (me_s, near_y), (near_x, near_y), (near_y, near_x))[kind]
        block = keys_values.at[image, tile, place]
        if kind >= 2:
            block = block.at[(upper, lower)[kind - 2]]
        return to_seq(block, block, pair_send.at[image], pair_recv.at[image, tile, min(kind, 2)], peer)

    def send_pairs(image, tile):
        for kind in range(2):
            pair_copy(image, tile, kind).start()

    def forward_pairs(image, tile):
        for kind in range(2):
            pair_copy(image, tile, kind).wait_recv()
            pair_copy(image, tile, 2 + kind).start()

    def await_pairs(image, tile):
        block = keys_values.at[image, tile, far]
        to_seq(block, block, pair_send.at[image], pair_recv.at[image, tile, 2], far).wait_recv()

    def att_copy(image):
        return to_partner(
            attended_send.at[image], attended_in.at[me_t, image], att_send.at[image], att_recv.at[image]
        )

    def datt_copy(image):
        return to_partner(
            grad_attended_send.at[image], grad_attended.at[me_t, image], datt_send.at[image], datt_recv.at[image]
        )

    def row_copies(image):
        moves = ((slim_rows.at[me_t, image], slim_rows), (wide_rows_send.at[image], wide_rows))
        return [
            to_partner(source, target.at[me_t, image], rows_send.at[image, number], rows_recv.at[image, number])
            for number, (source, target) in enumerate(moves)
        ]

    def back_copy(image, kind):
        place, rows, target, there, peer = (
            (far, upper, relay_x, slice(0, top), near_x),
            (far, lower, relay_y, slice(0, seq_rows - top), near_y),
            (near_x, upper, pairs_x, upper, near_x),
            (near_y, lower, pairs_y, lower, near_y),
            (near_x, lower, pairs_x, lower, near_x),
            (near_y, upper, pairs_y, upper, near_y),
        )[kind]
        return to_seq(
            pairs_send.at[image, place, rows], target.at[image, there],
            back_send.at[image], back_recv.at[image, min(kind, 2)], peer,
        )

    def relay_back(image):
        for place, rows, inbox, arrival, onward in ((near_y, upper, relay_x, 0, 5), (near_x, lower, relay_y, 1, 4)):
            back_copy(image, arrival).wait_recv()
            value = pairs_send[image, place, rows].astype(F32) + inbox[image].astype(F32)
            pairs_send[image, place, rows] = value.astype(BF)
            back_copy(image, onward).start()

    def final_copy(image):
        return to_partner(
            grad_one.at[image, other_rows], grad_one_recv.at[image], final_send.at[image], final_recv.at[image]
        )

    def inner_copy():
        return to_partner(
            inner_sums.at[other], inner_recv, final_send.at[images], final_recv.at[images]
        )

    gain_one, bias_one = norm_pack[0:1], norm_pack[1:2]
    gain_two, bias_two = norm_pack[2:3], norm_pack[3:4]

    cosine[...], sine[...] = angle_tables(me_s * seq_rows, seq_rows)
    loads[0].wait()
    for image in range(images):
        normed, _, _ = norm_parts(tokens[image].astype(F32), gain_one, bias_one)
        normed_one[me_t, image] = normed.astype(BF)
        if image == 0:
            pl.semaphore_wait(barrier, (nt - 1) + (ns - 1) + (nd - 1))
        one_copy(image).start()
    for load in loads[2:]:
        load.start()
    loads[1].wait()

    narrow = heads * DH
    pad = jnp.zeros((256 - narrow, width), BF)
    query_low[...] = jnp.concatenate([w_qkv[0].astype(BF), pad], 0)
    key_value_low[0:narrow] = w_qkv[1].astype(BF)
    key_value_low[narrow : 2 * narrow] = w_qkv[2].astype(BF)

    def project(image, carry):
        one_copy(image).wait_recv()
        blocks = [normed_one[half, image] for half in range(2)]
        pairs = jnp.concatenate([dot(block, key_value_low[...], NT) for block in blocks], 0)
        pairs = turn_pairs(pairs, cosine[...], sine[...])
        for tile in range(3):
            keys_values[image, tile, me_s] = pairs[:, 128 * tile : 128 * tile + 128].astype(BF)

        @pl.when(image == 0)
        def _():
            for tile in range(3):
                send_pairs(image, tile)

        raw = jnp.concatenate([dot(block, query_low[...], NT) for block in blocks], 0)
        raw = turn_queries(raw, cosine[...], sine[...]) * (DH ** (-0.5))
        lane = lax.broadcasted_iota(jnp.int32, (1, 128), 1)
        for head in range(heads):
            tile = raw[:, head // 2 * 128 : head // 2 * 128 + 128]
            queries[image * heads + head] = jnp.where(lax.div(lane, DH) == head % 2, tile, 0.0).astype(BF)
        normed_one_all[image] = jnp.concatenate([block.astype(F32) for block in blocks], 0).astype(BF)
        return carry

    lax.fori_loop(0, images, project, 0)

    for load in loads[2:5]:
        load.wait()
    out_low[me_t] = jnp.concatenate([pad, w_out[...].astype(BF)], 0)
    for index in range(2):
        gate_up_low[me_t, index] = w_gate_up[index].astype(BF)
    down_low[me_t] = w_down[...].astype(BF)
    inner_all[me_t] = jnp.zeros_like(inner_all[me_t])
    inner_all[me_t, 0:2] = inner_pack[...]
    for copy in weight_copies():
        copy.start()
    kept = jnp.concatenate([keep[...].astype(F32), jnp.zeros((8 - images, slots), F32)], 0)
    kept_rows[...] = jnp.transpose(kept)
    kept = kept_rows[pl.ds(pl.multiple_of(me_s * seq_rows, 8), seq_rows)]
    for image in range(images):
        mask[image] = kept[:, image : image + 1]
    loads[5].wait()
    loads[6].wait()
    late_sum[...] = sum(fine_dot(basis_qkv[index], full_qkv[index], NN) for index in range(3))
    gap = jnp.zeros((RANK, 256 - narrow), F32)
    thin_query[...] = two_rows(jnp.concatenate([basis_qkv[0], gap], -1))
    thin_pairs[...] = two_rows(jnp.concatenate([basis_qkv[1], basis_qkv[2]], -1))
    extra[...] = jnp.zeros_like(extra)
    inner_sums[...] = jnp.zeros_like(inner_sums)

    def halves_of(lower, upper):
        lane = lax.broadcasted_iota(jnp.int32, (1, 128), 1)
        return jnp.where(lane < DH, lower, upper)

    def half_of(value, half):
        return halves_of(value, 0.0) if half == 0 else halves_of(0.0, value)

    def key_tile(image, index):
        return keys_values[image, index].reshape(slots, 128)

    def attend(image):
        @pl.when(image == 0)
        def _():
            forward_pairs(0, 0)
            forward_pairs(0, 1)
            forward_pairs(0, 2)
            for tile in range(3):
                send_pairs(1, tile)
            for copy in weight_copies():
                copy.wait_recv()

            def ahead(place, carry):
                cotangent = out_grad[place, own_rows] * mask[place, own_rows]
                for index, half in enumerate((me_t, other)):
                    grad_down[place, index] = dot(cotangent.astype(BF), down_low[half], NT)
                for head in range(heads):
                    turned = jnp.transpose(queries[place * heads + head].astype(F32))
                    start = head % 2 * DH
                    queries_t[place * heads + head] = turned[start : start + DH].astype(BF)
                return carry

            lax.fori_loop(0, images, ahead, 0)

        bias = jnp.where(keep[pl.ds(image, 1), :] > 0, 0.0, -1e30)

        def score(head):
            scores[head % 2] = dot(queries[image * heads + head], key_tile(image, head // 2), NT)

        def chances(head):
            for start in range(0, seq_rows, CHUNK):
                rows = slice(start, start + CHUNK)
                part = scores[head % 2, rows] + bias
                part = jnp.exp(part - jnp.max(part, -1, keepdims=True))
                part = part * (1.0 / jnp.sum(part, -1, keepdims=True))
                probs[image * heads + head, rows] = part.astype(BF)

        def mix(head):
            return dot(probs[image * heads + head], key_tile(image, 1 + (head + 1) // 2), NN)

        await_pairs(image, 0)
        score(0)
        score(1)
        chances(0)
        await_pairs(image, 1)
        score(2)
        mixed = [mix(0)]
        chances(1)
        await_pairs(image, 2)
        mixed.append(mix(1))
        chances(2)
        mixed.append(mix(2))
        attended[:, 0:128] = half_of(mixed[0], 1)
        attended[:, 128:256] = halves_of(mixed[1], mixed[2])
        attended_low[image] = attended[...].astype(BF)
        attended_in[me_t, image] = attended[own_rows].astype(BF)
        attended_send[image] = attended[other_rows].astype(BF)
        att_copy(image).start()

        @pl.when(image == 0)
        def _():
            forward_pairs(1, 0)

        @pl.when(image == 1)
        def _():
            forward_pairs(2, 0)

        @pl.when(image == 2)
        def _():
            relay_back(0)

    def feed(image):
        att_copy(image).wait_recv()
        inputs = tokens[image].astype(F32)
        branch = sum(dot(attended_in[half, image], out_low[half], NN) for half in range(2))
        middle = inputs + branch
        extra[4:5] += column_sums(branch * branch)
        normed, hat_two, inverse_two = norm_parts(middle, gain_two, bias_two)
        rows_two = normed.astype(BF)
        slim_rows[me_t, image, :, 0:width] = rows_two
        halves = (me_t, other)
        gates = [dot(rows_two, gate_up_low[half, 0], NN) for half in halves]
        ups = [dot(rows_two, gate_up_low[half, 1], NN) for half in halves]
        sigmoids = [1.0 / (1.0 + jnp.exp(-gate)) for gate in gates]
        hiddens = [gate * sigmoid * up for gate, sigmoid, up in zip(gates, sigmoids, ups)]
        mean = sum(jnp.sum(hidden, -1, keepdims=True) for hidden in hiddens) / hidden_all
        centres = [hidden - mean for hidden in hiddens]
        spread = sum(jnp.sum(centre * centre, -1, keepdims=True) for centre in centres) / hidden_all
        inverse_three = lax.rsqrt(spread + EPSILON)
        hats = [centre * inverse_three for centre in centres]
        lows = [
            (hat * inner_all[half, 0:1] + inner_all[half, 1:2]).astype(BF)
            for hat, half in zip(hats, halves)
        ]
        branch = sum(dot(low, down_low[half], NN) for low, half in zip(lows, halves))
        extra[5:6] += column_sums(branch * branch)
        residual[image] = middle + branch

        @pl.when(image == 0)
        def _():
            forward_pairs(1, 1)
            forward_pairs(1, 2)
            for tile in range(3):
                send_pairs(2, tile)

        cotangent = out_grad[image, own_rows] * mask[image, own_rows]
        grads = [grad_down[image, index] for index in range(2)]
        for half, grad, hat in zip(halves, grads, hats):
            inner_sums[half, 0:1] += column_sums(grad * hat)
            inner_sums[half, 1:2] += column_sums(grad)
        scaled = [grad * inner_all[half, 0:1] for grad, half in zip(grads, halves)]
        first = sum(jnp.sum(value, -1, keepdims=True) for value in scaled) / hidden_all
        second = (
            sum(jnp.sum(value * hat, -1, keepdims=True) for value, hat in zip(scaled, hats)) / hidden_all
        )
        grad_hiddens = [
            inverse_three * (value - first - hat * second) for value, hat in zip(scaled, hats)
        ]
        gate_rows = [
            (grad * up * (sigmoid + gate * sigmoid * (1.0 - sigmoid))).astype(BF)
            for grad, up, sigmoid, gate in zip(grad_hiddens, ups, sigmoids, gates)
        ]
        up_rows = [
            (grad * gate * sigmoid).astype(BF)
            for grad, gate, sigmoid in zip(grad_hiddens, gates, sigmoids)
        ]
        for number, pair in enumerate((lows, gate_rows, up_rows)):
            wide_rows[me_t, image, :, number * wide : number * wide + wide] = pair[0]
            wide_rows_send[image, :, number * wide : number * wide + wide] = pair[1]
        grad_two = sum(
            dot(gate_row, gate_up_low[half, 0], NT) + dot(up_row, gate_up_low[half, 1], NT)
            for gate_row, up_row, half in zip(gate_rows, up_rows, halves)
        )
        extra[2:3] += column_sums(grad_two * hat_two)
        extra[3:4] += column_sums(grad_two)
        back = cotangent + norm_back(grad_two, hat_two, inverse_two, gain_two)
        grad_middle[image] = back
        low = back.astype(BF)
        slim_rows[me_t, image, :, width:] = low
        grad_attended[me_t, image] = dot(low, out_low[me_t], NT).astype(BF)
        grad_attended_send[image] = dot(low, out_low[other], NT).astype(BF)
        datt_copy(image).start()
        for copy in row_copies(image):
            copy.start()

    def attend_back(image):
        datt_copy(image).wait_recv()
        grad_attended_all[...] = jnp.concatenate(
            [grad_attended[half, image].astype(F32) for half in range(2)], 0
        )
        wides = [half_of(grad_attended_all[:, 0:128], 1)]
        wides += [half_of(grad_attended_all[:, 128:256], half) for half in range(2)]
        lows = [wide.astype(BF) for wide in wides]
        mixed = attended_low[image].astype(F32)
        deltas = [
            jnp.sum(wide * mixed[:, tile * 128 : tile * 128 + 128], -1, keepdims=True)
            for wide, tile in zip(wides, (0, 1, 1))
        ]

        def grad_chance(head):
            scores[head % 2] = dot(lows[head], key_tile(image, 1 + (head + 1) // 2), NT)

        def grad_score(head):
            for start in range(0, seq_rows, CHUNK):
                rows = slice(start, start + CHUNK)
                chance = probs[image * heads + head, rows].astype(F32)
                grad_scores[head, rows] = (chance * (scores[head % 2, rows] - deltas[head][rows])).astype(BF)

        def value_grad(head):
            start = (head + 1) % 2 * DH
            rows = jnp.transpose(wides[head])[start : start + DH].astype(BF)
            place = (heads + head) * DH
            grad_pairs[place : place + DH] = dot(rows, probs[image * heads + head], NN)

        def key_grad(head):
            place = head * DH
            grad_pairs[place : place + DH] = dot(queries_t[image * heads + head], grad_scores[head], NN)

        def query_grad(head):
            return dot(grad_scores[head], key_tile(image, head // 2), NN)

        grad_chance(0)
        grad_chance(1)
        value_grad(0)
        grad_score(0)
        grad_chance(2)
        value_grad(1)
        grad_score(1)
        query_grads = [query_grad(0)]
        key_grad(0)
        value_grad(2)
        grad_score(2)
        query_grads.append(query_grad(1))
        key_grad(1)
        query_grads.append(query_grad(2))
        key_grad(2)
        grad_query[:, 0:128] = halves_of(query_grads[0], query_grads[1])
        grad_query[:, 128:256] = half_of(query_grads[2], 0)

        pairs_send[image] = jnp.transpose(grad_pairs[...]).astype(BF).reshape(ns, seq_rows, width)

        @pl.when(image == 0)
        def _():
            forward_pairs(2, 1)
            forward_pairs(2, 2)

        for kind in range(4):
            back_copy(image, kind).start()
        raw = grad_query[...] * (DH ** (-0.5))
        raw = turn_queries(raw, cosine[...], -sine[...])
        grad_query_low[image] = raw.astype(BF)

    def weights(image):
        for copy in row_copies(image):
            copy.wait_recv()
        for half in range(2):
            place = slice(half * own, half * own + own)
            grad_branch = (out_grad[image, place] * mask[image, place]).astype(BF)
            normed_three, grad_gate, grad_up = (
                wide_rows[half, image, :, number * wide : number * wide + wide] for number in range(3)
            )
            full_down[...] += dot(normed_three, grad_branch, TN) * scale
            rows_two, low = slim_rows[half, image, :, 0:width], slim_rows[half, image, :, width:]
            full_gate_up[0] += dot(rows_two, grad_gate, TN) * scale
            full_gate_up[1] += dot(rows_two, grad_up, TN) * scale
            mixed = attended_low[image].astype(F32)[place].astype(BF)
            full_out[...] += dot(mixed, low, TN)[256 - narrow :] * scale

    def stage(step, carry):
        @pl.when(step < images)
        def _():
            attend(step)

        @pl.when(step == images)
        def _():
            for load in loads[7:10]:
                load.wait()
            lax.fori_loop(0, images - 1, lambda image, rest: weights(image) or rest, 0)
            relay_back(1)

        @pl.when(step >= 1)
        def _():
            attend_back(step - 1)

        @pl.when(step < images)
        def _():
            feed(step)

        return carry

    lax.fori_loop(0, images + 1, stage, 0)
    inner_copy().start()

    weights(images - 1)

    taken = []
    sizes_of = {"dp": nd, "seq": ns, "tensor": nt}

    def low_exchange(axes, *buffers):
        moves = []
        for buffer in buffers:
            place = len(taken)
            taken.append(place)
            moves.append(
                exchange(axes, [sizes_of[axis] for axis in axes], buffer, low_send.at[place], low_recv.at[place])
            )
        return moves

    def low_scatter(pieces, inbox):
        place = len(taken)
        taken.append(place)
        inbox[me_s] = pieces[me_s]
        return [exchange(("seq",), (ns,), inbox, low_send.at[place], low_recv.at[place], pieces)]

    share = 1.0 / (ns * nd)
    early = early_t.at[me_t]
    early[0] = fine_dot(basis_out[...], full_out[...], NN)
    for index in range(2):
        early[1 + index] = fine_dot(basis_gate_up[index], full_gate_up[index], NT)
    early[3] = fine_dot(basis_down[...], full_down[...], NN)
    early[4] = extra[...]
    early_moves = low_exchange(("tensor",), early_t)

    sum_query[...] = jnp.zeros_like(sum_query)
    sum_pairs[...] = jnp.zeros_like(sum_pairs)

    def pairs_of(image):
        both = pairs_send.at[image, 0:2]
        to_seq(both, both, back_send.at[image], back_recv.at[image, 2], far).wait_recv()
        pairs = pairs_send[image, me_s].astype(F32)
        pairs = pairs + pairs_x[image].astype(F32) + pairs_y[image].astype(F32)
        pairs = turn_pairs(pairs, cosine[...], -sine[...]).astype(BF)
        rows = dot(thin_query[...], grad_query_low[image], NT) + dot(thin_pairs[...], pairs, NT)
        late_sum[...] += fold(dot(two_rows(fold(rows)), normed_one_all[image], NN)) * scale
        return pairs

    def finish_pairs(image, pairs):
        query = grad_query_low[image]
        grad_one[image] = dot(query, query_low[...], NN) + dot(pairs, key_value_low[...], NN)
        final_copy(image).start()
        sum_query[...] += dot(query, normed_one_all[image], TN)
        sum_pairs[...] += dot(pairs, normed_one_all[image], TN)

    finish_pairs(0, pairs_of(0))
    arrive(early_moves)
    summed = total(early_t, nt)
    early_all[...] = summed[0:4]
    early_moves = low_scatter(early_all, early_in)
    inner_copy().wait_recv()
    tiny_s[me_s] = jnp.zeros_like(tiny_s[me_s])
    tiny_s[me_s, 0:2] = ((inner_sums[me_t] + inner_recv[...]) * scale)[0:2]
    tiny_s[me_s, 2:6, 0:width] = summed[4, 2:6]
    tiny_moves = low_exchange(("seq",), tiny_s)
    relay_back(images - 1)
    finish_pairs(1, pairs_of(1))
    arrive(early_moves)
    early_d[me_d] = total(early_in, ns)
    early_moves = low_exchange(("dp",), early_d)
    arrive(tiny_moves)
    tiny_d[me_d] = total(tiny_s, ns)
    tiny_moves = low_exchange(("dp",), tiny_d)
    pairs = pairs_of(images - 1)
    late_s[me_s * nt + me_t] = late_sum[...]
    late_moves = low_exchange(("seq", "tensor"), late_s)
    finish_pairs(images - 1, pairs)
    full_qkv[0] += sum_query[0:narrow] * scale
    full_qkv[1] += sum_pairs[0:narrow] * scale
    full_qkv[2] += sum_pairs[narrow : 2 * narrow] * scale

    norm_t[me_t] = jnp.zeros_like(norm_t[me_t])

    def finish(image, carry):
        final_copy(image).wait_recv()
        grad = grad_one[image, own_rows] + grad_one_recv[image]
        _, hat_one, inverse_one = norm_parts(tokens[image].astype(F32), gain_one, bias_one)
        input_grad[image] = grad_middle[image] + norm_back(grad, hat_one, inverse_one, gain_one)
        norm_t[me_t, 0:1] += column_sums(grad * hat_one)
        norm_t[me_t, 1:2] += column_sums(grad)
        return carry

    def orthonormal(rows):
        return gram_schmidt(rows.reshape(1, RANK, width))[0]

    arrive(early_moves)
    early_left[me_s] = orthonormal(total(early_d, nd))
    early_moves = low_exchange(("seq",), early_left)
    arrive(late_moves)
    late_d[me_d] = total(late_s, ns * nt)
    late_moves = low_exchange(("dp",), late_d)
    lax.fori_loop(0, images, finish, 0)
    norm_moves = low_exchange(("tensor",), norm_t)
    arrive(early_moves)
    right = fine_dot(early_left[0], full_out[...], NT)
    right_all[0] = jnp.concatenate([right, jnp.zeros((RANK, wide - narrow), F32)], -1).astype(BF)
    for index in range(2):
        right_all[1 + index] = fine_dot(early_left[1 + index], full_gate_up[index], NN).astype(BF)
    right_all[3] = fine_dot(early_left[3], full_down[...], NT).astype(BF)
    early_moves = low_scatter(right_all, right_in)
    for index in range(4):
        factor_left[1 + index] = early_left[index]
    arrive(norm_moves)
    norm_s[me_s] = total(norm_t, nt)[0:2]
    arrive(late_moves)
    left = orthonormal(total(late_d, nd))
    rights = []
    for index in range(3):
        rights.append(fine_dot(left, full_qkv[index], NT))
    slim_s[me_s] = jnp.concatenate(rights, 0).astype(BF)
    late_moves = low_exchange(("seq",), slim_s, norm_s)
    factor_left[0] = left
    arrive(early_moves)
    right_d[me_d] = total(right_in, ns).astype(BF)
    early_moves = low_exchange(("dp",), right_d)
    for load in loads[10:14]:
        load.wait()
    arrive(tiny_moves)
    tiny = total(tiny_d, nd)
    squares[...] = tiny[4:6, 0:width]
    arrive(late_moves)
    slim_d[me_d] = total(slim_s, ns).astype(BF)
    norm_d[me_d] = total(norm_s, ns)
    late_moves = low_exchange(("dp",), slim_d, norm_d)
    fresh = MOMENTUM * moment_norm[2:4] + tiny[2:4, 0:width] * (share * scale)
    new_moment_norm[2:4] = fresh
    new_norm_pack[2:4] = norm_pack[2:4] - STEP_RATE * fresh
    fresh = MOMENTUM * moment_inner[...] + tiny[0:2] * share
    new_moment_inner[...] = fresh
    new_inner_pack[...] = inner_pack[...] - STEP_RATE * fresh
    arrive(early_moves)
    right_sum[me_s] = (total(right_d, nd) * share).astype(BF)
    early_moves = low_exchange(("seq",), right_sum)
    arrive(early_moves)
    factor_out[...] = right_sum[0].astype(F32)[:, 0:narrow]
    for index in range(2):
        factor_gate_up[index] = right_sum[1 + index].astype(F32)
    factor_down[...] = right_sum[3].astype(F32)
    arrive(late_moves)
    slim = total(slim_d, nd) * share
    for index in range(3):
        factor_qkv[index] = slim[8 * index : 8 * index + 8]
    fresh = MOMENTUM * moment_norm[0:2] + total(norm_d, nd) * (share * scale)
    new_moment_norm[0:2] = fresh
    new_norm_pack[0:2] = norm_pack[0:2] - STEP_RATE * fresh

    for image in range(images):
        for copy in (
            one_copy(image), att_copy(image), datt_copy(image), *row_copies(image), final_copy(image),
            *(
                to_seq(span, span, send, receive, far)
                for span, send, receive in (
                    (keys_values.at[image, :, 0:3], pair_send.at[image], pair_recv.at[image, 0, 2]),
                    (pairs_send.at[image, 0:3], back_send.at[image], back_recv.at[image, 2]),
                )
            ),
        ):
            copy.wait_send()
    for copy in (*weight_copies(), inner_copy()):
        copy.wait_send()


def block(mesh_sizes, small, hbm):
    nd, ns, nt = mesh_sizes
    images, own, width = hbm[0].shape
    seq_rows = 2 * own
    slots = ns * seq_rows
    top = (own + 15) // 16 * 16
    narrow = hbm[1].shape[1]
    heads = narrow // DH
    wide = small[2].shape[1]
    shape = jax.ShapeDtypeStruct
    matrices = ((3, narrow, width), (narrow, width), (2, width, wide), (wide, width))
    shapes = (
        (images, own, width), (images, own, width),
        (5, RANK, width), (3, RANK, narrow), (RANK, narrow), (2, RANK, wide), (RANK, wide),
        *matrices, *matrices, (4, width), (2, wide), *matrices, (4, width), (2, wide), (2, width),
    )
    outs = [pltpu.VMEM(dims, F32) for dims in shapes]
    vmem = pl.BlockSpec(memory_space=pltpu.VMEM)
    hbm_spec = pl.BlockSpec(memory_space=pltpu.HBM)
    dma = pltpu.SemaphoreType.DMA
    scratch = [
        pltpu.VMEM((2, images, own, width), BF),
        pltpu.VMEM((images, seq_rows, width), BF),
        pltpu.VMEM((images, 3, ns, seq_rows, 128), BF),
        pltpu.VMEM((images * heads, seq_rows, 128), BF),
        pltpu.VMEM((images * heads, seq_rows, slots), BF),
        pltpu.VMEM((2, seq_rows, slots), F32),
        pltpu.VMEM((heads, seq_rows, slots), BF),
        pltpu.VMEM((seq_rows, 256), F32),
        pltpu.VMEM((images, seq_rows, 256), BF),
        pltpu.VMEM((2, images, own, 256), BF),
        pltpu.VMEM((images, own, 256), BF),
        pltpu.VMEM((2, 256, width), BF),
        pltpu.VMEM((2, 2, width, wide), BF),
        pltpu.VMEM((2, wide, width), BF),
        pltpu.VMEM((2, 8, wide), F32),
        pltpu.VMEM((256, width), BF),
        pltpu.VMEM((2 * narrow, width), BF),
        pltpu.VMEM((2, images, own, 2 * width), BF),
        pltpu.VMEM((images, own, width), F32),
        pltpu.VMEM((2, images, own, 3 * wide), BF),
        pltpu.VMEM((images, own, 3 * wide), BF),
        pltpu.VMEM((images, 2, own, wide), F32),
        pltpu.VMEM((images * heads, DH, seq_rows), BF),
        pltpu.VMEM((2, images, own, 256), BF),
        pltpu.VMEM((images, own, 256), BF),
        pltpu.VMEM((seq_rows, 256), F32),
        pltpu.VMEM((seq_rows, 256), F32),
        pltpu.VMEM((images, seq_rows, 256), BF),
        pltpu.VMEM((width, slots), F32),
        *[
            pltpu.VMEM((images, *rows, width), BF)
            for rows in ((ns, seq_rows), (seq_rows,), (seq_rows,), (top,), (seq_rows - top,))
        ],
        pltpu.VMEM((images, seq_rows, width), F32),
        pltpu.VMEM((images, own, width), F32),
        pltpu.VMEM((256, width), F32),
        pltpu.VMEM((2 * narrow, width), F32),
        pltpu.VMEM((2, 8, wide), F32),
        pltpu.VMEM((8, wide), F32),
        pltpu.VMEM(hbm[0].shape, BF),
        pltpu.VMEM(hbm[5].shape, F32),
        pltpu.VMEM((images, seq_rows, 1), F32),
        pltpu.VMEM((seq_rows, 128), F32),
        pltpu.VMEM((seq_rows, 128), F32),
        pltpu.VMEM((8, width), F32),
        pltpu.VMEM((slots, 8), F32),
        pltpu.VMEM((RANK, width), F32),
        pltpu.VMEM((2 * RANK, 256), BF),
        pltpu.VMEM((2 * RANK, 2 * narrow), BF),
        pltpu.VMEM((nt, 5, RANK, width), F32),
        pltpu.VMEM((4, RANK, width), F32),
        *[pltpu.VMEM((size, RANK, width), F32) for size in (ns, nd, ns)],
        *[pltpu.VMEM((size, RANK, width), F32) for size in (ns * nt, nd)],
        pltpu.VMEM((nt, RANK, width), F32),
        *[pltpu.VMEM((size, 2, width), F32) for size in (ns, nd)],
        *[pltpu.VMEM((size, RANK, wide), BF) for size in (4, ns, nd, ns)],
        *[pltpu.VMEM((size, 3 * RANK, narrow), BF) for size in (ns, nd)],
        *[pltpu.VMEM((size, RANK, wide), F32) for size in (ns, nd)],
        dma((14,)),
        *[dma((images,))] * 2,
        *[dma((4,))] * 2,
        dma((images,)),
        dma((images, 3, 3)),
        *[dma((images,))] * 4,
        *[dma((images, 2))] * 2,
        dma((images,)),
        dma((images, 3)),
        *[dma((images + 1,))] * 2,
        *[dma((16,))] * 2,
    ]
    return pl.pallas_call(
        functools.partial(block_kernel, mesh_sizes, images),
        out_shape=outs,
        in_specs=[vmem] * len(small) + [hbm_spec] * len(hbm),
        out_specs=[vmem] * len(outs),
        scratch_shapes=scratch,
        compiler_params=pltpu.CompilerParams(
            collective_id=0, has_side_effects=True, vmem_limit_bytes=(LIMIT + nd // 8) * 2**20
        ),
        name="block",
    )(*small, *hbm)


def per_device(
    tokens,
    out_grad,
    keep_mask,
    w_qkv,
    w_out,
    w_gate_up,
    w_down,
    norm_pack,
    inner_pack,
    moment_qkv,
    moment_out,
    moment_gate_up,
    moment_down,
    moment_norm,
    moment_inner,
    error_qkv,
    error_out,
    error_gate_up,
    error_down,
    basis_qkv,
    basis_out,
    basis_gate_up,
    basis_down,
):
    own_rows, images, width = tokens.shape
    slot_count = keep_mask.shape[0]
    sizes = tuple(lax.axis_size(axis) for axis in ("dp", "seq", "tensor"))

    def turn(array):
        return jnp.swapaxes(array, -1, -2)

    results = block(
        sizes,
        (
            jnp.transpose(keep_mask), norm_pack, inner_pack, moment_norm, moment_inner,
            *(turn(basis) for basis in (basis_qkv, basis_out, basis_gate_up, basis_down)),
        ),
        (
            jnp.swapaxes(tokens, 0, 1), turn(w_qkv), w_out, w_gate_up, w_down, jnp.swapaxes(out_grad, 0, 1),
            turn(error_qkv[0]), error_out[0], error_gate_up[0], error_down[0],
            turn(moment_qkv), moment_out, moment_gate_up, moment_down,
        ),
    )
    grads, lows, fulls, moments = results[0:2], results[2:7], results[7:11], results[11:15]
    (
        residual, input_grad, new_moment_norm, new_moment_inner, new_norm_pack, new_inner_pack,
        factor_left, factor_qkv, factor_out, factor_gate_up, factor_down,
        new_error_qkv, new_error_out, new_error_gate_up, new_error_down,
        new_moment_qkv, new_moment_out, new_moment_gate_up, new_moment_down,
        new_w_qkv, new_w_out, new_w_gate_up, new_w_down,
        branch_rms,
    ) = store(
        (*grads, *results[15:17], *results[21:23]), results[23], lows, fulls, moments, results[17:21],
        float(slot_count * images * lax.axis_size("dp") * width),
    )
    return (
        jnp.swapaxes(residual, 0, 1), jnp.swapaxes(input_grad, 0, 1),
        *(turn(factor) for factor in (factor_left, factor_qkv, factor_out, factor_gate_up, factor_down)),
        turn(new_error_qkv)[None], new_error_out[None], new_error_gate_up[None], new_error_down[None],
        turn(new_moment_qkv), new_moment_out, new_moment_gate_up, new_moment_down, new_moment_norm, new_moment_inner,
        turn(new_w_qkv), new_w_out, new_w_gate_up, new_w_down, new_norm_pack, new_inner_pack,
        branch_rms,
    )


def solution(mesh):
    placed = (
        P(("seq", "tensor"), "dp", None),
        P("seq", "dp", None),
        P(None, "dp"),
        P(None, None, "tensor"),
        P("tensor", None),
        P(None, None, "tensor"),
        P("tensor", None),
        P(),
        P(None, "tensor"),
        P(None, None, "tensor"),
        P("tensor", None),
        P(None, None, "tensor"),
        P("tensor", None),
        P(),
        P(None, "tensor"),
        P(("dp", "seq"), None, None, "tensor"),
        P(("dp", "seq"), "tensor", None),
        P(("dp", "seq"), None, None, "tensor"),
        P(("dp", "seq"), "tensor", None),
        P(None, "tensor", None),
        P("tensor", None),
        P(None, "tensor", None),
        P("tensor", None),
    )
    return jax.shard_map(
        per_device,
        mesh=mesh,
        in_specs=placed,
        out_specs=(
            P(("seq", "tensor"), "dp", None),
            P(("seq", "tensor"), "dp", None),
            P(),
            P(None, "tensor", None),
            P("tensor", None),
            P(None, "tensor", None),
            P("tensor", None),
            P(("dp", "seq"), None, None, "tensor"),
            P(("dp", "seq"), "tensor", None),
            P(("dp", "seq"), None, None, "tensor"),
            P(("dp", "seq"), "tensor", None),
            P(None, None, "tensor"),
            P("tensor", None),
            P(None, None, "tensor"),
            P("tensor", None),
            P(),
            P(None, "tensor"),
            P(None, None, "tensor"),
            P("tensor", None),
            P(None, None, "tensor"),
            P("tensor", None),
            P(),
            P(None, "tensor"),
            P(),
        ),
        check_vma=False,
    )
```

```python
import functools
import math

import jax
import jax.numpy as jnp
from jax import lax
from jax.experimental import pallas as pl
from jax.experimental.pallas import tpu as pltpu
from jax.sharding import PartitionSpec as P

DH = 64
FF = 1024
GRID = 32
RANK = 8
QUARTER = DH // 4
CHUNK = 16
LIMIT = 46


EPSILON = 1e-06
MOMENTUM = 0.9
STEP_RATE = 0.5
MESH = pl.DeviceIdType.MESH
BF = jnp.bfloat16
F32 = jnp.float32


def split(value):
    high = value.astype(BF)
    return high, (value - high.astype(F32)).astype(BF)


def dot(left, right, dims):
    return lax.dot_general(left, right, (dims, ((), ())), preferred_element_type=F32)


NN = ((1,), (0,))
NT = ((1,), (1,))
TN = ((0,), (0,))


def two_rows(rows):
    high, low = split(rows)
    return jnp.concatenate([high.astype(F32), low.astype(F32)], 0).astype(BF)


def fold(rows):
    return rows[0:RANK] + rows[RANK:]


def fine_dot(left, right, dims):
    right_high, right_low = split(right)
    return fold(dot(two_rows(left), right_high, dims)) + dot(left.astype(BF), right_low, dims)


def gram_schmidt(stack):
    rows = lax.broadcasted_iota(jnp.int32, (1, RANK, 1), 1)
    for index in range(RANK):
        column = stack[:, index : index + 1, :]
        products = jnp.sum(stack * column, -1, keepdims=True)
        scale = lax.rsqrt(products[:, index : index + 1, :] + EPSILON)
        done = column * scale
        rest = stack - (products * scale) * done
        stack = jnp.where(rows < index, stack, jnp.where(rows == index, done, rest))
    return stack


class Moves:
    def __init__(self, span, send, receive, device):
        self.whole = pltpu.make_async_remote_copy(
            src_ref=span, dst_ref=span, send_sem=send, recv_sem=receive, device_id=device, device_id_type=MESH
        )

    def arrive(self):
        self.whole.wait()


def exchange(axes, sizes, buffer, send, receive, pieces=None):
    count = math.prod(sizes)
    place = 0
    for axis, size in zip(axes, sizes):
        place = place * size + lax.axis_index(axis)
    for step in range(1, count):
        peer = lax.rem(place + step, count)
        device, rest = {}, peer
        for axis, size in reversed(tuple(zip(axes, sizes))):
            device[axis] = lax.rem(rest, size)
            rest = lax.div(rest, size)
        pltpu.make_async_remote_copy(
            src_ref=buffer.at[place] if pieces is None else pieces.at[peer],
            dst_ref=buffer.at[place],
            send_sem=send,
            recv_sem=receive,
            device_id=device,
            device_id_type=MESH,
        ).start()
    return Moves(buffer.at[0 : count - 1], send, receive, device)


def arrive(moves):
    for move in moves:
        move.arrive()


def total(buffer, size):
    value = buffer[0].astype(F32)
    for index in range(1, size):
        value = value + buffer[index].astype(F32)
    return value


def greet(axes, barrier):
    for axis, size in axes:
        me = lax.axis_index(axis)
        for step in range(1, size):
            pl.semaphore_signal(
                barrier, inc=1, device_id={axis: lax.rem(me + step, size)}, device_id_type=MESH
            )


def triple_first(rows):
    high, low = split(rows)
    return jnp.concatenate([high.astype(F32), high.astype(F32), low.astype(F32)], 0)


def triple_second(rows):
    high, low = split(rows)
    return jnp.concatenate([high.astype(F32), low.astype(F32), high.astype(F32)], 0)


def store_kernel(total_rows, plain, *refs):
    sources, rest = refs[:plain], refs[plain:]
    squares, factor_left, factor_qkv, factor_out, factor_gate_up, factor_down = rest[:6]
    fulls, moments, weights = rest[6:10], rest[10:14], rest[14:18]
    targets, rest = rest[18 : 18 + plain], rest[18 + plain :]
    results, branch_rms, fresh, roots_kept, sems = rest[:12], rest[12], rest[13:25], rest[25], rest[26]
    copies = [
        pltpu.make_async_copy(source, target, sems.at[number])
        for number, (source, target) in enumerate(zip(sources, targets))
    ]
    for copy in copies:
        copy.start()

    def settle(number, approx, pick):
        full, moment, weight = (pick(group[number]) for group in (fulls, moments, weights))
        places = (number, 4 + number, 8 + number)
        error_to, moment_to, weight_to = (pick(fresh[place]) for place in places)
        error_to[...] = full[...] - approx
        momentum = MOMENTUM * moment[...] + approx
        moment_to[...] = momentum
        weight_to[...] = weight[...] - STEP_RATE * momentum
        for place in places:
            copy = pltpu.make_async_copy(pick(fresh[place]), pick(results[place]), sems.at[len(copies)])
            copy.start()
            copies.append(copy)

    roots = jnp.sqrt(jnp.sum(squares[...], -1, keepdims=True) / total_rows)
    for index in range(2):
        roots_kept[index] = roots[index, 0]
    copies.append(pltpu.make_async_copy(roots_kept, branch_rms, sems.at[len(copies)]))
    copies[-1].start()

    def product(rows, columns):
        return dot(rows.astype(BF), columns.astype(BF), TN)

    lefts = [triple_first(factor_left[index]) for index in range(5)]
    for index in range(2):
        settle(2, product(lefts[2 + index], triple_second(factor_gate_up[index])), lambda ref: ref.at[index])
    settle(3, product(triple_second(factor_down[...]), lefts[4]), lambda ref: ref)
    settle(1, product(triple_second(factor_out[...]), lefts[1]), lambda ref: ref)
    for index in range(3):
        settle(0, product(triple_second(factor_qkv[index]), lefts[0]), lambda ref: ref.at[index])
    for copy in copies:
        copy.wait()


def store(plain, squares, factors, fulls, moments, weights, total_rows):
    vmem = pl.BlockSpec(memory_space=pltpu.VMEM)
    matrices = [*fulls, *moments, *weights]
    shapes = [jax.ShapeDtypeStruct(array.shape, F32) for array in (*plain, *factors, *matrices)]
    count = len(plain) + len(factors)
    return pl.pallas_call(
        functools.partial(store_kernel, total_rows, count),
        out_shape=[*shapes, jax.ShapeDtypeStruct((2,), F32)],
        in_specs=[vmem] * (count + 1 + len(factors) + 12),
        out_specs=[pl.BlockSpec(memory_space=pltpu.HBM)] * (len(shapes) + 1),
        scratch_shapes=[
            *[pltpu.VMEM(array.shape, F32) for array in matrices],
            pltpu.SMEM((2,), F32),
            pltpu.SemaphoreType.DMA((count + 22,)),
        ],
        compiler_params=pltpu.CompilerParams(vmem_limit_bytes=24 * 2**20),
        name="store",
    )(*plain, *factors, squares, *factors, *matrices)


def swap_quarters(tile):
    lane = lax.broadcasted_iota(jnp.int32, (1, 128), 1)
    low = lax.rem(lax.div(lane, QUARTER), 2) == 0
    return jnp.where(low, pltpu.roll(tile, 128 - QUARTER, 1), pltpu.roll(tile, QUARTER, 1))


def turn_pairs(pairs, cosine, sine):
    keys = lax.broadcasted_iota(jnp.int32, (1, 128), 1) < DH
    first, second, third = (pairs[:, start : start + 128] for start in (0, 128, 256))
    first = first * cosine + swap_quarters(first) * sine
    second = jnp.where(keys, second * cosine + swap_quarters(second) * sine, second)
    return jnp.concatenate([first, second, third], -1)


def turn_queries(raw, cosine, sine):
    tiles = (raw[:, start : start + 128] for start in (0, 128))
    return jnp.concatenate([tile * cosine + swap_quarters(tile) * sine for tile in tiles], -1)


def angle_tables(first_slot, count):
    slots = first_slot + lax.broadcasted_iota(jnp.int32, (count, 128), 0)
    place = lax.rem(lax.broadcasted_iota(jnp.int32, (count, 128), 1), DH)
    inside = jnp.logical_and(slots >= 1, slots <= GRID * GRID)
    patch = jnp.where(inside, slots - 1, 0)
    quarter = lax.div(place, QUARTER)
    position = jnp.where(quarter < 2, lax.div(patch, GRID), lax.rem(patch, GRID)).astype(F32)
    power = lax.rem(place, QUARTER).astype(F32)
    angles = position * jnp.exp(power * (-math.log(10000.0) / QUARTER)) * (16.0 / GRID)
    sine = jnp.sin(angles)
    return jnp.cos(angles), jnp.where(lax.rem(quarter, 2) == 0, -sine, sine)


def norm_parts(values, gain, bias):
    centre = values - jnp.mean(values, -1, keepdims=True)
    spread = jnp.mean(centre * centre, -1, keepdims=True)
    inverse = lax.rsqrt(spread + EPSILON)
    normed = centre * inverse
    return (normed * gain + bias, normed, inverse)


def norm_back(grad, normed, inverse, gain):
    scaled = grad * gain
    return inverse * (
        scaled
        - jnp.mean(scaled, -1, keepdims=True)
        - normed * jnp.mean(scaled * normed, -1, keepdims=True)
    )


def column_sums(value):
    return jnp.sum(value, 0, keepdims=True)


def block_kernel(sizes, images, *refs):
    smalls = refs[0:9]
    (
        tokens_hbm, w_qkv_hbm, w_out_hbm, w_gate_up_hbm, w_down_hbm, out_grad_hbm,
        error_qkv_hbm, error_out_hbm, error_gate_up_hbm, error_down_hbm,
        moment_qkv_hbm, moment_out_hbm, moment_gate_up_hbm, moment_down_hbm,
    ) = refs[9:23]
    (
        residual, input_grad, factor_left, factor_qkv, factor_out, factor_gate_up, factor_down,
        full_qkv, full_out, full_gate_up, full_down,
        moment_qkv, moment_out, moment_gate_up, moment_down, new_moment_norm, new_moment_inner,
        w_qkv, w_out, w_gate_up, w_down, new_norm_pack, new_inner_pack, squares,
        normed_one, normed_one_all, keys_values, queries, probs, scores, grad_scores,
        attended, attended_low, attended_in, attended_send,
        out_low, gate_up_low, down_low, inner_all, query_low, key_value_low,
        slim_rows, grad_middle, wide_rows, wide_rows_send, grad_down, queries_t,
        grad_attended, grad_attended_send, grad_attended_all, grad_query, grad_query_low, grad_pairs,
        *rest,
    ) = refs[23:]
    pairs_send, pairs_x, pairs_y, relay_x, relay_y = rest[0:5]
    ( grad_one, grad_one_recv, sum_query, sum_pairs, inner_sums, inner_recv,
        tokens, out_grad, mask, cosine, sine, extra, kept_rows, late_sum, thin_query, thin_pairs,
        early_t, early_all, early_in, early_d, early_left, late_s, late_d, norm_t, norm_s, norm_d,
        right_all, right_in, right_d, right_sum, slim_s, slim_d, tiny_s, tiny_d,
        local_sems, one_send, one_recv, weight_send, weight_recv, pair_send, pair_recv,
        att_send, att_recv, datt_send, datt_recv, rows_send, rows_recv, back_send, back_recv,
        final_send, final_recv, low_send, low_recv,
        keep, norm_pack, inner_pack, moment_norm, moment_inner, basis_qkv, basis_out, basis_gate_up, basis_down,
    ) = rest[5:]
    copied = (keep, norm_pack, inner_pack, moment_norm, moment_inner, basis_qkv, basis_out, basis_gate_up, basis_down)
    nd, ns, nt = sizes
    me_t, me_s = lax.axis_index("tensor"), lax.axis_index("seq")
    other = 1 - me_t
    near_x = me_s + 1 - 2 * lax.rem(me_s, 2)
    near_y = lax.rem(me_s + 2, 4)
    far = 3 - me_s
    me_d = lax.axis_index("dp")
    own, width = tokens.shape[1], tokens.shape[2]
    seq_rows = 2 * own
    slots = ns * seq_rows
    heads = w_qkv.shape[1] // DH
    wide = w_down.shape[0]
    hidden_all = 2 * wide
    scale = (images * seq_rows) ** (-0.5)
    top = (own + 15) // 16 * 16
    upper, lower = slice(0, top), slice(top, seq_rows)
    own_rows = pl.ds(pl.multiple_of(me_t * own, 8), own)
    other_rows = pl.ds(pl.multiple_of(other * own, 8), own)

    barrier = pltpu.get_barrier_semaphore()
    greet((("tensor", nt), ("seq", ns), ("dp", nd)), barrier)
    loads = [
        pltpu.make_async_copy(source, target, local_sems.at[number])
        for number, (source, target) in enumerate(
            (
                (tokens_hbm, tokens), (w_qkv_hbm, w_qkv),
                (w_out_hbm, w_out), (w_gate_up_hbm, w_gate_up), (w_down_hbm, w_down), (out_grad_hbm, out_grad),
                (error_qkv_hbm, full_qkv), (error_out_hbm, full_out),
                (error_gate_up_hbm, full_gate_up), (error_down_hbm, full_down),
                (moment_qkv_hbm, moment_qkv), (moment_out_hbm, moment_out),
                (moment_gate_up_hbm, moment_gate_up), (moment_down_hbm, moment_down), *zip(smalls, copied),
            )
        )
    ]
    for load in (loads[15], loads[0], loads[1]):
        load.start()

    def to_partner(source, target, send, receive):
        return pltpu.make_async_remote_copy(
            src_ref=source, dst_ref=target, send_sem=send, recv_sem=receive,
            device_id={"tensor": other}, device_id_type=MESH,
        )

    def to_seq(source, target, send, receive, peer):
        return pltpu.make_async_remote_copy(
            src_ref=source, dst_ref=target, send_sem=send, recv_sem=receive,
            device_id={"seq": peer}, device_id_type=MESH,
        )

    def one_copy(image):
        block = normed_one.at[me_t, image]
        return to_partner(block, block, one_send.at[image], one_recv.at[image])

    def weight_copies():
        return [
            to_partner(ref.at[me_t], ref.at[me_t], weight_send.at[number], weight_recv.at[number])
            for number, ref in enumerate((out_low, gate_up_low, down_low, inner_all))
        ]

    def pair_copy(image, tile, kind):
        place, peer = ((me_s, near_x), (me_s, near_y), (near_x, near_y), (near_y, near_x))[kind]
        block = keys_values.at[image, tile, place]
        if kind >= 2:
            block = block.at[(upper, lower)[kind - 2]]
        return to_seq(block, block, pair_send.at[image], pair_recv.at[image, tile, min(kind, 2)], peer)

    def send_pairs(image, tile):
        for kind in range(2):
            pair_copy(image, tile, kind).start()

    def forward_pairs(image, tile):
        for kind in range(2):
            pair_copy(image, tile, kind).wait_recv()
            pair_copy(image, tile, 2 + kind).start()

    def await_pairs(image, tile):
        block = keys_values.at[image, tile, far]
        to_seq(block, block, pair_send.at[image], pair_recv.at[image, tile, 2], far).wait_recv()

    def att_copy(image):
        return to_partner(
            attended_send.at[image], attended_in.at[me_t, image], att_send.at[image], att_recv.at[image]
        )

    def datt_copy(image):
        return to_partner(
            grad_attended_send.at[image], grad_attended.at[me_t, image], datt_send.at[image], datt_recv.at[image]
        )

    def row_copies(image):
        moves = ((slim_rows.at[me_t, image], slim_rows), (wide_rows_send.at[image], wide_rows))
        return [
            to_partner(source, target.at[me_t, image], rows_send.at[image, number], rows_recv.at[image, number])
            for number, (source, target) in enumerate(moves)
        ]

    def back_copy(image, kind):
        place, rows, target, there, peer = (
            (far, upper, relay_x, slice(0, top), near_x),
            (far, lower, relay_y, slice(0, seq_rows - top), near_y),
            (near_x, upper, pairs_x, upper, near_x),
            (near_y, lower, pairs_y, lower, near_y),
            (near_x, lower, pairs_x, lower, near_x),
            (near_y, upper, pairs_y, upper, near_y),
        )[kind]
        return to_seq(
            pairs_send.at[image, place, rows], target.at[image, there],
            back_send.at[image], back_recv.at[image, min(kind, 2)], peer,
        )

    def relay_back(image):
        for place, rows, inbox, arrival, onward in ((near_y, upper, relay_x, 0, 5), (near_x, lower, relay_y, 1, 4)):
            back_copy(image, arrival).wait_recv()
            value = pairs_send[image, place, rows].astype(F32) + inbox[image].astype(F32)
            pairs_send[image, place, rows] = value.astype(BF)
            back_copy(image, onward).start()

    def final_copy(image):
        return to_partner(
            grad_one.at[image, other_rows], grad_one_recv.at[image], final_send.at[image], final_recv.at[image]
        )

    def inner_copy():
        return to_partner(
            inner_sums.at[other], inner_recv, final_send.at[images], final_recv.at[images]
        )


    cosine[...], sine[...] = angle_tables(me_s * seq_rows, seq_rows)
    loads[15].wait()
    gain_one, bias_one = norm_pack[0:1], norm_pack[1:2]
    gain_two, bias_two = norm_pack[2:3], norm_pack[3:4]
    loads[0].wait()
    for image in range(images):
        normed, _, _ = norm_parts(tokens[image].astype(F32), gain_one, bias_one)
        normed_one[me_t, image] = normed.astype(BF)
        if image == 0:
            pl.semaphore_wait(barrier, (nt - 1) + (ns - 1) + (nd - 1))
        one_copy(image).start()
    for load in (*loads[2:5], loads[14], *loads[16:23], *loads[5:14]):
        load.start()
    loads[1].wait()

    narrow = heads * DH
    pad = jnp.zeros((256 - narrow, width), BF)
    query_low[...] = jnp.concatenate([w_qkv[0].astype(BF), pad], 0)
    key_value_low[0:narrow] = w_qkv[1].astype(BF)
    key_value_low[narrow : 2 * narrow] = w_qkv[2].astype(BF)

    def project(image, carry):
        one_copy(image).wait_recv()
        blocks = [normed_one[half, image] for half in range(2)]
        pairs = jnp.concatenate([dot(block, key_value_low[...], NT) for block in blocks], 0)
        pairs = turn_pairs(pairs, cosine[...], sine[...])
        for tile in range(3):
            keys_values[image, tile, me_s] = pairs[:, 128 * tile : 128 * tile + 128].astype(BF)

        @pl.when(image == 0)
        def _():
            for tile in range(3):
                send_pairs(image, tile)

        raw = jnp.concatenate([dot(block, query_low[...], NT) for block in blocks], 0)
        raw = turn_queries(raw, cosine[...], sine[...]) * (DH ** (-0.5))
        lane = lax.broadcasted_iota(jnp.int32, (1, 128), 1)
        for head in range(heads):
            tile = raw[:, head // 2 * 128 : head // 2 * 128 + 128]
            queries[image * heads + head] = jnp.where(lax.div(lane, DH) == head % 2, tile, 0.0).astype(BF)
        normed_one_all[image] = jnp.concatenate([block.astype(F32) for block in blocks], 0).astype(BF)
        return carry

    lax.fori_loop(0, images, project, 0)

    for load in (loads[14], *loads[16:23]):
        load.wait()
    for load in loads[2:5]:
        load.wait()
    out_low[me_t] = jnp.concatenate([pad, w_out[...].astype(BF)], 0)
    for index in range(2):
        gate_up_low[me_t, index] = w_gate_up[index].astype(BF)
    down_low[me_t] = w_down[...].astype(BF)
    inner_all[me_t] = jnp.zeros_like(inner_all[me_t])
    inner_all[me_t, 0:2] = inner_pack[...]
    for copy in weight_copies():
        copy.start()
    kept = jnp.concatenate([keep[...].astype(F32), jnp.zeros((8 - images, slots), F32)], 0)
    kept_rows[...] = jnp.transpose(kept)
    kept = kept_rows[pl.ds(pl.multiple_of(me_s * seq_rows, 8), seq_rows)]
    for image in range(images):
        mask[image] = kept[:, image : image + 1]
    loads[5].wait()
    loads[6].wait()
    late_sum[...] = sum(fine_dot(basis_qkv[index], full_qkv[index], NN) for index in range(3))
    gap = jnp.zeros((RANK, 256 - narrow), F32)
    thin_query[...] = two_rows(jnp.concatenate([basis_qkv[0], gap], -1))
    thin_pairs[...] = two_rows(jnp.concatenate([basis_qkv[1], basis_qkv[2]], -1))
    extra[...] = jnp.zeros_like(extra)
    inner_sums[...] = jnp.zeros_like(inner_sums)

    def halves_of(lower, upper):
        lane = lax.broadcasted_iota(jnp.int32, (1, 128), 1)
        return jnp.where(lane < DH, lower, upper)

    def half_of(value, half):
        return halves_of(value, 0.0) if half == 0 else halves_of(0.0, value)

    def key_tile(image, index):
        return keys_values[image, index].reshape(slots, 128)

    def attend(image):
        @pl.when(image == 0)
        def _():
            forward_pairs(0, 0)
            forward_pairs(0, 1)
            forward_pairs(0, 2)
            for tile in range(3):
                send_pairs(1, tile)
            for copy in weight_copies():
                copy.wait_recv()

            def ahead(place, carry):
                cotangent = out_grad[place, own_rows] * mask[place, own_rows]
                for index, half in enumerate((me_t, other)):
                    grad_down[place, index] = dot(cotangent.astype(BF), down_low[half], NT)
                for head in range(heads):
                    turned = jnp.transpose(queries[place * heads + head].astype(F32))
                    start = head % 2 * DH
                    queries_t[place * heads + head] = turned[start : start + DH].astype(BF)
                return carry

            lax.fori_loop(0, images, ahead, 0)

        bias = jnp.where(keep[pl.ds(image, 1), :] > 0, 0.0, -1e30)

        def score(head):
            scores[head % 2] = dot(queries[image * heads + head], key_tile(image, head // 2), NT)

        def chances(head):
            for start in range(0, seq_rows, CHUNK):
                rows = slice(start, start + CHUNK)
                part = scores[head % 2, rows] + bias
                part = jnp.exp(part - jnp.max(part, -1, keepdims=True))
                part = part * (1.0 / jnp.sum(part, -1, keepdims=True))
                probs[image * heads + head, rows] = part.astype(BF)

        def mix(head):
            return dot(probs[image * heads + head], key_tile(image, 1 + (head + 1) // 2), NN)

        await_pairs(image, 0)
        score(0)
        score(1)
        chances(0)
        await_pairs(image, 1)
        score(2)
        mixed = [mix(0)]
        chances(1)
        chances(2)
        await_pairs(image, 2)
        mixed.append(mix(1))
        mixed.append(mix(2))
        attended[:, 0:128] = half_of(mixed[0], 1)
        attended[:, 128:256] = halves_of(mixed[1], mixed[2])
        attended_low[image] = attended[...].astype(BF)
        attended_in[me_t, image] = attended[own_rows].astype(BF)
        attended_send[image] = attended[other_rows].astype(BF)
        att_copy(image).start()

        @pl.when(image == 0)
        def _():
            forward_pairs(1, 0)

        @pl.when(image == 1)
        def _():
            for load in loads[7:10]:
                load.wait()
            weights(0)
            forward_pairs(2, 0)

        @pl.when(image == 2)
        def _():
            relay_back(0)

    def feed(image):
        att_copy(image).wait_recv()
        inputs = tokens[image].astype(F32)
        branch = sum(dot(attended_in[half, image], out_low[half], NN) for half in range(2))
        middle = inputs + branch
        extra[4:5] += column_sums(branch * branch)
        normed, hat_two, inverse_two = norm_parts(middle, gain_two, bias_two)
        rows_two = normed.astype(BF)
        slim_rows[me_t, image, :, 0:width] = rows_two
        halves = (me_t, other)
        gates = [dot(rows_two, gate_up_low[half, 0], NN) for half in halves]
        ups = [dot(rows_two, gate_up_low[half, 1], NN) for half in halves]
        sigmoids = [1.0 / (1.0 + jnp.exp(-gate)) for gate in gates]
        hiddens = [gate * sigmoid * up for gate, sigmoid, up in zip(gates, sigmoids, ups)]
        mean = sum(jnp.sum(hidden, -1, keepdims=True) for hidden in hiddens) / hidden_all
        centres = [hidden - mean for hidden in hiddens]
        spread = sum(jnp.sum(centre * centre, -1, keepdims=True) for centre in centres) / hidden_all
        inverse_three = lax.rsqrt(spread + EPSILON)
        hats = [centre * inverse_three for centre in centres]
        lows = [
            (hat * inner_all[half, 0:1] + inner_all[half, 1:2]).astype(BF)
            for hat, half in zip(hats, halves)
        ]
        branch = sum(dot(low, down_low[half], NN) for low, half in zip(lows, halves))
        extra[5:6] += column_sums(branch * branch)
        residual[image] = middle + branch

        @pl.when(image == 0)
        def _():
            forward_pairs(1, 1)

        cotangent = out_grad[image, own_rows] * mask[image, own_rows]
        grads = [grad_down[image, index] for index in range(2)]
        for half, grad, hat in zip(halves, grads, hats):
            inner_sums[half, 0:1] += column_sums(grad * hat)
            inner_sums[half, 1:2] += column_sums(grad)
        scaled = [grad * inner_all[half, 0:1] for grad, half in zip(grads, halves)]
        first = sum(jnp.sum(value, -1, keepdims=True) for value in scaled) / hidden_all
        second = (
            sum(jnp.sum(value * hat, -1, keepdims=True) for value, hat in zip(scaled, hats)) / hidden_all
        )
        grad_hiddens = [
            inverse_three * (value - first - hat * second) for value, hat in zip(scaled, hats)
        ]
        gate_rows = [
            (grad * up * (sigmoid + gate * sigmoid * (1.0 - sigmoid))).astype(BF)
            for grad, up, sigmoid, gate in zip(grad_hiddens, ups, sigmoids, gates)
        ]
        up_rows = [
            (grad * gate * sigmoid).astype(BF)
            for grad, gate, sigmoid in zip(grad_hiddens, gates, sigmoids)
        ]
        for number, pair in enumerate((lows, gate_rows, up_rows)):
            wide_rows[me_t, image, :, number * wide : number * wide + wide] = pair[0]
            wide_rows_send[image, :, number * wide : number * wide + wide] = pair[1]
        grad_two = sum(
            dot(gate_row, gate_up_low[half, 0], NT) + dot(up_row, gate_up_low[half, 1], NT)
            for gate_row, up_row, half in zip(gate_rows, up_rows, halves)
        )
        extra[2:3] += column_sums(grad_two * hat_two)
        extra[3:4] += column_sums(grad_two)
        back = cotangent + norm_back(grad_two, hat_two, inverse_two, gain_two)
        grad_middle[image] = back
        low = back.astype(BF)
        slim_rows[me_t, image, :, width:] = low
        grad_attended[me_t, image] = dot(low, out_low[me_t], NT).astype(BF)
        grad_attended_send[image] = dot(low, out_low[other], NT).astype(BF)
        datt_copy(image).start()
        for copy in row_copies(image):
            copy.start()

        @pl.when(image == 0)
        def _():
            forward_pairs(1, 2)
            for tile in range(3):
                send_pairs(2, tile)

    def attend_back(image):
        datt_copy(image).wait_recv()
        grad_attended_all[...] = jnp.concatenate(
            [grad_attended[half, image].astype(F32) for half in range(2)], 0
        )
        wides = [half_of(grad_attended_all[:, 0:128], 1)]
        wides += [half_of(grad_attended_all[:, 128:256], half) for half in range(2)]
        lows = [wide.astype(BF) for wide in wides]
        mixed = attended_low[image].astype(F32)
        deltas = [
            jnp.sum(wide * mixed[:, tile * 128 : tile * 128 + 128], -1, keepdims=True)
            for wide, tile in zip(wides, (0, 1, 1))
        ]

        def grad_chance(head):
            scores[head % 2] = dot(lows[head], key_tile(image, 1 + (head + 1) // 2), NT)

        def grad_score(head):
            for start in range(0, seq_rows, CHUNK):
                rows = slice(start, start + CHUNK)
                chance = probs[image * heads + head, rows].astype(F32)
                grad_scores[head, rows] = (chance * (scores[head % 2, rows] - deltas[head][rows])).astype(BF)

        def value_grad(head):
            start = (head + 1) % 2 * DH
            rows = jnp.transpose(wides[head])[start : start + DH].astype(BF)
            place = (heads + head) * DH
            grad_pairs[place : place + DH] = dot(rows, probs[image * heads + head], NN)

        def key_grad(head):
            place = head * DH
            grad_pairs[place : place + DH] = dot(queries_t[image * heads + head], grad_scores[head], NN)

        def query_grad(head):
            return dot(grad_scores[head], key_tile(image, head // 2), NN)

        grad_chance(0)
        grad_chance(1)
        value_grad(0)
        grad_score(0)
        grad_chance(2)
        value_grad(1)
        grad_score(1)
        query_grads = [query_grad(0)]
        key_grad(0)
        value_grad(2)
        grad_score(2)
        query_grads.append(query_grad(1))
        key_grad(1)
        query_grads.append(query_grad(2))
        key_grad(2)
        grad_query[:, 0:128] = halves_of(query_grads[0], query_grads[1])
        grad_query[:, 128:256] = half_of(query_grads[2], 0)

        pairs_send[image] = jnp.transpose(grad_pairs[...]).astype(BF).reshape(ns, seq_rows, width)

        @pl.when(image == 0)
        def _():
            forward_pairs(2, 1)
            forward_pairs(2, 2)

        for kind in range(4):
            back_copy(image, kind).start()
        raw = grad_query[...] * (DH ** (-0.5))
        raw = turn_queries(raw, cosine[...], -sine[...])
        grad_query_low[image] = raw.astype(BF)

    def weights(image):
        for copy in row_copies(image):
            copy.wait_recv()
        parts = []
        for half in range(2):
            place = slice(half * own, half * own + own)
            grad_branch = (out_grad[image, place] * mask[image, place]).astype(BF)
            normed_three, grad_gate, grad_up = (
                wide_rows[half, image, :, number * wide : number * wide + wide] for number in range(3)
            )
            rows_two, low = slim_rows[half, image, :, 0:width], slim_rows[half, image, :, width:]
            mixed = attended_low[image].astype(F32)[place].astype(BF)
            parts.append(((normed_three, grad_branch), (rows_two, grad_gate), (rows_two, grad_up), (mixed, low)))
        down, gate, up, out = (dot(*first, TN) + dot(*second, TN) for first, second in zip(*parts))
        full_down[...] += down * scale
        full_gate_up[0] += gate * scale
        full_gate_up[1] += up * scale
        full_out[...] += out[256 - narrow :] * scale

    def stage(step, carry):
        @pl.when(step < images)
        def _():
            attend(step)

        @pl.when(step == images)
        def _():
            weights(1)
            relay_back(1)

        @pl.when(step >= 1)
        def _():
            attend_back(step - 1)

        @pl.when(step < images)
        def _():
            feed(step)

        return carry

    lax.fori_loop(0, images + 1, stage, 0)
    inner_copy().start()

    weights(images - 1)

    taken = []
    sizes_of = {"dp": nd, "seq": ns, "tensor": nt}

    def low_exchange(axes, *buffers):
        moves = []
        for buffer in buffers:
            place = len(taken)
            taken.append(place)
            moves.append(
                exchange(axes, [sizes_of[axis] for axis in axes], buffer, low_send.at[place], low_recv.at[place])
            )
        return moves

    def low_scatter(pieces, inbox):
        place = len(taken)
        taken.append(place)
        inbox[me_s] = pieces[me_s]
        return [exchange(("seq",), (ns,), inbox, low_send.at[place], low_recv.at[place], pieces)]

    share = 1.0 / (ns * nd)
    early = early_t.at[me_t]
    early[0] = fine_dot(basis_out[...], full_out[...], NN)
    for index in range(2):
        early[1 + index] = fine_dot(basis_gate_up[index], full_gate_up[index], NT)
    early[3] = fine_dot(basis_down[...], full_down[...], NN)
    early[4] = extra[...]
    early_moves = low_exchange(("tensor",), early_t)

    sum_query[...] = jnp.zeros_like(sum_query)
    sum_pairs[...] = jnp.zeros_like(sum_pairs)

    def pairs_of(image):
        both = pairs_send.at[image, 0:2]
        to_seq(both, both, back_send.at[image], back_recv.at[image, 2], far).wait_recv()
        pairs = pairs_send[image, me_s].astype(F32)
        pairs = pairs + pairs_x[image].astype(F32) + pairs_y[image].astype(F32)
        pairs = turn_pairs(pairs, cosine[...], -sine[...]).astype(BF)
        rows = dot(thin_query[...], grad_query_low[image], NT) + dot(thin_pairs[...], pairs, NT)
        late_sum[...] += fold(dot(two_rows(fold(rows)), normed_one_all[image], NN)) * scale
        return pairs

    def finish_pairs(image, pairs):
        query = grad_query_low[image]
        grad_one[image] = dot(query, query_low[...], NN) + dot(pairs, key_value_low[...], NN)
        final_copy(image).start()
        sum_query[...] += dot(query, normed_one_all[image], TN)
        sum_pairs[...] += dot(pairs, normed_one_all[image], TN)

    finish_pairs(0, pairs_of(0))
    arrive(early_moves)
    summed = total(early_t, nt)
    early_all[...] = summed[0:4]
    early_moves = low_scatter(early_all, early_in)
    inner_copy().wait_recv()
    tiny_s[me_s] = jnp.zeros_like(tiny_s[me_s])
    tiny_s[me_s, 0:2] = ((inner_sums[me_t] + inner_recv[...]) * scale)[0:2]
    tiny_s[me_s, 2:6, 0:width] = summed[4, 2:6]
    tiny_moves = low_exchange(("seq",), tiny_s)
    relay_back(images - 1)
    finish_pairs(1, pairs_of(1))
    arrive(early_moves)
    early_d[me_d] = total(early_in, ns)
    early_moves = low_exchange(("dp",), early_d)
    arrive(tiny_moves)
    tiny_d[me_d] = total(tiny_s, ns)
    tiny_moves = low_exchange(("dp",), tiny_d)
    pairs = pairs_of(images - 1)
    late_s[me_s * nt + me_t] = late_sum[...]
    late_moves = low_exchange(("seq", "tensor"), late_s)
    finish_pairs(images - 1, pairs)
    full_qkv[0] += sum_query[0:narrow] * scale
    full_qkv[1] += sum_pairs[0:narrow] * scale
    full_qkv[2] += sum_pairs[narrow : 2 * narrow] * scale

    norm_t[me_t] = jnp.zeros_like(norm_t[me_t])

    def finish(image, carry):
        final_copy(image).wait_recv()
        grad = grad_one[image, own_rows] + grad_one_recv[image]
        _, hat_one, inverse_one = norm_parts(tokens[image].astype(F32), gain_one, bias_one)
        input_grad[image] = grad_middle[image] + norm_back(grad, hat_one, inverse_one, gain_one)
        norm_t[me_t, 0:1] += column_sums(grad * hat_one)
        norm_t[me_t, 1:2] += column_sums(grad)
        return carry

    def orthonormal(rows):
        return gram_schmidt(rows.reshape(1, RANK, width))[0]

    arrive(early_moves)
    early_left[me_s] = orthonormal(total(early_d, nd))
    early_moves = low_exchange(("seq",), early_left)
    arrive(late_moves)
    late_d[me_d] = total(late_s, ns * nt)
    late_moves = low_exchange(("dp",), late_d)
    lax.fori_loop(0, images, finish, 0)
    norm_moves = low_exchange(("tensor",), norm_t)
    arrive(early_moves)
    right = fine_dot(early_left[0], full_out[...], NT)
    right_all[0] = jnp.concatenate([right, jnp.zeros((RANK, wide - narrow), F32)], -1).astype(BF)
    for index in range(2):
        right_all[1 + index] = fine_dot(early_left[1 + index], full_gate_up[index], NN).astype(BF)
    right_all[3] = fine_dot(early_left[3], full_down[...], NT).astype(BF)
    early_moves = low_scatter(right_all, right_in)
    for index in range(4):
        factor_left[1 + index] = early_left[index]
    arrive(norm_moves)
    norm_s[me_s] = total(norm_t, nt)[0:2]
    arrive(late_moves)
    left = orthonormal(total(late_d, nd))
    rights = []
    for index in range(3):
        rights.append(fine_dot(left, full_qkv[index], NT))
    slim_s[me_s] = jnp.concatenate(rights, 0).astype(BF)
    late_moves = low_exchange(("seq",), slim_s, norm_s)
    factor_left[0] = left
    arrive(early_moves)
    right_d[me_d] = total(right_in, ns).astype(BF)
    early_moves = low_exchange(("dp",), right_d)
    for load in loads[10:14]:
        load.wait()
    arrive(tiny_moves)
    tiny = total(tiny_d, nd)
    squares[...] = tiny[4:6, 0:width]
    arrive(late_moves)
    slim_d[me_d] = total(slim_s, ns).astype(BF)
    norm_d[me_d] = total(norm_s, ns)
    late_moves = low_exchange(("dp",), slim_d, norm_d)
    fresh = MOMENTUM * moment_norm[2:4] + tiny[2:4, 0:width] * (share * scale)
    new_moment_norm[2:4] = fresh
    new_norm_pack[2:4] = norm_pack[2:4] - STEP_RATE * fresh
    fresh = MOMENTUM * moment_inner[...] + tiny[0:2] * share
    new_moment_inner[...] = fresh
    new_inner_pack[...] = inner_pack[...] - STEP_RATE * fresh
    arrive(early_moves)
    right_sum[me_s] = (total(right_d, nd) * share).astype(BF)
    early_moves = low_exchange(("seq",), right_sum)
    arrive(early_moves)
    factor_out[...] = right_sum[0].astype(F32)[:, 0:narrow]
    for index in range(2):
        factor_gate_up[index] = right_sum[1 + index].astype(F32)
    factor_down[...] = right_sum[3].astype(F32)
    arrive(late_moves)
    slim = total(slim_d, nd) * share
    for index in range(3):
        factor_qkv[index] = slim[8 * index : 8 * index + 8]
    fresh = MOMENTUM * moment_norm[0:2] + total(norm_d, nd) * (share * scale)
    new_moment_norm[0:2] = fresh
    new_norm_pack[0:2] = norm_pack[0:2] - STEP_RATE * fresh

    for image in range(images):
        for copy in (
            one_copy(image), att_copy(image), datt_copy(image), *row_copies(image), final_copy(image),
            *(
                to_seq(span, span, send, receive, far)
                for span, send, receive in (
                    (keys_values.at[image, :, 0:3], pair_send.at[image], pair_recv.at[image, 0, 2]),
                    (pairs_send.at[image, 0:3], back_send.at[image], back_recv.at[image, 2]),
                )
            ),
        ):
            copy.wait_send()
    for copy in (*weight_copies(), inner_copy()):
        copy.wait_send()


def block(mesh_sizes, small, hbm):
    nd, ns, nt = mesh_sizes
    images, own, width = hbm[0].shape
    seq_rows = 2 * own
    slots = ns * seq_rows
    top = (own + 15) // 16 * 16
    narrow = hbm[1].shape[1]
    heads = narrow // DH
    wide = small[2].shape[1]
    shape = jax.ShapeDtypeStruct
    matrices = ((3, narrow, width), (narrow, width), (2, width, wide), (wide, width))
    shapes = (
        (images, own, width), (images, own, width),
        (5, RANK, width), (3, RANK, narrow), (RANK, narrow), (2, RANK, wide), (RANK, wide),
        *matrices, *matrices, (4, width), (2, wide), *matrices, (4, width), (2, wide), (2, width),
    )
    outs = [pltpu.VMEM(dims, F32) for dims in shapes]
    vmem = pl.BlockSpec(memory_space=pltpu.VMEM)
    hbm_spec = pl.BlockSpec(memory_space=pltpu.HBM)
    dma = pltpu.SemaphoreType.DMA
    scratch = [
        pltpu.VMEM((2, images, own, width), BF),
        pltpu.VMEM((images, seq_rows, width), BF),
        pltpu.VMEM((images, 3, ns, seq_rows, 128), BF),
        pltpu.VMEM((images * heads, seq_rows, 128), BF),
        pltpu.VMEM((images * heads, seq_rows, slots), BF),
        pltpu.VMEM((2, seq_rows, slots), F32),
        pltpu.VMEM((heads, seq_rows, slots), BF),
        pltpu.VMEM((seq_rows, 256), F32),
        pltpu.VMEM((images, seq_rows, 256), BF),
        pltpu.VMEM((2, images, own, 256), BF),
        pltpu.VMEM((images, own, 256), BF),
        pltpu.VMEM((2, 256, width), BF),
        pltpu.VMEM((2, 2, width, wide), BF),
        pltpu.VMEM((2, wide, width), BF),
        pltpu.VMEM((2, 8, wide), F32),
        pltpu.VMEM((256, width), BF),
        pltpu.VMEM((2 * narrow, width), BF),
        pltpu.VMEM((2, images, own, 2 * width), BF),
        pltpu.VMEM((images, own, width), F32),
        pltpu.VMEM((2, images, own, 3 * wide), BF),
        pltpu.VMEM((images, own, 3 * wide), BF),
        pltpu.VMEM((images, 2, own, wide), F32),
        pltpu.VMEM((images * heads, DH, seq_rows), BF),
        pltpu.VMEM((2, images, own, 256), BF),
        pltpu.VMEM((images, own, 256), BF),
        pltpu.VMEM((seq_rows, 256), F32),
        pltpu.VMEM((seq_rows, 256), F32),
        pltpu.VMEM((images, seq_rows, 256), BF),
        pltpu.VMEM((width, slots), F32),
        *[
            pltpu.VMEM((images, *rows, width), BF)
            for rows in ((ns, seq_rows), (seq_rows,), (seq_rows,), (top,), (seq_rows - top,))
        ],
        pltpu.VMEM((images, seq_rows, width), F32),
        pltpu.VMEM((images, own, width), F32),
        pltpu.VMEM((256, width), F32),
        pltpu.VMEM((2 * narrow, width), F32),
        pltpu.VMEM((2, 8, wide), F32),
        pltpu.VMEM((8, wide), F32),
        pltpu.VMEM(hbm[0].shape, BF),
        pltpu.VMEM(hbm[5].shape, F32),
        pltpu.VMEM((images, seq_rows, 1), F32),
        pltpu.VMEM((seq_rows, 128), F32),
        pltpu.VMEM((seq_rows, 128), F32),
        pltpu.VMEM((8, width), F32),
        pltpu.VMEM((slots, 8), F32),
        pltpu.VMEM((RANK, width), F32),
        pltpu.VMEM((2 * RANK, 256), BF),
        pltpu.VMEM((2 * RANK, 2 * narrow), BF),
        pltpu.VMEM((nt, 5, RANK, width), F32),
        pltpu.VMEM((4, RANK, width), F32),
        *[pltpu.VMEM((size, RANK, width), F32) for size in (ns, nd, ns)],
        *[pltpu.VMEM((size, RANK, width), F32) for size in (ns * nt, nd)],
        pltpu.VMEM((nt, RANK, width), F32),
        *[pltpu.VMEM((size, 2, width), F32) for size in (ns, nd)],
        *[pltpu.VMEM((size, RANK, wide), BF) for size in (4, ns, nd, ns)],
        *[pltpu.VMEM((size, 3 * RANK, narrow), BF) for size in (ns, nd)],
        *[pltpu.VMEM((size, RANK, wide), F32) for size in (ns, nd)],
        dma((23,)),
        *[dma((images,))] * 2,
        *[dma((4,))] * 2,
        dma((images,)),
        dma((images, 3, 3)),
        *[dma((images,))] * 4,
        *[dma((images, 2))] * 2,
        dma((images,)),
        dma((images, 3)),
        *[dma((images + 1,))] * 2,
        *[dma((16,))] * 2,
        *[pltpu.VMEM(array.shape, array.dtype) for array in small],
    ]
    return pl.pallas_call(
        functools.partial(block_kernel, mesh_sizes, images),
        out_shape=outs,
        in_specs=[hbm_spec] * (len(small) + len(hbm)),
        out_specs=[vmem] * len(outs),
        scratch_shapes=scratch,
        compiler_params=pltpu.CompilerParams(
            collective_id=0, has_side_effects=True, vmem_limit_bytes=(LIMIT + nd // 8) * 2**20
        ),
        name="block",
    )(*small, *hbm)


def per_device(
    tokens,
    out_grad,
    keep_mask,
    w_qkv,
    w_out,
    w_gate_up,
    w_down,
    norm_pack,
    inner_pack,
    moment_qkv,
    moment_out,
    moment_gate_up,
    moment_down,
    moment_norm,
    moment_inner,
    error_qkv,
    error_out,
    error_gate_up,
    error_down,
    basis_qkv,
    basis_out,
    basis_gate_up,
    basis_down,
):
    own_rows, images, width = tokens.shape
    slot_count = keep_mask.shape[0]
    sizes = tuple(lax.axis_size(axis) for axis in ("dp", "seq", "tensor"))

    def turn(array):
        return jnp.swapaxes(array, -1, -2)

    results = block(
        sizes,
        (
            jnp.transpose(keep_mask), norm_pack, inner_pack, moment_norm, moment_inner,
            *(turn(basis) for basis in (basis_qkv, basis_out, basis_gate_up, basis_down)),
        ),
        (
            jnp.swapaxes(tokens, 0, 1), turn(w_qkv), w_out, w_gate_up, w_down, jnp.swapaxes(out_grad, 0, 1),
            turn(error_qkv[0]), error_out[0], error_gate_up[0], error_down[0],
            turn(moment_qkv), moment_out, moment_gate_up, moment_down,
        ),
    )
    grads, lows, fulls, moments = results[0:2], results[2:7], results[7:11], results[11:15]
    (
        residual, input_grad, new_moment_norm, new_moment_inner, new_norm_pack, new_inner_pack,
        factor_left, factor_qkv, factor_out, factor_gate_up, factor_down,
        new_error_qkv, new_error_out, new_error_gate_up, new_error_down,
        new_moment_qkv, new_moment_out, new_moment_gate_up, new_moment_down,
        new_w_qkv, new_w_out, new_w_gate_up, new_w_down,
        branch_rms,
    ) = store(
        (*grads, *results[15:17], *results[21:23]), results[23], lows, fulls, moments, results[17:21],
        float(slot_count * images * lax.axis_size("dp") * width),
    )
    return (
        jnp.swapaxes(residual, 0, 1), jnp.swapaxes(input_grad, 0, 1),
        *(turn(factor) for factor in (factor_left, factor_qkv, factor_out, factor_gate_up, factor_down)),
        turn(new_error_qkv)[None], new_error_out[None], new_error_gate_up[None], new_error_down[None],
        turn(new_moment_qkv), new_moment_out, new_moment_gate_up, new_moment_down, new_moment_norm, new_moment_inner,
        turn(new_w_qkv), new_w_out, new_w_gate_up, new_w_down, new_norm_pack, new_inner_pack,
        branch_rms,
    )


def solution(mesh):
    placed = (
        P(("seq", "tensor"), "dp", None),
        P("seq", "dp", None),
        P(None, "dp"),
        P(None, None, "tensor"),
        P("tensor", None),
        P(None, None, "tensor"),
        P("tensor", None),
        P(),
        P(None, "tensor"),
        P(None, None, "tensor"),
        P("tensor", None),
        P(None, None, "tensor"),
        P("tensor", None),
        P(),
        P(None, "tensor"),
        P(("dp", "seq"), None, None, "tensor"),
        P(("dp", "seq"), "tensor", None),
        P(("dp", "seq"), None, None, "tensor"),
        P(("dp", "seq"), "tensor", None),
        P(None, "tensor", None),
        P("tensor", None),
        P(None, "tensor", None),
        P("tensor", None),
    )
    return jax.shard_map(
        per_device,
        mesh=mesh,
        in_specs=placed,
        out_specs=(
            P(("seq", "tensor"), "dp", None),
            P(("seq", "tensor"), "dp", None),
            P(),
            P(None, "tensor", None),
            P("tensor", None),
            P(None, "tensor", None),
            P("tensor", None),
            P(("dp", "seq"), None, None, "tensor"),
            P(("dp", "seq"), "tensor", None),
            P(("dp", "seq"), None, None, "tensor"),
            P(("dp", "seq"), "tensor", None),
            P(None, None, "tensor"),
            P("tensor", None),
            P(None, None, "tensor"),
            P("tensor", None),
            P(),
            P(None, "tensor"),
            P(None, None, "tensor"),
            P("tensor", None),
            P(None, None, "tensor"),
            P("tensor", None),
            P(),
            P(None, "tensor"),
            P(),
        ),
        check_vma=False,
    )
```

```python
import functools
import math

import jax
import jax.numpy as jnp
from jax import lax
from jax.experimental import pallas as pl
from jax.experimental.pallas import tpu as pltpu
from jax.sharding import PartitionSpec as P

DH = 64
FF = 1024
GRID = 32
RANK = 8
QUARTER = DH // 4
CHUNK = 16
LIMIT = 46


EPSILON = 1e-06
MOMENTUM = 0.9
STEP_RATE = 0.5
MESH = pl.DeviceIdType.MESH
BF = jnp.bfloat16
F32 = jnp.float32


def split(value):
    high = value.astype(BF)
    return high, (value - high.astype(F32)).astype(BF)


def dot(left, right, dims):
    return lax.dot_general(left, right, (dims, ((), ())), preferred_element_type=F32)


NN = ((1,), (0,))
NT = ((1,), (1,))
TN = ((0,), (0,))


def two_rows(rows):
    high, low = split(rows)
    return jnp.concatenate([high.astype(F32), low.astype(F32)], 0).astype(BF)


def fold(rows):
    return rows[0:RANK] + rows[RANK:]


def fine_dot(left, right, dims):
    right_high, right_low = split(right)
    return fold(dot(two_rows(left), right_high, dims)) + dot(left.astype(BF), right_low, dims)


def gram_schmidt(stack):
    rows = lax.broadcasted_iota(jnp.int32, (1, RANK, 1), 1)
    for index in range(RANK):
        column = stack[:, index : index + 1, :]
        products = jnp.sum(stack * column, -1, keepdims=True)
        scale = lax.rsqrt(products[:, index : index + 1, :] + EPSILON)
        done = column * scale
        rest = stack - (products * scale) * done
        stack = jnp.where(rows < index, stack, jnp.where(rows == index, done, rest))
    return stack


class Moves:
    def __init__(self, span, send, receive, device):
        self.whole = pltpu.make_async_remote_copy(
            src_ref=span, dst_ref=span, send_sem=send, recv_sem=receive, device_id=device, device_id_type=MESH
        )

    def arrive(self):
        self.whole.wait()


def peers_of(axis, size):
    me = lax.axis_index(axis)
    if size == 4 and axis == "dp":
        upper = lax.div(me, 2)
        return [3 - 3 * upper, 2 - upper, 1 - me + 4 * upper]
    if size == 4 and axis == "seq":
        return [3 - me, me + 1 - 2 * lax.rem(me, 2), lax.rem(me + 2, 4)]
    return [lax.rem(me + step, size) for step in range(1, size)]


def exchange(axes, sizes, buffer, send, receive, pieces=None):
    own = [lax.axis_index(axis) for axis in axes]
    place = own[0]
    devices = [{axes[0]: peer} for peer in peers_of(axes[0], sizes[0])]
    if len(axes) == 2:
        place = own[0] * sizes[1] + own[1]
        others = peers_of(axes[1], sizes[1])
        devices = [{**device, axes[1]: peer} for device in devices for peer in (own[1], *others)]
        devices += [{axes[0]: own[0], axes[1]: peer} for peer in others]
    for device in devices:
        pltpu.make_async_remote_copy(
            src_ref=buffer.at[place] if pieces is None else pieces.at[device[axes[0]]],
            dst_ref=buffer.at[place],
            send_sem=send,
            recv_sem=receive,
            device_id=device,
            device_id_type=MESH,
        ).start()
    return Moves(buffer.at[0 : len(devices)], send, receive, devices[0])


def arrive(moves):
    for move in moves:
        move.arrive()


def total(buffer, size):
    value = buffer[0].astype(F32)
    for index in range(1, size):
        value = value + buffer[index].astype(F32)
    return value


def greet(axes, barrier):
    for axis, size in axes:
        me = lax.axis_index(axis)
        for step in range(1, size):
            pl.semaphore_signal(
                barrier, inc=1, device_id={axis: lax.rem(me + step, size)}, device_id_type=MESH
            )


def triple_first(rows):
    high, low = split(rows)
    return jnp.concatenate([high.astype(F32), high.astype(F32), low.astype(F32)], 0)


def triple_second(rows):
    high, low = split(rows)
    return jnp.concatenate([high.astype(F32), low.astype(F32), high.astype(F32)], 0)


def store_kernel(total_rows, plain, *refs):
    sources, rest = refs[:plain], refs[plain:]
    squares, factor_left, factor_qkv, factor_out, factor_gate_up, factor_down = rest[:6]
    fulls, moments, weights = rest[6:10], rest[10:14], rest[14:18]
    targets, rest = rest[18 : 18 + plain], rest[18 + plain :]
    results, branch_rms, fresh, roots_kept, sems = rest[:12], rest[12], rest[13:25], rest[25], rest[26]
    copies = [
        pltpu.make_async_copy(source, target, sems.at[number])
        for number, (source, target) in enumerate(zip(sources, targets))
    ]
    for copy in copies:
        copy.start()

    def settle(number, approx, pick):
        full, moment, weight = (pick(group[number]) for group in (fulls, moments, weights))
        places = (number, 4 + number, 8 + number)
        error_to, moment_to, weight_to = (pick(fresh[place]) for place in places)
        error_to[...] = full[...] - approx
        momentum = MOMENTUM * moment[...] + approx
        moment_to[...] = momentum
        weight_to[...] = weight[...] - STEP_RATE * momentum
        for place in places:
            copy = pltpu.make_async_copy(pick(fresh[place]), pick(results[place]), sems.at[len(copies)])
            copy.start()
            copies.append(copy)

    roots = jnp.sqrt(jnp.sum(squares[...], -1, keepdims=True) / total_rows)
    for index in range(2):
        roots_kept[index] = roots[index, 0]
    copies.append(pltpu.make_async_copy(roots_kept, branch_rms, sems.at[len(copies)]))
    copies[-1].start()

    def product(rows, columns):
        return dot(rows.astype(BF), columns.astype(BF), TN)

    lefts = [triple_first(factor_left[index]) for index in range(5)]
    for index in range(2):
        settle(2, product(lefts[2 + index], triple_second(factor_gate_up[index])), lambda ref: ref.at[index])
    settle(3, product(triple_second(factor_down[...]), lefts[4]), lambda ref: ref)
    settle(1, product(triple_second(factor_out[...]), lefts[1]), lambda ref: ref)
    for index in range(3):
        settle(0, product(triple_second(factor_qkv[index]), lefts[0]), lambda ref: ref.at[index])
    for copy in copies:
        copy.wait()


def store(plain, squares, factors, fulls, moments, weights, total_rows):
    vmem = pl.BlockSpec(memory_space=pltpu.VMEM)
    matrices = [*fulls, *moments, *weights]
    shapes = [jax.ShapeDtypeStruct(array.shape, F32) for array in (*plain, *factors, *matrices)]
    count = len(plain) + len(factors)
    return pl.pallas_call(
        functools.partial(store_kernel, total_rows, count),
        out_shape=[*shapes, jax.ShapeDtypeStruct((2,), F32)],
        in_specs=[vmem] * (count + 1 + len(factors) + 12),
        out_specs=[pl.BlockSpec(memory_space=pltpu.HBM)] * (len(shapes) + 1),
        scratch_shapes=[
            *[pltpu.VMEM(array.shape, F32) for array in matrices],
            pltpu.SMEM((2,), F32),
            pltpu.SemaphoreType.DMA((count + 22,)),
        ],
        compiler_params=pltpu.CompilerParams(vmem_limit_bytes=24 * 2**20),
        name="store",
    )(*plain, *factors, squares, *factors, *matrices)


def swap_quarters(tile):
    lane = lax.broadcasted_iota(jnp.int32, (1, 128), 1)
    low = lax.rem(lax.div(lane, QUARTER), 2) == 0
    return jnp.where(low, pltpu.roll(tile, 128 - QUARTER, 1), pltpu.roll(tile, QUARTER, 1))


def turn_pairs(pairs, cosine, sine):
    keys = lax.broadcasted_iota(jnp.int32, (1, 128), 1) < DH
    first, second, third = (pairs[:, start : start + 128] for start in (0, 128, 256))
    first = first * cosine + swap_quarters(first) * sine
    second = jnp.where(keys, second * cosine + swap_quarters(second) * sine, second)
    return jnp.concatenate([first, second, third], -1)


def turn_queries(raw, cosine, sine):
    tiles = (raw[:, start : start + 128] for start in (0, 128))
    return jnp.concatenate([tile * cosine + swap_quarters(tile) * sine for tile in tiles], -1)


def angle_tables(first_slot, count):
    slots = first_slot + lax.broadcasted_iota(jnp.int32, (count, 128), 0)
    place = lax.rem(lax.broadcasted_iota(jnp.int32, (count, 128), 1), DH)
    inside = jnp.logical_and(slots >= 1, slots <= GRID * GRID)
    patch = jnp.where(inside, slots - 1, 0)
    quarter = lax.div(place, QUARTER)
    position = jnp.where(quarter < 2, lax.div(patch, GRID), lax.rem(patch, GRID)).astype(F32)
    power = lax.rem(place, QUARTER).astype(F32)
    angles = position * jnp.exp(power * (-math.log(10000.0) / QUARTER)) * (16.0 / GRID)
    sine = jnp.sin(angles)
    return jnp.cos(angles), jnp.where(lax.rem(quarter, 2) == 0, -sine, sine)


def norm_parts(values, gain, bias):
    centre = values - jnp.mean(values, -1, keepdims=True)
    spread = jnp.mean(centre * centre, -1, keepdims=True)
    inverse = lax.rsqrt(spread + EPSILON)
    normed = centre * inverse
    return (normed * gain + bias, normed, inverse)


def norm_back(grad, normed, inverse, gain):
    scaled = grad * gain
    return inverse * (
        scaled
        - jnp.mean(scaled, -1, keepdims=True)
        - normed * jnp.mean(scaled * normed, -1, keepdims=True)
    )


def column_sums(value):
    return jnp.sum(value, 0, keepdims=True)


def block_kernel(sizes, images, *refs):
    smalls = refs[0:9]
    (
        tokens_hbm, w_qkv_hbm, w_out_hbm, w_gate_up_hbm, w_down_hbm, out_grad_hbm,
        error_qkv_hbm, error_out_hbm, error_gate_up_hbm, error_down_hbm,
        moment_qkv_hbm, moment_out_hbm, moment_gate_up_hbm, moment_down_hbm,
    ) = refs[9:23]
    (
        residual, input_grad, factor_left, factor_qkv, factor_out, factor_gate_up, factor_down,
        full_qkv, full_out, full_gate_up, full_down,
        moment_qkv, moment_out, moment_gate_up, moment_down, new_moment_norm, new_moment_inner,
        w_qkv, w_out, w_gate_up, w_down, new_norm_pack, new_inner_pack, squares,
        normed_one, normed_one_all, keys_values, queries, probs, scores, grad_scores,
        attended, attended_low, attended_in, attended_send,
        out_low, gate_up_low, down_low, inner_all, query_low, key_value_low,
        slim_rows, grad_middle, wide_rows, wide_rows_send, grad_down, queries_t,
        grad_attended, grad_attended_send, grad_attended_all, grad_query, grad_query_low, grad_pairs,
        *rest,
    ) = refs[23:]
    pairs_send, pairs_x, pairs_y, relay_x, relay_y = rest[0:5]
    ( grad_one, grad_one_recv, sum_query, sum_pairs, inner_sums, inner_recv,
        tokens, out_grad, mask, cosine, sine, extra, kept_rows, late_sum, thin_query, thin_pairs,
        early_t, early_all, early_in, early_d, early_left, late_s, late_d, norm_t, norm_s, norm_d,
        right_all, right_in, right_d, right_sum, slim_s, slim_d, tiny_s, tiny_d,
        local_sems, one_send, one_recv, weight_send, weight_recv, pair_send, pair_recv,
        att_send, att_recv, datt_send, datt_recv, rows_send, rows_recv, back_send, back_recv,
        final_send, final_recv, low_send, low_recv,
        keep, norm_pack, inner_pack, moment_norm, moment_inner, basis_qkv, basis_out, basis_gate_up, basis_down,
    ) = rest[5:]
    copied = (keep, norm_pack, inner_pack, moment_norm, moment_inner, basis_qkv, basis_out, basis_gate_up, basis_down)
    nd, ns, nt = sizes
    me_t, me_s = lax.axis_index("tensor"), lax.axis_index("seq")
    other = 1 - me_t
    near_x = me_s + 1 - 2 * lax.rem(me_s, 2)
    near_y = lax.rem(me_s + 2, 4)
    far = 3 - me_s
    me_d = lax.axis_index("dp")
    own, width = tokens.shape[1], tokens.shape[2]
    seq_rows = 2 * own
    slots = ns * seq_rows
    heads = w_qkv.shape[1] // DH
    wide = w_down.shape[0]
    hidden_all = 2 * wide
    scale = (images * seq_rows) ** (-0.5)
    top = (own + 15) // 16 * 16
    upper, lower = slice(0, top), slice(top, seq_rows)
    own_rows = pl.ds(pl.multiple_of(me_t * own, 8), own)
    other_rows = pl.ds(pl.multiple_of(other * own, 8), own)

    barrier = pltpu.get_barrier_semaphore()
    greet((("tensor", nt), ("seq", ns), ("dp", nd)), barrier)
    loads = [
        pltpu.make_async_copy(source, target, local_sems.at[number])
        for number, (source, target) in enumerate(
            (
                (tokens_hbm, tokens), (w_qkv_hbm, w_qkv),
                (w_out_hbm, w_out), (w_gate_up_hbm, w_gate_up), (w_down_hbm, w_down), (out_grad_hbm, out_grad),
                (error_qkv_hbm, full_qkv), (error_out_hbm, full_out),
                (error_gate_up_hbm, full_gate_up), (error_down_hbm, full_down),
                (moment_qkv_hbm, moment_qkv), (moment_out_hbm, moment_out),
                (moment_gate_up_hbm, moment_gate_up), (moment_down_hbm, moment_down), *zip(smalls, copied),
            )
        )
    ]
    for load in (loads[15], loads[0], loads[1]):
        load.start()

    def to_partner(source, target, send, receive):
        return pltpu.make_async_remote_copy(
            src_ref=source, dst_ref=target, send_sem=send, recv_sem=receive,
            device_id={"tensor": other}, device_id_type=MESH,
        )

    def to_seq(source, target, send, receive, peer):
        return pltpu.make_async_remote_copy(
            src_ref=source, dst_ref=target, send_sem=send, recv_sem=receive,
            device_id={"seq": peer}, device_id_type=MESH,
        )

    def one_copy(image):
        block = normed_one.at[me_t, image]
        return to_partner(block, block, one_send.at[image], one_recv.at[image])

    def weight_copies():
        return [
            to_partner(ref.at[me_t], ref.at[me_t], weight_send.at[number], weight_recv.at[number])
            for number, ref in enumerate((out_low, gate_up_low, down_low, inner_all))
        ]

    def pair_copy(image, tile, kind):
        place, peer = ((me_s, near_x), (me_s, near_y), (near_x, near_y), (near_y, near_x))[kind]
        block = keys_values.at[image, tile, place]
        if kind >= 2:
            block = block.at[(upper, lower)[kind - 2]]
        return to_seq(block, block, pair_send.at[image], pair_recv.at[image, tile, min(kind, 2)], peer)

    def send_pairs(image, tile):
        for kind in range(2):
            pair_copy(image, tile, kind).start()

    def forward_pairs(image, tile):
        for kind in range(2):
            pair_copy(image, tile, kind).wait_recv()
            pair_copy(image, tile, 2 + kind).start()

    def await_pairs(image, tile):
        block = keys_values.at[image, tile, far]
        to_seq(block, block, pair_send.at[image], pair_recv.at[image, tile, 2], far).wait_recv()

    def att_copy(image):
        return to_partner(
            attended_send.at[image], attended_in.at[me_t, image], att_send.at[image], att_recv.at[image]
        )

    def datt_copy(image):
        return to_partner(
            grad_attended_send.at[image], grad_attended.at[me_t, image], datt_send.at[image], datt_recv.at[image]
        )

    def row_copies(image):
        moves = ((slim_rows.at[me_t, image], slim_rows), (wide_rows_send.at[image], wide_rows))
        return [
            to_partner(source, target.at[me_t, image], rows_send.at[image, number], rows_recv.at[image, number])
            for number, (source, target) in enumerate(moves)
        ]

    def back_copy(image, kind):
        place, rows, target, there, peer = (
            (far, upper, relay_x, slice(0, top), near_x),
            (far, lower, relay_y, slice(0, seq_rows - top), near_y),
            (near_x, upper, pairs_x, upper, near_x),
            (near_y, lower, pairs_y, lower, near_y),
            (near_x, lower, pairs_x, lower, near_x),
            (near_y, upper, pairs_y, upper, near_y),
        )[kind]
        return to_seq(
            pairs_send.at[image, place, rows], target.at[image, there],
            back_send.at[image], back_recv.at[image, min(kind, 2)], peer,
        )

    def relay_back(image):
        for place, rows, inbox, arrival, onward in ((near_y, upper, relay_x, 0, 5), (near_x, lower, relay_y, 1, 4)):
            back_copy(image, arrival).wait_recv()
            value = pairs_send[image, place, rows].astype(F32) + inbox[image].astype(F32)
            pairs_send[image, place, rows] = value.astype(BF)
            back_copy(image, onward).start()

    def final_copy(image):
        return to_partner(
            grad_one.at[image, other_rows], grad_one_recv.at[image], final_send.at[image], final_recv.at[image]
        )

    def inner_copy():
        return to_partner(
            inner_sums.at[other], inner_recv, final_send.at[images], final_recv.at[images]
        )


    cosine[...], sine[...] = angle_tables(me_s * seq_rows, seq_rows)
    loads[15].wait()
    gain_one, bias_one = norm_pack[0:1], norm_pack[1:2]
    gain_two, bias_two = norm_pack[2:3], norm_pack[3:4]
    loads[0].wait()
    for image in range(images):
        normed, _, _ = norm_parts(tokens[image].astype(F32), gain_one, bias_one)
        normed_one[me_t, image] = normed.astype(BF)
        if image == 0:
            pl.semaphore_wait(barrier, (nt - 1) + (ns - 1) + (nd - 1))
        one_copy(image).start()
    for load in (*loads[2:5], loads[14], *loads[16:23], *loads[5:14]):
        load.start()
    loads[1].wait()

    narrow = heads * DH
    pad = jnp.zeros((256 - narrow, width), BF)
    query_low[...] = jnp.concatenate([w_qkv[0].astype(BF), pad], 0)
    key_value_low[0:narrow] = w_qkv[1].astype(BF)
    key_value_low[narrow : 2 * narrow] = w_qkv[2].astype(BF)

    def project(image, carry):
        one_copy(image).wait_recv()
        blocks = [normed_one[half, image] for half in range(2)]
        pairs = jnp.concatenate([dot(block, key_value_low[...], NT) for block in blocks], 0)
        pairs = turn_pairs(pairs, cosine[...], sine[...])
        for tile in range(3):
            keys_values[image, tile, me_s] = pairs[:, 128 * tile : 128 * tile + 128].astype(BF)

        @pl.when(image == 0)
        def _():
            for tile in range(3):
                send_pairs(image, tile)

        raw = jnp.concatenate([dot(block, query_low[...], NT) for block in blocks], 0)
        raw = turn_queries(raw, cosine[...], sine[...]) * (DH ** (-0.5))
        lane = lax.broadcasted_iota(jnp.int32, (1, 128), 1)
        for head in range(heads):
            tile = raw[:, head // 2 * 128 : head // 2 * 128 + 128]
            queries[image * heads + head] = jnp.where(lax.div(lane, DH) == head % 2, tile, 0.0).astype(BF)
        normed_one_all[image] = jnp.concatenate([block.astype(F32) for block in blocks], 0).astype(BF)
        return carry

    lax.fori_loop(0, images, project, 0)

    for load in (loads[14], *loads[16:23]):
        load.wait()
    for load in loads[2:5]:
        load.wait()
    out_low[me_t] = jnp.concatenate([pad, w_out[...].astype(BF)], 0)
    for index in range(2):
        gate_up_low[me_t, index] = w_gate_up[index].astype(BF)
    down_low[me_t] = w_down[...].astype(BF)
    inner_all[me_t] = jnp.zeros_like(inner_all[me_t])
    inner_all[me_t, 0:2] = inner_pack[...]
    for copy in weight_copies():
        copy.start()
    kept = jnp.concatenate([keep[...].astype(F32), jnp.zeros((8 - images, slots), F32)], 0)
    kept_rows[...] = jnp.transpose(kept)
    kept = kept_rows[pl.ds(pl.multiple_of(me_s * seq_rows, 8), seq_rows)]
    for image in range(images):
        mask[image] = kept[:, image : image + 1]
    loads[5].wait()
    loads[6].wait()
    late_sum[...] = sum(fine_dot(basis_qkv[index], full_qkv[index], NN) for index in range(3))
    gap = jnp.zeros((RANK, 256 - narrow), F32)
    thin_query[...] = two_rows(jnp.concatenate([basis_qkv[0], gap], -1))
    thin_pairs[...] = two_rows(jnp.concatenate([basis_qkv[1], basis_qkv[2]], -1))
    extra[...] = jnp.zeros_like(extra)
    inner_sums[...] = jnp.zeros_like(inner_sums)

    def halves_of(lower, upper):
        lane = lax.broadcasted_iota(jnp.int32, (1, 128), 1)
        return jnp.where(lane < DH, lower, upper)

    def half_of(value, half):
        return halves_of(value, 0.0) if half == 0 else halves_of(0.0, value)

    def key_tile(image, index):
        return keys_values[image, index].reshape(slots, 128)

    def attend(image):
        @pl.when(image == 0)
        def _():
            forward_pairs(0, 0)
            forward_pairs(0, 1)
            forward_pairs(0, 2)
            for tile in range(3):
                send_pairs(1, tile)
            for copy in weight_copies():
                copy.wait_recv()

            def ahead(place, carry):
                cotangent = out_grad[place, own_rows] * mask[place, own_rows]
                for index, half in enumerate((me_t, other)):
                    grad_down[place, index] = dot(cotangent.astype(BF), down_low[half], NT)
                for head in range(heads):
                    turned = jnp.transpose(queries[place * heads + head].astype(F32))
                    start = head % 2 * DH
                    queries_t[place * heads + head] = turned[start : start + DH].astype(BF)
                return carry

            lax.fori_loop(0, images, ahead, 0)

        bias = jnp.where(keep[pl.ds(image, 1), :] > 0, 0.0, -1e30)

        def score(head):
            scores[head % 2] = dot(queries[image * heads + head], key_tile(image, head // 2), NT)

        def chances(head):
            for start in range(0, seq_rows, CHUNK):
                rows = slice(start, start + CHUNK)
                part = scores[head % 2, rows] + bias
                part = jnp.exp(part - jnp.max(part, -1, keepdims=True))
                part = part * (1.0 / jnp.sum(part, -1, keepdims=True))
                probs[image * heads + head, rows] = part.astype(BF)

        def mix(head):
            return dot(probs[image * heads + head], key_tile(image, 1 + (head + 1) // 2), NN)

        await_pairs(image, 0)
        score(0)
        score(1)
        chances(0)
        await_pairs(image, 1)
        score(2)
        mixed = [mix(0)]
        chances(1)
        chances(2)
        await_pairs(image, 2)
        mixed.append(mix(1))
        mixed.append(mix(2))
        attended[:, 0:128] = half_of(mixed[0], 1)
        attended[:, 128:256] = halves_of(mixed[1], mixed[2])
        attended_low[image] = attended[...].astype(BF)
        attended_in[me_t, image] = attended[own_rows].astype(BF)
        attended_send[image] = attended[other_rows].astype(BF)
        att_copy(image).start()

        @pl.when(image == 0)
        def _():
            forward_pairs(1, 0)

        @pl.when(image == 1)
        def _():
            for load in loads[7:10]:
                load.wait()
            weights(0)
            forward_pairs(2, 0)

        @pl.when(image == 2)
        def _():
            relay_back(0)

    def feed(image):
        att_copy(image).wait_recv()
        inputs = tokens[image].astype(F32)
        branch = sum(dot(attended_in[half, image], out_low[half], NN) for half in range(2))
        middle = inputs + branch
        extra[4:5] += column_sums(branch * branch)
        normed, hat_two, inverse_two = norm_parts(middle, gain_two, bias_two)
        rows_two = normed.astype(BF)
        slim_rows[me_t, image, :, 0:width] = rows_two
        halves = (me_t, other)
        gates = [dot(rows_two, gate_up_low[half, 0], NN) for half in halves]
        ups = [dot(rows_two, gate_up_low[half, 1], NN) for half in halves]
        sigmoids = [1.0 / (1.0 + jnp.exp(-gate)) for gate in gates]
        hiddens = [gate * sigmoid * up for gate, sigmoid, up in zip(gates, sigmoids, ups)]
        mean = sum(jnp.sum(hidden, -1, keepdims=True) for hidden in hiddens) / hidden_all
        centres = [hidden - mean for hidden in hiddens]
        spread = sum(jnp.sum(centre * centre, -1, keepdims=True) for centre in centres) / hidden_all
        inverse_three = lax.rsqrt(spread + EPSILON)
        hats = [centre * inverse_three for centre in centres]
        lows = [
            (hat * inner_all[half, 0:1] + inner_all[half, 1:2]).astype(BF)
            for hat, half in zip(hats, halves)
        ]
        branch = sum(dot(low, down_low[half], NN) for low, half in zip(lows, halves))
        extra[5:6] += column_sums(branch * branch)
        residual[image] = middle + branch

        @pl.when(image == 0)
        def _():
            forward_pairs(1, 1)

        cotangent = out_grad[image, own_rows] * mask[image, own_rows]
        grads = [grad_down[image, index] for index in range(2)]
        for half, grad, hat in zip(halves, grads, hats):
            inner_sums[half, 0:1] += column_sums(grad * hat)
            inner_sums[half, 1:2] += column_sums(grad)
        scaled = [grad * inner_all[half, 0:1] for grad, half in zip(grads, halves)]
        first = sum(jnp.sum(value, -1, keepdims=True) for value in scaled) / hidden_all
        second = (
            sum(jnp.sum(value * hat, -1, keepdims=True) for value, hat in zip(scaled, hats)) / hidden_all
        )
        grad_hiddens = [
            inverse_three * (value - first - hat * second) for value, hat in zip(scaled, hats)
        ]
        gate_rows = [
            (grad * up * (sigmoid + gate * sigmoid * (1.0 - sigmoid))).astype(BF)
            for grad, up, sigmoid, gate in zip(grad_hiddens, ups, sigmoids, gates)
        ]
        up_rows = [
            (grad * gate * sigmoid).astype(BF)
            for grad, gate, sigmoid in zip(grad_hiddens, gates, sigmoids)
        ]
        for number, pair in enumerate((lows, gate_rows, up_rows)):
            wide_rows[me_t, image, :, number * wide : number * wide + wide] = pair[0]
            wide_rows_send[image, :, number * wide : number * wide + wide] = pair[1]
        grad_two = sum(
            dot(gate_row, gate_up_low[half, 0], NT) + dot(up_row, gate_up_low[half, 1], NT)
            for gate_row, up_row, half in zip(gate_rows, up_rows, halves)
        )
        extra[2:3] += column_sums(grad_two * hat_two)
        extra[3:4] += column_sums(grad_two)
        back = cotangent + norm_back(grad_two, hat_two, inverse_two, gain_two)
        grad_middle[image] = back
        low = back.astype(BF)
        slim_rows[me_t, image, :, width:] = low
        grad_attended[me_t, image] = dot(low, out_low[me_t], NT).astype(BF)
        grad_attended_send[image] = dot(low, out_low[other], NT).astype(BF)
        datt_copy(image).start()
        for copy in row_copies(image):
            copy.start()

        @pl.when(image == 0)
        def _():
            forward_pairs(1, 2)
            for tile in range(3):
                send_pairs(2, tile)

    def attend_back(image):
        datt_copy(image).wait_recv()
        grad_attended_all[...] = jnp.concatenate(
            [grad_attended[half, image].astype(F32) for half in range(2)], 0
        )
        wides = [half_of(grad_attended_all[:, 0:128], 1)]
        wides += [half_of(grad_attended_all[:, 128:256], half) for half in range(2)]
        lows = [wide.astype(BF) for wide in wides]
        mixed = attended_low[image].astype(F32)
        deltas = [
            jnp.sum(wide * mixed[:, tile * 128 : tile * 128 + 128], -1, keepdims=True)
            for wide, tile in zip(wides, (0, 1, 1))
        ]

        def grad_chance(head):
            scores[head % 2] = dot(lows[head], key_tile(image, 1 + (head + 1) // 2), NT)

        def grad_score(head):
            for start in range(0, seq_rows, CHUNK):
                rows = slice(start, start + CHUNK)
                chance = probs[image * heads + head, rows].astype(F32)
                grad_scores[head, rows] = (chance * (scores[head % 2, rows] - deltas[head][rows])).astype(BF)

        def value_grad(head):
            start = (head + 1) % 2 * DH
            rows = jnp.transpose(wides[head])[start : start + DH].astype(BF)
            place = (heads + head) * DH
            grad_pairs[place : place + DH] = dot(rows, probs[image * heads + head], NN)

        def key_grad(head):
            place = head * DH
            grad_pairs[place : place + DH] = dot(queries_t[image * heads + head], grad_scores[head], NN)

        def query_grad(head):
            return dot(grad_scores[head], key_tile(image, head // 2), NN)

        grad_chance(0)
        grad_chance(1)
        value_grad(0)
        grad_score(0)
        grad_chance(2)
        value_grad(1)
        grad_score(1)
        query_grads = [query_grad(0)]
        key_grad(0)
        value_grad(2)
        grad_score(2)
        query_grads.append(query_grad(1))
        key_grad(1)
        query_grads.append(query_grad(2))
        key_grad(2)
        grad_query[:, 0:128] = halves_of(query_grads[0], query_grads[1])
        grad_query[:, 128:256] = half_of(query_grads[2], 0)

        pairs_send[image] = jnp.transpose(grad_pairs[...]).astype(BF).reshape(ns, seq_rows, width)

        @pl.when(image == 0)
        def _():
            forward_pairs(2, 1)
            forward_pairs(2, 2)

        for kind in range(4):
            back_copy(image, kind).start()
        raw = grad_query[...] * (DH ** (-0.5))
        raw = turn_queries(raw, cosine[...], -sine[...])
        grad_query_low[image] = raw.astype(BF)

    def weights(image):
        for copy in row_copies(image):
            copy.wait_recv()
        parts = []
        for half in range(2):
            place = slice(half * own, half * own + own)
            grad_branch = (out_grad[image, place] * mask[image, place]).astype(BF)
            normed_three, grad_gate, grad_up = (
                wide_rows[half, image, :, number * wide : number * wide + wide] for number in range(3)
            )
            rows_two, low = slim_rows[half, image, :, 0:width], slim_rows[half, image, :, width:]
            mixed = attended_low[image].astype(F32)[place].astype(BF)
            parts.append(((normed_three, grad_branch), (rows_two, grad_gate), (rows_two, grad_up), (mixed, low)))
        down, gate, up, out = (dot(*first, TN) + dot(*second, TN) for first, second in zip(*parts))
        full_down[...] += down * scale
        full_gate_up[0] += gate * scale
        full_gate_up[1] += up * scale
        full_out[...] += out[256 - narrow :] * scale

    def stage(step, carry):
        @pl.when(step < images)
        def _():
            attend(step)

        @pl.when(step == images)
        def _():
            weights(1)
            relay_back(1)

        @pl.when(step >= 1)
        def _():
            attend_back(step - 1)

        @pl.when(step < images)
        def _():
            feed(step)

        return carry

    lax.fori_loop(0, images + 1, stage, 0)
    inner_copy().start()

    weights(images - 1)

    taken = []
    sizes_of = {"dp": nd, "seq": ns, "tensor": nt}

    def low_exchange(axes, *buffers):
        moves = []
        for buffer in buffers:
            place = len(taken)
            taken.append(place)
            moves.append(
                exchange(axes, [sizes_of[axis] for axis in axes], buffer, low_send.at[place], low_recv.at[place])
            )
        return moves

    def low_scatter(pieces, inbox):
        place = len(taken)
        taken.append(place)
        inbox[me_s] = pieces[me_s]
        return [exchange(("seq",), (ns,), inbox, low_send.at[place], low_recv.at[place], pieces)]

    share = 1.0 / (ns * nd)
    early = early_t.at[me_t]
    early[0] = fine_dot(basis_out[...], full_out[...], NN)
    for index in range(2):
        early[1 + index] = fine_dot(basis_gate_up[index], full_gate_up[index], NT)
    early[3] = fine_dot(basis_down[...], full_down[...], NN)
    early[4] = extra[...]
    early_moves = low_exchange(("tensor",), early_t)

    sum_query[...] = jnp.zeros_like(sum_query)
    sum_pairs[...] = jnp.zeros_like(sum_pairs)

    def pairs_of(image):
        both = pairs_send.at[image, 0:2]
        to_seq(both, both, back_send.at[image], back_recv.at[image, 2], far).wait_recv()
        pairs = pairs_send[image, me_s].astype(F32)
        pairs = pairs + pairs_x[image].astype(F32) + pairs_y[image].astype(F32)
        pairs = turn_pairs(pairs, cosine[...], -sine[...]).astype(BF)
        rows = dot(thin_query[...], grad_query_low[image], NT) + dot(thin_pairs[...], pairs, NT)
        late_sum[...] += fold(dot(two_rows(fold(rows)), normed_one_all[image], NN)) * scale
        return pairs

    def finish_pairs(image, pairs):
        query = grad_query_low[image]
        grad_one[image] = dot(query, query_low[...], NN) + dot(pairs, key_value_low[...], NN)
        final_copy(image).start()
        sum_query[...] += dot(query, normed_one_all[image], TN)
        sum_pairs[...] += dot(pairs, normed_one_all[image], TN)

    finish_pairs(0, pairs_of(0))
    arrive(early_moves)
    summed = total(early_t, nt)
    early_all[...] = summed[0:4]
    early_moves = low_scatter(early_all, early_in)
    inner_copy().wait_recv()
    tiny_s[me_s] = jnp.zeros_like(tiny_s[me_s])
    tiny_s[me_s, 0:2] = ((inner_sums[me_t] + inner_recv[...]) * scale)[0:2]
    tiny_s[me_s, 2:6, 0:width] = summed[4, 2:6]
    tiny_moves = low_exchange(("seq",), tiny_s)
    relay_back(images - 1)
    finish_pairs(1, pairs_of(1))
    arrive(early_moves)
    early_d[me_d] = total(early_in, ns)
    early_moves = low_exchange(("dp",), early_d)
    arrive(tiny_moves)
    tiny_d[me_d] = total(tiny_s, ns)
    tiny_moves = low_exchange(("dp",), tiny_d)
    pairs = pairs_of(images - 1)
    late_s[me_s * nt + me_t] = late_sum[...]
    late_moves = low_exchange(("seq", "tensor"), late_s)
    finish_pairs(images - 1, pairs)
    full_qkv[0] += sum_query[0:narrow] * scale
    full_qkv[1] += sum_pairs[0:narrow] * scale
    full_qkv[2] += sum_pairs[narrow : 2 * narrow] * scale

    norm_t[me_t] = jnp.zeros_like(norm_t[me_t])

    def finish(image, carry):
        final_copy(image).wait_recv()
        grad = grad_one[image, own_rows] + grad_one_recv[image]
        _, hat_one, inverse_one = norm_parts(tokens[image].astype(F32), gain_one, bias_one)
        input_grad[image] = grad_middle[image] + norm_back(grad, hat_one, inverse_one, gain_one)
        norm_t[me_t, 0:1] += column_sums(grad * hat_one)
        norm_t[me_t, 1:2] += column_sums(grad)
        return carry

    def orthonormal(rows):
        return gram_schmidt(rows.reshape(1, RANK, width))[0]

    arrive(early_moves)
    early_left[me_s] = orthonormal(total(early_d, nd))
    early_moves = low_exchange(("seq",), early_left)
    arrive(late_moves)
    late_d[me_d] = total(late_s, ns * nt)
    late_moves = low_exchange(("dp",), late_d)
    lax.fori_loop(0, images, finish, 0)
    norm_moves = low_exchange(("tensor",), norm_t)
    arrive(early_moves)
    right = fine_dot(early_left[0], full_out[...], NT)
    right_all[0] = jnp.concatenate([right, jnp.zeros((RANK, wide - narrow), F32)], -1).astype(BF)
    for index in range(2):
        right_all[1 + index] = fine_dot(early_left[1 + index], full_gate_up[index], NN).astype(BF)
    right_all[3] = fine_dot(early_left[3], full_down[...], NT).astype(BF)
    early_moves = low_scatter(right_all, right_in)
    for index in range(4):
        factor_left[1 + index] = early_left[index]
    arrive(norm_moves)
    norm_s[me_s] = total(norm_t, nt)[0:2]
    arrive(late_moves)
    left = orthonormal(total(late_d, nd))
    rights = []
    for index in range(3):
        rights.append(fine_dot(left, full_qkv[index], NT))
    slim_s[me_s] = jnp.concatenate(rights, 0).astype(BF)
    late_moves = low_exchange(("seq",), slim_s, norm_s)
    factor_left[0] = left
    arrive(early_moves)
    right_d[me_d] = total(right_in, ns).astype(BF)
    early_moves = low_exchange(("dp",), right_d)
    for load in loads[10:14]:
        load.wait()
    arrive(tiny_moves)
    tiny = total(tiny_d, nd)
    squares[...] = tiny[4:6, 0:width]
    arrive(late_moves)
    slim_d[me_d] = total(slim_s, ns).astype(BF)
    norm_d[me_d] = total(norm_s, ns)
    late_moves = low_exchange(("dp",), slim_d, norm_d)
    fresh = MOMENTUM * moment_norm[2:4] + tiny[2:4, 0:width] * (share * scale)
    new_moment_norm[2:4] = fresh
    new_norm_pack[2:4] = norm_pack[2:4] - STEP_RATE * fresh
    fresh = MOMENTUM * moment_inner[...] + tiny[0:2] * share
    new_moment_inner[...] = fresh
    new_inner_pack[...] = inner_pack[...] - STEP_RATE * fresh
    arrive(early_moves)
    right_sum[me_s] = (total(right_d, nd) * share).astype(BF)
    early_moves = low_exchange(("seq",), right_sum)
    arrive(early_moves)
    factor_out[...] = right_sum[0].astype(F32)[:, 0:narrow]
    for index in range(2):
        factor_gate_up[index] = right_sum[1 + index].astype(F32)
    factor_down[...] = right_sum[3].astype(F32)
    arrive(late_moves)
    slim = total(slim_d, nd) * share
    for index in range(3):
        factor_qkv[index] = slim[8 * index : 8 * index + 8]
    fresh = MOMENTUM * moment_norm[0:2] + total(norm_d, nd) * (share * scale)
    new_moment_norm[0:2] = fresh
    new_norm_pack[0:2] = norm_pack[0:2] - STEP_RATE * fresh

    for image in range(images):
        for copy in (
            one_copy(image), att_copy(image), datt_copy(image), *row_copies(image), final_copy(image),
            *(
                to_seq(span, span, send, receive, far)
                for span, send, receive in (
                    (keys_values.at[image, :, 0:3], pair_send.at[image], pair_recv.at[image, 0, 2]),
                    (pairs_send.at[image, 0:3], back_send.at[image], back_recv.at[image, 2]),
                )
            ),
        ):
            copy.wait_send()
    for copy in (*weight_copies(), inner_copy()):
        copy.wait_send()


def block(mesh_sizes, small, hbm):
    nd, ns, nt = mesh_sizes
    images, own, width = hbm[0].shape
    seq_rows = 2 * own
    slots = ns * seq_rows
    top = (own + 15) // 16 * 16
    narrow = hbm[1].shape[1]
    heads = narrow // DH
    wide = small[2].shape[1]
    shape = jax.ShapeDtypeStruct
    matrices = ((3, narrow, width), (narrow, width), (2, width, wide), (wide, width))
    shapes = (
        (images, own, width), (images, own, width),
        (5, RANK, width), (3, RANK, narrow), (RANK, narrow), (2, RANK, wide), (RANK, wide),
        *matrices, *matrices, (4, width), (2, wide), *matrices, (4, width), (2, wide), (2, width),
    )
    outs = [pltpu.VMEM(dims, F32) for dims in shapes]
    vmem = pl.BlockSpec(memory_space=pltpu.VMEM)
    hbm_spec = pl.BlockSpec(memory_space=pltpu.HBM)
    dma = pltpu.SemaphoreType.DMA
    scratch = [
        pltpu.VMEM((2, images, own, width), BF),
        pltpu.VMEM((images, seq_rows, width), BF),
        pltpu.VMEM((images, 3, ns, seq_rows, 128), BF),
        pltpu.VMEM((images * heads, seq_rows, 128), BF),
        pltpu.VMEM((images * heads, seq_rows, slots), BF),
        pltpu.VMEM((2, seq_rows, slots), F32),
        pltpu.VMEM((heads, seq_rows, slots), BF),
        pltpu.VMEM((seq_rows, 256), F32),
        pltpu.VMEM((images, seq_rows, 256), BF),
        pltpu.VMEM((2, images, own, 256), BF),
        pltpu.VMEM((images, own, 256), BF),
        pltpu.VMEM((2, 256, width), BF),
        pltpu.VMEM((2, 2, width, wide), BF),
        pltpu.VMEM((2, wide, width), BF),
        pltpu.VMEM((2, 8, wide), F32),
        pltpu.VMEM((256, width), BF),
        pltpu.VMEM((2 * narrow, width), BF),
        pltpu.VMEM((2, images, own, 2 * width), BF),
        pltpu.VMEM((images, own, width), F32),
        pltpu.VMEM((2, images, own, 3 * wide), BF),
        pltpu.VMEM((images, own, 3 * wide), BF),
        pltpu.VMEM((images, 2, own, wide), F32),
        pltpu.VMEM((images * heads, DH, seq_rows), BF),
        pltpu.VMEM((2, images, own, 256), BF),
        pltpu.VMEM((images, own, 256), BF),
        pltpu.VMEM((seq_rows, 256), F32),
        pltpu.VMEM((seq_rows, 256), F32),
        pltpu.VMEM((images, seq_rows, 256), BF),
        pltpu.VMEM((width, slots), F32),
        *[
            pltpu.VMEM((images, *rows, width), BF)
            for rows in ((ns, seq_rows), (seq_rows,), (seq_rows,), (top,), (seq_rows - top,))
        ],
        pltpu.VMEM((images, seq_rows, width), F32),
        pltpu.VMEM((images, own, width), F32),
        pltpu.VMEM((256, width), F32),
        pltpu.VMEM((2 * narrow, width), F32),
        pltpu.VMEM((2, 8, wide), F32),
        pltpu.VMEM((8, wide), F32),
        pltpu.VMEM(hbm[0].shape, BF),
        pltpu.VMEM(hbm[5].shape, F32),
        pltpu.VMEM((images, seq_rows, 1), F32),
        pltpu.VMEM((seq_rows, 128), F32),
        pltpu.VMEM((seq_rows, 128), F32),
        pltpu.VMEM((8, width), F32),
        pltpu.VMEM((slots, 8), F32),
        pltpu.VMEM((RANK, width), F32),
        pltpu.VMEM((2 * RANK, 256), BF),
        pltpu.VMEM((2 * RANK, 2 * narrow), BF),
        pltpu.VMEM((nt, 5, RANK, width), F32),
        pltpu.VMEM((4, RANK, width), F32),
        *[pltpu.VMEM((size, RANK, width), F32) for size in (ns, nd, ns)],
        *[pltpu.VMEM((size, RANK, width), F32) for size in (ns * nt, nd)],
        pltpu.VMEM((nt, RANK, width), F32),
        *[pltpu.VMEM((size, 2, width), F32) for size in (ns, nd)],
        *[pltpu.VMEM((size, RANK, wide), BF) for size in (4, ns, nd, ns)],
        *[pltpu.VMEM((size, 3 * RANK, narrow), BF) for size in (ns, nd)],
        *[pltpu.VMEM((size, RANK, wide), F32) for size in (ns, nd)],
        dma((23,)),
        *[dma((images,))] * 2,
        *[dma((4,))] * 2,
        dma((images,)),
        dma((images, 3, 3)),
        *[dma((images,))] * 4,
        *[dma((images, 2))] * 2,
        dma((images,)),
        dma((images, 3)),
        *[dma((images + 1,))] * 2,
        *[dma((16,))] * 2,
        *[pltpu.VMEM(array.shape, array.dtype) for array in small],
    ]
    return pl.pallas_call(
        functools.partial(block_kernel, mesh_sizes, images),
        out_shape=outs,
        in_specs=[hbm_spec] * (len(small) + len(hbm)),
        out_specs=[vmem] * len(outs),
        scratch_shapes=scratch,
        compiler_params=pltpu.CompilerParams(
            collective_id=0, has_side_effects=True, vmem_limit_bytes=(LIMIT + nd // 8) * 2**20
        ),
        name="block",
    )(*small, *hbm)


def per_device(
    tokens,
    out_grad,
    keep_mask,
    w_qkv,
    w_out,
    w_gate_up,
    w_down,
    norm_pack,
    inner_pack,
    moment_qkv,
    moment_out,
    moment_gate_up,
    moment_down,
    moment_norm,
    moment_inner,
    error_qkv,
    error_out,
    error_gate_up,
    error_down,
    basis_qkv,
    basis_out,
    basis_gate_up,
    basis_down,
):
    own_rows, images, width = tokens.shape
    slot_count = keep_mask.shape[0]
    sizes = tuple(lax.axis_size(axis) for axis in ("dp", "seq", "tensor"))

    def turn(array):
        return jnp.swapaxes(array, -1, -2)

    results = block(
        sizes,
        (
            jnp.transpose(keep_mask), norm_pack, inner_pack, moment_norm, moment_inner,
            *(turn(basis) for basis in (basis_qkv, basis_out, basis_gate_up, basis_down)),
        ),
        (
            jnp.swapaxes(tokens, 0, 1), turn(w_qkv), w_out, w_gate_up, w_down, jnp.swapaxes(out_grad, 0, 1),
            turn(error_qkv[0]), error_out[0], error_gate_up[0], error_down[0],
            turn(moment_qkv), moment_out, moment_gate_up, moment_down,
        ),
    )
    grads, lows, fulls, moments = results[0:2], results[2:7], results[7:11], results[11:15]
    (
        residual, input_grad, new_moment_norm, new_moment_inner, new_norm_pack, new_inner_pack,
        factor_left, factor_qkv, factor_out, factor_gate_up, factor_down,
        new_error_qkv, new_error_out, new_error_gate_up, new_error_down,
        new_moment_qkv, new_moment_out, new_moment_gate_up, new_moment_down,
        new_w_qkv, new_w_out, new_w_gate_up, new_w_down,
        branch_rms,
    ) = store(
        (*grads, *results[15:17], *results[21:23]), results[23], lows, fulls, moments, results[17:21],
        float(slot_count * images * lax.axis_size("dp") * width),
    )
    return (
        jnp.swapaxes(residual, 0, 1), jnp.swapaxes(input_grad, 0, 1),
        *(turn(factor) for factor in (factor_left, factor_qkv, factor_out, factor_gate_up, factor_down)),
        turn(new_error_qkv)[None], new_error_out[None], new_error_gate_up[None], new_error_down[None],
        turn(new_moment_qkv), new_moment_out, new_moment_gate_up, new_moment_down, new_moment_norm, new_moment_inner,
        turn(new_w_qkv), new_w_out, new_w_gate_up, new_w_down, new_norm_pack, new_inner_pack,
        branch_rms,
    )


def solution(mesh):
    placed = (
        P(("seq", "tensor"), "dp", None),
        P("seq", "dp", None),
        P(None, "dp"),
        P(None, None, "tensor"),
        P("tensor", None),
        P(None, None, "tensor"),
        P("tensor", None),
        P(),
        P(None, "tensor"),
        P(None, None, "tensor"),
        P("tensor", None),
        P(None, None, "tensor"),
        P("tensor", None),
        P(),
        P(None, "tensor"),
        P(("dp", "seq"), None, None, "tensor"),
        P(("dp", "seq"), "tensor", None),
        P(("dp", "seq"), None, None, "tensor"),
        P(("dp", "seq"), "tensor", None),
        P(None, "tensor", None),
        P("tensor", None),
        P(None, "tensor", None),
        P("tensor", None),
    )
    return jax.shard_map(
        per_device,
        mesh=mesh,
        in_specs=placed,
        out_specs=(
            P(("seq", "tensor"), "dp", None),
            P(("seq", "tensor"), "dp", None),
            P(),
            P(None, "tensor", None),
            P("tensor", None),
            P(None, "tensor", None),
            P("tensor", None),
            P(("dp", "seq"), None, None, "tensor"),
            P(("dp", "seq"), "tensor", None),
            P(("dp", "seq"), None, None, "tensor"),
            P(("dp", "seq"), "tensor", None),
            P(None, None, "tensor"),
            P("tensor", None),
            P(None, None, "tensor"),
            P("tensor", None),
            P(),
            P(None, "tensor"),
            P(None, None, "tensor"),
            P("tensor", None),
            P(None, None, "tensor"),
            P("tensor", None),
            P(),
            P(None, "tensor"),
            P(),
        ),
        check_vma=False,
    )
```
